128 devices in a mesh: row: 8 (over z, core), col: 16 (over y, x).
Axes of the slice: x: 4, y: 4, z: 4, core: 2. Of those that a mesh axis runs over, the one named last changes fastest.
Arguments:
- clean: float32 [1344, 16384], P('row', 'col'), may hold values from -6 to 6
- noise: float32 [1344, 16384], P('row', 'col'), may hold values from -6 to 6
- bucket: int32 [64], replicated, may hold values from 0 to 31
- mod_table: float32 [1, 32, 1344], replicated, may hold values from -3 to 3
- w_first: float32 [1, 1344, 1344], P(None, 'row', 'col'), may hold values from -0.15625 to 0.15625
- w_second: float32 [1, 1344, 1344], P(None, 'col', 'row'), may hold values from -0.15625 to 0.15625
Outputs:
- grad_first: float32 [1, 1344, 1344], P(None, 'row', 'col')
- grad_second: float32 [1, 1344, 1344], P(None, 'col', 'row')
The draws below stay inside these ranges and needn't reach their ends.
All inputs are finite; a program needn't handle non-finite values.
Results may differ from the reference program's by a relative error of at most 0.018.
Values may be sent and summed in bfloat16 or wider, within the bound.
A program may use at most 64 MiB of HBM per device.

```python
import math
import jax
import jax.numpy as jnp
from jax import lax

WIDTH = 1344
PIX = 256
BLOCKS = 1
BUCKETS = 32
SAMPLES = 64


def place_ends(array, own_key, least, top_value):
    longest = array.shape.index(max(array.shape))
    spots = []
    for shift in (0, 1):
        where = [jax.random.randint(jax.random.fold_in(own_key, axis), (), 0, length) for axis, length in enumerate(array.shape)]
        where[longest] = (where[longest] + shift) % array.shape[longest]
        spots.append(tuple(where))
    return array.at[spots[0]].set(least).at[spots[1]].set(top_value)


def shard_levels(rng, extent, cuts, low, high):
    def one(dim, shards_of):
        heights = jax.random.uniform(jax.random.fold_in(jax.random.fold_in(rng, 6), dim), (shards_of,), jnp.float32, low / len(cuts), high / len(cuts))
        return jnp.repeat(jnp.exp(heights), extent[dim] // shards_of).reshape((-1,) + (1,) * (len(extent) - dim - 1))

    level = one(*cuts[0])
    for cut in cuts[1:]:
        level = level * one(*cut)
    return level


def scatter_about(stream_key, dims, deviation, bound, cuts=(), kind=jnp.bfloat16):
    values = jax.random.normal(stream_key, dims, jnp.float32) * deviation
    if len(cuts) > 0:
        values = shard_levels(stream_key, dims, cuts, -0.22, 0.18) * values
    return jnp.clip(values, min=-bound, max=bound).astype(kind)


def setup_inputs(seed: int = 0) -> dict:
    seeds = jax.random.split(jax.random.key(seed), 7)
    clean = scatter_about(seeds[0], (WIDTH, SAMPLES * PIX), 1.0, 6.0, ((0, 8), (1, 16)), jnp.float32)
    noise = scatter_about(seeds[1], (WIDTH, SAMPLES * PIX), 1.0, 6.0, ((0, 8), (1, 16)), jnp.float32)
    bucket = place_ends(jax.random.randint(seeds[2], (SAMPLES,), 0, BUCKETS), jax.random.fold_in(seeds[2], 1), 0, BUCKETS - 1).astype(jnp.int32)
    mod_table = scatter_about(seeds[3], (BLOCKS, BUCKETS, WIDTH), 0.3, 3.0, (), jnp.float32)
    w_first = scatter_about(seeds[4], (BLOCKS, WIDTH, WIDTH), WIDTH ** -0.5, 0.15625, ((1, 8), (2, 16)), jnp.float32)
    w_second = scatter_about(seeds[5], (BLOCKS, WIDTH, WIDTH), WIDTH ** -0.5, 0.15625, ((1, 16), (2, 8)), jnp.float32)
    return dict(clean=clean, noise=noise, bucket=bucket, mod_table=mod_table, w_first=w_first, w_second=w_second)


MIX_WEIGHT = 0.3
KEEP_COEF = (1.0 - MIX_WEIGHT) / math.sqrt((1.0 - MIX_WEIGHT) ** 2 + MIX_WEIGHT ** 2)
ADD_COEF = MIX_WEIGHT / math.sqrt((1.0 - MIX_WEIGHT) ** 2 + MIX_WEIGHT ** 2)
SILU_GAIN = 1.0 / 0.596

def noise_levels(bucket):
    return jnp.exp(-3.0 + 5.0 * (bucket.astype(jnp.float32) + 0.5) / BUCKETS)

def silu_slope(values):
    sig = jax.nn.sigmoid(values)
    return sig * (1.0 + values * (1.0 - sig))

def reference(clean, noise, bucket, mod_table, w_first, w_second):
    clean = clean.T
    noise = noise.T
    levels = jnp.repeat(noise_levels(bucket), PIX)[:, None]
    spread_root = jnp.sqrt(levels * levels + 0.25)
    state = ((clean + levels * noise) / spread_root).astype(jnp.bfloat16)
    target = clean * (2.0 * levels / spread_root) - noise * (0.5 / spread_root)
    onehot = (bucket[:, None] == jnp.arange(BUCKETS, dtype=jnp.int32)[None, :]).astype(jnp.float32)
    saved = []
    for block in range(BLOCKS):
        col_first = jnp.sqrt(lax.optimization_barrier(jnp.sum(w_first[block] * w_first[block], axis=0)) + 1.0)
        col_second = jnp.sqrt(lax.optimization_barrier(jnp.sum(w_second[block] * w_second[block], axis=0)) + 1.0)
        normed_first = (w_first[block] / col_first[None, :]).astype(jnp.bfloat16)
        normed_second = (w_second[block] / col_second[None, :]).astype(jnp.bfloat16)
        gains = jnp.dot(onehot, 1.0 + mod_table[block], precision=lax.Precision.HIGHEST, preferred_element_type=jnp.float32)
        gains = jnp.repeat(gains, PIX, axis=0)
        pre_act = jnp.dot(state, normed_first, preferred_element_type=jnp.float32)
        hidden = (jax.nn.silu(pre_act) * SILU_GAIN * gains).astype(jnp.bfloat16)
        branch = jnp.dot(hidden, normed_second, preferred_element_type=jnp.float32)
        saved.append((state, hidden, pre_act, gains, normed_first, normed_second, col_first, col_second))
        state = (KEEP_COEF * state.astype(jnp.float32) + ADD_COEF * branch).astype(jnp.bfloat16)
    grad_state = (state.astype(jnp.float32) - target) / SAMPLES
    firsts = []
    seconds = []
    for block in range(BLOCKS - 1, -1, -1):
        state_in, hidden, pre_act, gains, normed_first, normed_second, col_first, col_second = saved[block]
        dbranch = (ADD_COEF * grad_state).astype(jnp.bfloat16)
        gsecond = jnp.dot(hidden.T, dbranch, preferred_element_type=jnp.float32)
        dhidden = jnp.dot(dbranch, normed_second.T, preferred_element_type=jnp.float32)
        dpre = (dhidden * gains * silu_slope(pre_act) * SILU_GAIN).astype(jnp.bfloat16)
        gfirst = jnp.dot(state_in.T, dpre, preferred_element_type=jnp.float32)
        if block > 0:
            grad_state = KEEP_COEF * grad_state + jnp.dot(dpre, normed_first.T, preferred_element_type=jnp.float32)
        dot_first = lax.optimization_barrier(jnp.sum(w_first[block] * gfirst, axis=0))
        dot_second = lax.optimization_barrier(jnp.sum(w_second[block] * gsecond, axis=0))
        firsts.append(gfirst / col_first[None, :] - w_first[block] * (dot_first / col_first ** 3)[None, :])
        seconds.append(gsecond / col_second[None, :] - w_second[block] * (dot_second / col_second ** 3)[None, :])
    grad_first = jnp.stack(firsts[::-1], axis=0)
    grad_second = jnp.stack(seconds[::-1], axis=0)
    return (grad_first, grad_second)
```

```python
import math

import jax
import jax.numpy as jnp
from jax import lax
from jax.experimental import pallas as pl
from jax.experimental.pallas import tpu as pltpu
from jax.sharding import PartitionSpec as P

MESH = pl.DeviceIdType.MESH
F32 = jnp.float32
BF16 = jnp.bfloat16

WIDTH = 1344
PIX = 256
SAMPLES = 64
BUCKETS = 32
MIX_WEIGHT = 0.3
KEEP_COEF = (1.0 - MIX_WEIGHT) / math.sqrt((1.0 - MIX_WEIGHT) ** 2 + MIX_WEIGHT**2)
ADD_COEF = MIX_WEIGHT / math.sqrt((1.0 - MIX_WEIGHT) ** 2 + MIX_WEIGHT**2)
SILU_GAIN = 1.0 / 0.596

ROWS = 8
CHAN = WIDTH // ROWS
CHAN_PAD = 176
CP = ROWS * CHAN_PAD
BLOCK = WIDTH // 16
HALF = BLOCK // 2
HP = 48
HT = 16 * HP
PACK = 384
NN = (((1,), (0,)), ((), ()))
NT = (((1,), (1,)), ((), ()))
TN = (((0,), (0,)), ((), ()))
MAX_COPIES = 160


def dot(a, b, dims):
    return lax.dot_general(a, b, dims, preferred_element_type=F32)


def kernel(
    clean, noise, bucket, mod, wz, out,
    st, tg, s_all, t_all, wz_in, wa, wb, ga, gb,
    ra1, ra2, rx1, rx2, rb1, rb2, ry1, ry2,
    gain, scale1, pre, hid, dpre, raw2, raw2_in, norm_row, norm_in,
    dbr, dbn, dh, zs, zr, send_sems, recv_sems,
):
    r = lax.axis_index("row")
    k = lax.axis_index("col")
    z, c = r // 2, r % 2
    y, x = k // 4, k % 4

    def peer(dz=0, dc=0, dy=0, dx=0):
        return (
            ((z + dz) % 4) * 2 + (c + dc) % 2,
            ((y + dy) % 4) * 4 + (x + dx) % 4,
        )

    started = []

    def send(src, dst, device):
        i = len(started)
        copy = pltpu.make_async_remote_copy(
            src_ref=src,
            dst_ref=dst,
            send_sem=send_sems.at[i],
            recv_sem=recv_sems.at[i],
            device_id=device,
            device_id_type=MESH,
        )
        copy.start()
        started.append(copy)
        return copy

    group = [(dz, dc) for dz in (2, 1, 3, 0) for dc in (0, 1) if (dz, dc) != (0, 0)]
    barrier = pltpu.get_barrier_semaphore()
    near = [peer(dz=dz, dc=dc) for dz, dc in group]
    near += [peer(dx=1), peer(dx=3), peer(dy=1), peer(dy=3)]
    for device in near:
        pl.semaphore_signal(barrier, inc=1, device_id=device, device_id_type=MESH)

    def state_piece(d):
        zq = (z + d) % 4
        level_of = jnp.full((1, PIX), bucket[k * 4 + zq], jnp.int32).astype(F32)
        level = jnp.exp(-3.0 + 5.0 * (level_of + 0.5) / BUCKETS)
        spread = jnp.sqrt(level * level + 0.25)
        cols = pl.ds(pl.multiple_of(zq * PIX, PIX), PIX)
        cl = clean[:, cols]
        no = noise[:, cols]
        pad = jnp.zeros((CHAN_PAD - CHAN, PIX), F32)
        state = (cl + level * no) / spread
        target = cl * (2.0 * level / spread) - no * (0.5 / spread)
        return (
            jnp.concatenate([state, pad], axis=0).astype(BF16),
            jnp.concatenate([target, pad], axis=0).astype(BF16),
        )

    for d in range(4):
        state, target = state_piece(d)
        st[d] = state
        tg[d] = target
    s_all[r] = st[0]
    t_all[r] = tg[0]
    wz_in[r] = wz[c]

    pl.semaphore_wait(barrier, len(near))

    w_copies = [
        send(wz.at[(c + dc) % 2], wz_in.at[r], peer(dz=dz, dc=dc)) for dz, dc in group
    ]
    s_copies = {d: send(st.at[d], s_all.at[r], peer(dz=d)) for d in (2, 1, 3)}
    s_own = send(st.at[0], s_all.at[r], peer(dc=1))
    t_copies = {d: send(tg.at[d], t_all.at[r], peer(dz=d)) for d in (2, 1, 3)}
    t_own = send(tg.at[0], t_all.at[r], peer(dc=1))

    sample = k * 4 + z
    picked = lax.broadcasted_iota(jnp.int32, (BUCKETS, CP), 0) == bucket[sample]
    mod_row = jnp.sum(jnp.where(picked, 1.0 + mod[...], 0.0), axis=0, keepdims=True)
    for b in range(16):
        first = (BLOCK * b // 128) * 128
        lane = lax.broadcasted_iota(jnp.int32, (HP, 256), 1) + first
        row = lax.broadcasted_iota(jnp.int32, (HP, 256), 0)
        take = (lane == row + (BLOCK * b + HALF * c)) & (row < HALF)
        window = jnp.broadcast_to(mod_row[:, first : first + 256], (HP, 256))
        value = jnp.sum(jnp.where(take, window, 0.0), axis=1, keepdims=True)
        gain[b] = jnp.broadcast_to(value, (HP, PIX))

    for copy in w_copies:
        copy.wait_recv()
    wa[y, x] = jnp.concatenate(
        [wz_in[q][:, :CHAN_PAD].astype(F32) for q in range(ROWS)], axis=1
    ).astype(BF16)
    wb[x, y] = jnp.concatenate(
        [wz_in[q][:, CHAN_PAD : 2 * CHAN_PAD].astype(F32) for q in range(ROWS)], axis=1
    ).astype(BF16)

    class Side:
        pass

    def side_a():
        s = Side()
        s.w, s.g, s.i1, s.i2 = wa, ga, x, y
        s.p1 = lambda d: peer(dx=d)
        s.p2 = lambda d: peer(dy=d)
        s.cut = 32
        s.half1, s.half2, s.full1, s.full2 = rx1, ra1, rx2, ra2
        return s

    def side_b():
        s = Side()
        s.w, s.g, s.i1, s.i2 = wb, gb, y, x
        s.p1 = lambda d: peer(dy=d)
        s.p2 = lambda d: peer(dx=d)
        s.cut = 16
        s.half1, s.half2, s.full1, s.full2 = ry1, rb1, ry2, rb2
        return s

    a, b = side_a(), side_b()

    def at1(s, d):
        return (s.i1 + d) % 4

    def at2(s, d):
        return (s.i2 + d) % 4

    def own_out(s):
        block = s.w.at[s.i2, s.i1]
        s.first = {d: send(block, block, s.p1(d)) for d in (1, 3)}

    def spread_out(s, d):
        block = s.w.at[s.i2, at1(s, d)]
        s.second[d] = {e: send(block, block, s.p2(e)) for e in (1, 3)}

    for s in (a, b):
        own_out(s)
    for s in (a, b):
        s.second = {}
        spread_out(s, 0)

    for s in (a, b):
        s.first[1].wait_recv()
        block = s.w.at[s.i2, at1(s, 3), pl.ds(0, s.cut)]
        s.far_up = send(block, block, s.p1(1))
        s.first[3].wait_recv()
        block = s.w.at[s.i2, at1(s, 1), pl.ds(s.cut, HP - s.cut)]
        s.far_down = send(block, block, s.p1(3))
        spread_out(s, 3)
        spread_out(s, 1)
    for d in (2, 1, 3):
        s_copies[d].wait_recv()
        slot = s_all.at[((z - d) % 4) * 2 + c]
        s_copies[d + 4] = send(slot, slot, peer(dc=1))
    for s in (a, b):
        s.far_up.wait_recv()
        s.far_down.wait_recv()
        spread_out(s, 2)
    s_own.wait_recv()
    for s in (a, b):
        s.far = {}
        for d in (0, 3):
            s.second[d][1].wait_recv()
            block = s.w.at[at2(s, 3), at1(s, d)]
            s.far[d] = send(block, block, s.p2(1))
        for d in (1, 2):
            s.second[d][3].wait_recv()
            block = s.w.at[at2(s, 1), at1(s, d)]
            s.far[d] = send(block, block, s.p2(3))
    for d in (2, 1, 3):
        t_copies[d].wait_recv()
        slot = t_all.at[((z - d) % 4) * 2 + c]
        t_copies[d + 4] = send(slot, slot, peer(dc=1))
        s_copies[d + 4].wait_recv()
    t_own.wait_recv()
    for s in (a, b):
        for d in (0, 3):
            s.second[d][3].wait_recv()
        for d in (1, 2):
            s.second[d][1].wait_recv()
        for d in range(4):
            s.far[d].wait_recv()

    def square_rows(i, total):
        block = wb[i // 4, i % 4].astype(F32)
        return total + jnp.sum((block * block).reshape(HP // 8, 8, CP), axis=0)

    norm_row[0] = lax.fori_loop(0, 16, square_rows, jnp.zeros((8, CP), F32))
    n_copy = send(norm_row.at[0], norm_in, peer(dc=1))

    def first_matmul(i, _):
        slab = wa[i].reshape(4 * HP, CP)
        pre[pl.ds(i * 4, 4)] = dot(slab, s_all[...].reshape(CP, PIX), NN).reshape(4, HP, PIX)
        return 0

    lax.fori_loop(0, 4, first_matmul, 0)

    def activate(i, _):
        block = wa[i // 4, i % 4].astype(F32)
        squares = jnp.sum(block * block, axis=1, keepdims=True)
        inv = jnp.broadcast_to(lax.rsqrt(squares + 1.0), (HP, PIX))
        value = pre[i] * inv
        pre[i] = value
        hidden = value * jax.nn.sigmoid(value) * SILU_GAIN * gain[i]
        hid[(i % 4) * 4 + i // 4] = hidden.astype(BF16)
        return 0

    lax.fori_loop(0, 16, activate, 0)

    def second_matmul(i, _):
        for part in range(2):
            cols = slice(part * 768, min(CP, (part + 1) * 768))
            value = dot(
                wb[i, :, :, cols].reshape(4 * HP, -1), hid[pl.ds(i * 4, 4)].reshape(4 * HP, PIX), TN
            )
            @pl.when(i == 0)
            def _():
                raw2[cols, :] = value
            @pl.when(i > 0)
            def _():
                raw2[cols, :] += value
        return 0

    lax.fori_loop(0, 4, second_matmul, 0)
    raw_copy = send(raw2, raw2_in, peer(dc=1))

    n_copy.wait_recv()
    norm = jnp.sum(norm_row[0] + norm_in[...], axis=0, keepdims=True)
    inv_row = lax.rsqrt(norm + 1.0)
    norm_row[1] = jnp.broadcast_to(inv_row, (8, CP))
    raw_copy.wait_recv()
    for d in (2, 1, 3):
        t_copies[d + 4].wait_recv()

    dot_row = jnp.zeros((16, CP), F32)
    for q in range(CP // 128):
        rows = pl.ds(q * 128, 128)
        inv_col = jnp.broadcast_to(inv_row[:, q * 128 : (q + 1) * 128], (128, 128)).T
        inv_col = jnp.concatenate([inv_col, inv_col], axis=1)
        total = raw2[rows, :] + raw2_in[rows, :]
        state = s_all[...].reshape(CP, PIX)[q * 128 : (q + 1) * 128].astype(F32)
        target = t_all[...].reshape(CP, PIX)[q * 128 : (q + 1) * 128].astype(F32)
        grad = (KEEP_COEF * state + ADD_COEF * (total * inv_col) - target) / SAMPLES
        dbranch = (ADD_COEF * grad).astype(BF16)
        dbr[rows, :] = dbranch
        wide = dbranch.astype(F32)
        dbn[rows, :] = (wide * inv_col).astype(BF16)
        raw2_in[rows, :] = wide * total
    dot_row = dot(jnp.ones((16, PIX), BF16), raw2_in[...].astype(BF16), NT)[0:1]
    dot_high = dot_row.astype(BF16).astype(F32)
    dot_low = dot_row - dot_high

    row = lax.broadcasted_iota(jnp.int32, (HP, 1), 0)

    def second_grad(i, _):
        value = dot(hid[pl.ds(i * 4, 4)].reshape(4 * HP, PIX), dbr[...], NT)
        for j in range(4):
            block = value[j * HP : (j + 1) * HP]
            block = jnp.where(row == HALF, dot_high, block)
            block = jnp.where(row == HALF + 1, dot_low, block)
            gb[i, j] = block.astype(BF16)
        return 0

    def first_grad(i, _):
        value = dot(dpre[pl.ds(i * 4, 4)].reshape(4 * HP, PIX), s_all[...].reshape(CP, PIX), NT)
        ga[i] = value.reshape(4, HP, CP).astype(BF16)
        return 0

    def hidden_grad(i, _):
        dh[pl.ds(i * 4, 4)] = dot(wb[i].reshape(4 * HP, CP), dbn[...], NN).reshape(4, HP, PIX)
        return 0

    def activate_grad(i, _):
        value = pre[i]
        sig = jax.nn.sigmoid(value)
        slope = sig * (1.0 + value * (1.0 - sig))
        grad = dh[(i % 4) * 4 + i // 4]
        dpre[i] = (grad * gain[i] * slope * SILU_GAIN).astype(BF16)
        return 0

    def scatter_far(s):
        s.got_half = {}
        for n, d in enumerate((0, 1)):
            s.got_half[d] = send(s.g.at[at2(s, 2), at1(s, d)], s.half2.at[n], s.p2(1))
        for n, d in enumerate((2, 3)):
            s.got_half[d] = send(s.g.at[at2(s, 2), at1(s, d)], s.half2.at[2 + n], s.p2(3))

    def scatter_near(s):
        s.got_full = {}
        for d in (2, 3):
            s.got_full[0, d] = send(s.g.at[at2(s, 1), at1(s, d)], s.full2.at[0, d], s.p2(1))
        for d in (0, 1):
            s.got_full[1, d] = send(s.g.at[at2(s, 3), at1(s, d)], s.full2.at[1, d], s.p2(3))

    def scatter_relay(s):
        for n, d in enumerate((0, 1, 2, 3)):
            s.got_half[d].wait_recv()
            up = d < 2
            spot = (at2(s, 1 if up else 3), at1(s, d))
            s.g[spot] = (s.g[spot].astype(F32) + s.half2[n].astype(F32)).astype(BF16)
            way = 0 if up else 1
            s.got_full[way, d] = send(
                s.g.at[spot[0], spot[1]], s.full2.at[way, d], s.p2(1 if up else 3)
            )

    def scatter_sum(s, d):
        s.got_full[0, d].wait_recv()
        s.got_full[1, d].wait_recv()
        spot = (s.i2, at1(s, d))
        total = (
            s.g[spot].astype(F32) + s.full2[0, d].astype(F32) + s.full2[1, d].astype(F32)
        )
        if d == 0:
            s.own = total
        s.g[spot] = total.astype(BF16)

    def ring_far(s):
        spot = s.g.at[s.i2, at1(s, 2)]
        low, high = pl.ds(0, s.cut), pl.ds(s.cut, HP - s.cut)
        s.far_up = send(spot.at[low], s.half1.at[low], s.p1(1))
        s.far_down = send(spot.at[high], s.half1.at[high], s.p1(3))

    def ring_near(s):
        low, high = pl.ds(0, s.cut), pl.ds(s.cut, HP - s.cut)
        s.near = [
            send(s.g.at[s.i2, at1(s, 1), high], s.full1.at[0, high], s.p1(1)),
            send(s.g.at[s.i2, at1(s, 3), low], s.full1.at[1, low], s.p1(3)),
        ]

    def ring_relay(s):
        low, high = slice(0, s.cut), slice(s.cut, HP)
        for copy, part, d, way in ((s.far_up, low, 1, 0), (s.far_down, high, 3, 1)):
            copy.wait_recv()
            at = at1(s, d)
            s.g[s.i2, at, part] = (
                s.g[s.i2, at, part].astype(F32) + s.half1[part].astype(F32)
            ).astype(BF16)
            rows = pl.ds(part.start, part.stop - part.start)
            s.near.append(send(s.g.at[s.i2, at, rows], s.full1.at[way, rows], s.p1(d)))

    def ring_sum(s):
        for copy in s.near:
            copy.wait_recv()
        return s.own + s.full1[0].astype(F32) + s.full1[1].astype(F32)

    lax.fori_loop(0, 4, second_grad, 0)
    scatter_far(b)
    scatter_near(b)
    lax.fori_loop(0, 4, hidden_grad, 0)
    lax.fori_loop(0, 16, activate_grad, 0)
    lax.fori_loop(0, 4, first_grad, 0)
    scatter_far(a)
    scatter_near(a)
    scatter_relay(b)
    scatter_relay(a)
    for s in (b, a):
        scatter_sum(s, 2)
        ring_far(s)
        scatter_sum(s, 1)
        scatter_sum(s, 3)
        ring_near(s)
        scatter_sum(s, 0)
    ring_relay(b)
    ring_relay(a)
    grad2 = ring_sum(b)
    grad1 = ring_sum(a)

    w1 = wa[y, x].astype(F32)
    inv1 = lax.rsqrt(jnp.sum(w1 * w1, axis=1, keepdims=True) + 1.0)
    dot1 = jnp.sum(w1 * grad1, axis=1, keepdims=True)
    out1 = grad1 * inv1 - w1 * (dot1 * inv1 * inv1 * inv1)
    w2 = wb[x, y].astype(F32)
    inv2 = norm_row[1][0:1]
    dot2 = grad2[HALF : HALF + 1] + grad2[HALF + 1 : HALF + 2]
    out2 = grad2 * inv2 - w2 * (dot2 * inv2 * inv2 * inv2)
    fill = jnp.zeros((HP, PACK - 2 * CHAN_PAD), F32)
    for q in range(ROWS):
        cols = slice(q * CHAN_PAD, (q + 1) * CHAN_PAD)
        zs[q] = jnp.concatenate([out1[:, cols], out2[:, cols], fill], axis=1).astype(BF16)
    z_copies = [
        send(zs.at[((z + dz) % 4) * 2 + (c + dc) % 2], zr.at[r], peer(dz=dz, dc=dc))
        for dz, dc in group
    ]
    zr[r] = zs[r]
    for copy in z_copies:
        copy.wait_recv()
    for core in range(2):
        out[core] = sum(zr[2 * q + core].astype(F32) for q in range(4))
    for copy in started:
        copy.wait_send()


def local(clean, noise, bucket, mod_table, w_first, w_second):
    def halves(w):
        w = w.reshape(2, HALF, CHAN)
        return jnp.pad(w, ((0, 0), (0, HP - HALF), (0, CHAN_PAD - CHAN)))

    packed = jnp.concatenate([halves(w_first[0].T), halves(w_second[0])], axis=2)
    packed = jnp.pad(packed, ((0, 0), (0, 0), (0, PACK - 2 * CHAN_PAD))).astype(BF16)
    mod = jnp.pad(mod_table[0], ((0, 0), (0, CP - WIDTH)))
    vmem = pl.BlockSpec(memory_space=pltpu.VMEM)
    smem = pl.BlockSpec(memory_space=pltpu.SMEM)
    block = (HP, CP)
    result = pl.pallas_call(
        kernel,
        out_shape=jax.ShapeDtypeStruct((2, HP, PACK), F32),
        in_specs=[vmem, vmem, smem, vmem, vmem],
        out_specs=vmem,
        scratch_shapes=[
            pltpu.VMEM((4, CHAN_PAD, PIX), BF16),
            pltpu.VMEM((4, CHAN_PAD, PIX), BF16),
            pltpu.VMEM((ROWS, CHAN_PAD, PIX), BF16),
            pltpu.VMEM((ROWS, CHAN_PAD, PIX), BF16),
            pltpu.VMEM((ROWS, HP, PACK), BF16),
            pltpu.VMEM((4, 4, *block), BF16),
            pltpu.VMEM((4, 4, *block), BF16),
            pltpu.VMEM((4, 4, *block), BF16),
            pltpu.VMEM((4, 4, *block), BF16),
            pltpu.VMEM((4, *block), BF16),
            pltpu.VMEM((2, 4, *block), BF16),
            pltpu.VMEM(block, BF16),
            pltpu.VMEM((2, *block), BF16),
            pltpu.VMEM((4, *block), BF16),
            pltpu.VMEM((2, 4, *block), BF16),
            pltpu.VMEM(block, BF16),
            pltpu.VMEM((2, *block), BF16),
            pltpu.VMEM((16, HP, PIX), F32),
            pltpu.VMEM((16, HP, PIX), F32),
            pltpu.VMEM((16, HP, PIX), F32),
            pltpu.VMEM((16, HP, PIX), BF16),
            pltpu.VMEM((16, HP, PIX), BF16),
            pltpu.VMEM((CP, PIX), F32),
            pltpu.VMEM((CP, PIX), F32),
            pltpu.VMEM((2, 8, CP), F32),
            pltpu.VMEM((8, CP), F32),
            pltpu.VMEM((CP, PIX), BF16),
            pltpu.VMEM((CP, PIX), BF16),
            pltpu.VMEM((16, HP, PIX), F32),
            pltpu.VMEM((ROWS, HP, PACK), BF16),
            pltpu.VMEM((ROWS, HP, PACK), BF16),
            pltpu.SemaphoreType.DMA((MAX_COPIES,)),
            pltpu.SemaphoreType.DMA((MAX_COPIES,)),
        ],
        compiler_params=pltpu.CompilerParams(
            collective_id=0, has_side_effects=True, vmem_limit_bytes=60 * 1024 * 1024
        ),
    )(clean, noise, bucket, mod, packed)
    part = result[:, :HALF]
    first = part[:, :, :CHAN].reshape(BLOCK, CHAN).T
    second = part[:, :, CHAN_PAD : CHAN_PAD + CHAN].reshape(BLOCK, CHAN)
    return first[None], second[None]


def solution(mesh):
    in_specs = (
        P("row", "col"),
        P("row", "col"),
        P(),
        P(),
        P(None, "row", "col"),
        P(None, "col", "row"),
    )
    out_specs = (P(None, "row", "col"), P(None, "col", "row"))
    return jax.shard_map(local, mesh=mesh, in_specs=in_specs, out_specs=out_specs, check_vma=False)
```

```python
import math

import jax
import jax.numpy as jnp
from jax import lax
from jax.experimental import pallas as pl
from jax.experimental.pallas import tpu as pltpu
from jax.sharding import PartitionSpec as P

MESH = pl.DeviceIdType.MESH
F32 = jnp.float32
BF16 = jnp.bfloat16

WIDTH = 1344
PIX = 256
SAMPLES = 64
BUCKETS = 32
MIX_WEIGHT = 0.3
KEEP_COEF = (1.0 - MIX_WEIGHT) / math.sqrt((1.0 - MIX_WEIGHT) ** 2 + MIX_WEIGHT**2)
ADD_COEF = MIX_WEIGHT / math.sqrt((1.0 - MIX_WEIGHT) ** 2 + MIX_WEIGHT**2)
SILU_GAIN = 1.0 / 0.596

ROWS = 8
CHAN = WIDTH // ROWS
CHAN_PAD = 176
CP = ROWS * CHAN_PAD
BLOCK = WIDTH // 16
HALF = BLOCK // 2
HP = 48
HT = 16 * HP
WP = 256
CUTS = ((0, 768), (768, 1408))
NN = (((1,), (0,)), ((), ()))
NT = (((1,), (1,)), ((), ()))
TN = (((0,), (0,)), ((), ()))
MAX_COPIES = 160


def dot(a, b, dims):
    return lax.dot_general(a, b, dims, preferred_element_type=F32)


def kernel(
    clean_hbm, noise_hbm, bucket, mod_hbm, w1_hbm, w2_hbm, out1, out2,
    clean, noise, mod, w1_in, w2_in, w1_out, w2_out, w1_got, w2_got,
    st, tg, s_all, t_all, s_tok, t_tok, wa, wb, ga, gb,
    ra1, ra2, rx1, rx2, rb1, rb2, ry1, ry2,
    gain, pre, hid, dpre, raw, raw_out, raw_in, norm_row, norm_in,
    dbr, dbn, dot_rows, dh, zs1, zs2, zr1, zr2, load_sems, send_sems, recv_sems,
):
    r = lax.axis_index("row")
    k = lax.axis_index("col")
    z, c = r // 2, r % 2
    y, x = k // 4, k % 4

    def peer(dz=0, dc=0, dy=0, dx=0):
        return (
            ((z + dz) % 4) * 2 + (c + dc) % 2,
            ((y + dy) % 4) * 4 + (x + dx) % 4,
        )

    started = []

    def send(src, dst, device):
        i = len(started)
        copy = pltpu.make_async_remote_copy(
            src_ref=src,
            dst_ref=dst,
            send_sem=send_sems.at[i],
            recv_sem=recv_sems.at[i],
            device_id=device,
            device_id_type=MESH,
        )
        copy.start()
        started.append(copy)
        return copy

    group = [(dz, dc) for dz in (1, 3, 2, 0) for dc in (0, 1) if (dz, dc) != (0, 0)]
    barrier = pltpu.get_barrier_semaphore()
    near = [peer(dz=dz, dc=dc) for dz, dc in group]
    near += [peer(dx=1), peer(dx=3), peer(dy=1), peer(dy=3)]
    for device in near:
        pl.semaphore_signal(barrier, inc=1, device_id=device, device_id_type=MESH)

    loads = [
        pltpu.make_async_copy(src, dst, load_sems.at[i])
        for i, (src, dst) in enumerate(
            (
                (w1_hbm.at[0], w1_in),
                (w2_hbm.at[0], w2_in),
                (clean_hbm, clean),
                (noise_hbm, noise),
                (mod_hbm.at[0], mod),
            )
        )
    ]
    for load in loads:
        load.start()

    loads[0].wait()
    loads[1].wait()
    hid_of = lax.broadcasted_iota(jnp.int32, (HP, BLOCK), 0)
    col_of = lax.broadcasted_iota(jnp.int32, (HP, BLOCK), 1)
    w1_bf = w1_in[...].astype(BF16)
    w2_bf = w2_in[...].astype(BF16)
    for core in range(2):
        pick = (col_of == hid_of + HALF * core) & (hid_of < HALF)
        pick = jnp.where(pick, 1.0, 0.0).astype(BF16)
        fill = jnp.zeros((HP, WP - CHAN), F32)
        w1_out[core] = jnp.concatenate([dot(pick, w1_bf, NT), fill], axis=1).astype(BF16)
        w2_out[core] = jnp.concatenate([dot(pick, w2_bf, NN), fill], axis=1).astype(BF16)
    w1_got[r] = w1_out[c]
    w2_got[r] = w2_out[c]

    def state_piece(d):
        zq = (z + d) % 4
        level_of = jnp.full((1, PIX), bucket[k * 4 + zq], jnp.int32).astype(F32)
        level = jnp.exp(-3.0 + 5.0 * (level_of + 0.5) / BUCKETS)
        spread = jnp.sqrt(level * level + 0.25)
        cols = pl.ds(pl.multiple_of(zq * PIX, PIX), PIX)
        cl = clean[:, cols]
        no = noise[:, cols]
        pad = jnp.zeros((CHAN_PAD - CHAN, PIX), F32)
        state = (cl + level * no) / spread
        target = cl * (2.0 * level / spread) - no * (0.5 / spread)
        return (
            jnp.concatenate([state, pad], axis=0).astype(BF16),
            jnp.concatenate([target, pad], axis=0).astype(BF16),
        )

    loads[2].wait()
    loads[3].wait()
    loads[4].wait()
    for d in range(4):
        state, target = state_piece(d)
        st[d] = state
        tg[d] = target
    s_all[r] = st[0]
    t_all[r] = tg[0]

    pl.semaphore_wait(barrier, len(near))

    w1_copies = [
        send(w1_out.at[(c + dc) % 2], w1_got.at[r], peer(dz=dz, dc=dc)) for dz, dc in group
    ]
    w2_copies = [
        send(w2_out.at[(c + dc) % 2], w2_got.at[r], peer(dz=dz, dc=dc)) for dz, dc in group
    ]
    s_copies = {d: send(st.at[d], s_all.at[r], peer(dz=d)) for d in (2, 1, 3)}
    s_own = send(st.at[0], s_all.at[r], peer(dc=1))
    t_copies = {d: send(tg.at[d], t_all.at[r], peer(dz=d)) for d in (2, 1, 3)}
    t_own = send(tg.at[0], t_all.at[r], peer(dc=1))

    sample = k * 4 + z
    picked = lax.broadcasted_iota(jnp.int32, (BUCKETS, WIDTH), 0) == bucket[sample]
    mod_row = jnp.sum(jnp.where(picked, 1.0 + mod[...], 0.0), axis=0, keepdims=True)
    mod_row = jnp.concatenate([mod_row, jnp.zeros((1, CP - WIDTH), F32)], axis=1)
    for b in range(16):
        first = (BLOCK * b // 128) * 128
        lane = lax.broadcasted_iota(jnp.int32, (HP, 256), 1) + first
        row = lax.broadcasted_iota(jnp.int32, (HP, 256), 0)
        take = (lane == row + (BLOCK * b + HALF * c)) & (row < HALF)
        window = jnp.broadcast_to(mod_row[:, first : first + 256], (HP, 256))
        value = jnp.sum(jnp.where(take, window, 0.0), axis=1, keepdims=True)
        gain[b] = jnp.broadcast_to(value, (HP, PIX))

    class Side:
        pass

    def side_a():
        s = Side()
        s.w, s.g, s.i1, s.i2 = wa, ga, x, y
        s.p1 = lambda d: peer(dx=d)
        s.p2 = lambda d: peer(dy=d)
        s.cut = 32
        s.half1, s.half2, s.full1, s.full2 = rx1, ra1, rx2, ra2
        return s

    def side_b():
        s = Side()
        s.w, s.g, s.i1, s.i2 = wb, gb, y, x
        s.p1 = lambda d: peer(dy=d)
        s.p2 = lambda d: peer(dx=d)
        s.cut = 16
        s.half1, s.half2, s.full1, s.full2 = ry1, rb1, ry2, rb2
        return s

    a, b = side_a(), side_b()

    def at1(s, d):
        return (s.i1 + d) % 4

    def at2(s, d):
        return (s.i2 + d) % 4

    def spread_out(s, d):
        block = s.w.at[s.i2, at1(s, d)]
        s.second[d] = {e: send(block, block, s.p2(e)) for e in (1, 3)}

    for s, copies, got in ((a, w1_copies, w1_got), (b, w2_copies, w2_got)):
        for copy in copies:
            copy.wait_recv()
        s.w[s.i2, s.i1] = jnp.concatenate(
            [got[q][:, :CHAN_PAD].astype(F32) for q in range(ROWS)], axis=1
        ).astype(BF16)
        block = s.w.at[s.i2, s.i1]
        s.first = {d: send(block, block, s.p1(d)) for d in (1, 3)}
        s.second = {}
        spread_out(s, 0)

    for s in (a, b):
        s.first[1].wait_recv()
        block = s.w.at[s.i2, at1(s, 3), pl.ds(0, s.cut)]
        s.far_up = send(block, block, s.p1(1))
        s.first[3].wait_recv()
        block = s.w.at[s.i2, at1(s, 1), pl.ds(s.cut, HP - s.cut)]
        s.far_down = send(block, block, s.p1(3))
        spread_out(s, 3)
        spread_out(s, 1)
    for d in (2, 1, 3):
        s_copies[d].wait_recv()
        slot = s_all.at[((z - d) % 4) * 2 + c]
        s_copies[d + 4] = send(slot, slot, peer(dc=1))
    for s in (a, b):
        s.far_up.wait_recv()
        s.far_down.wait_recv()
        spread_out(s, 2)
        s.far = {}
    s_own.wait_recv()
    for d in (2, 1, 3):
        s_copies[d + 4].wait_recv()

    def first_half(slab):
        weights = wa[slab].reshape(4 * HP, CP)
        value = dot(weights, s_all[...].reshape(CP, PIX), NN).reshape(4, HP, PIX)
        for j in range(4):
            block = wa[slab, j].astype(F32)
            squares = jnp.sum(block * block, axis=1, keepdims=True)
            inv = jnp.broadcast_to(lax.rsqrt(squares + 1.0), (HP, PIX))
            act = value[j] * inv
            pre[slab * 4 + j] = act
            hidden = act * jax.nn.sigmoid(act) * SILU_GAIN * gain[slab * 4 + j]
            hid[j * 4 + slab] = hidden.astype(BF16)

    first_half(y)
    s_tok[...] = s_all[...].reshape(CP, PIX).T

    def pass_on(s, d, up):
        if up:
            s.second[d][1].wait_recv()
            block = s.w.at[at2(s, 3), at1(s, d)]
            s.far[d] = send(block, block, s.p2(1))
        else:
            s.second[d][3].wait_recv()
            block = s.w.at[at2(s, 1), at1(s, d)]
            s.far[d] = send(block, block, s.p2(3))

    for d, up in ((0, True), (3, False), (1, True), (2, False)):
        pass_on(a, d, up)
        pass_on(b, d, up)
    for d in (2, 1, 3):
        t_copies[d].wait_recv()
        slot = t_all.at[((z - d) % 4) * 2 + c]
        t_copies[d + 4] = send(slot, slot, peer(dc=1))

    def squares_of(slab):
        total = jnp.zeros((8, CP), F32)
        for j in range(4):
            block = wb[slab, j].astype(F32)
            total = total + jnp.sum((block * block).reshape(HP // 8, 8, CP), axis=0)
        return total

    for d in (3, 2):
        a.second[d][1].wait_recv()
    first_half(at2(a, 3))
    for d in (0, 1):
        a.second[d][3].wait_recv()
    first_half(at2(a, 1))
    t_own.wait_recv()
    for d in (2, 1, 3):
        t_copies[d + 4].wait_recv()
    t_tok[...] = t_all[...].reshape(CP, PIX).T
    for d in (3, 2):
        b.second[d][1].wait_recv()
    for d in (0, 1):
        b.second[d][3].wait_recv()
    squares = squares_of(x) + squares_of(at2(b, 1)) + squares_of(at2(b, 3))
    for d in (0, 3, 1, 2):
        a.far[d].wait_recv()
    first_half(at2(a, 2))
    for d in (0, 3, 1, 2):
        b.far[d].wait_recv()
    norm_row[0] = squares + squares_of(at2(b, 2))
    n_copy = send(norm_row.at[0], norm_in, peer(dc=1))

    raw_copies = []
    for low, high in CUTS:
        cols = slice(low, high)
        value = dot(
            hid[...].reshape(HT, PIX), wb[:, :, :, cols].reshape(HT, high - low), TN
        )
        raw[:, cols] = value
        raw_out[:, cols] = value.astype(BF16)
        part = pl.ds(low, high - low)
        raw_copies.append(send(raw_out.at[:, part], raw_in.at[:, part], peer(dc=1)))

    n_copy.wait_recv()
    norm = jnp.sum(norm_row[0] + norm_in[...], axis=0, keepdims=True)
    inv_row = lax.rsqrt(norm + 1.0)
    norm_row[1] = jnp.broadcast_to(inv_row, (8, CP))
    for copy, (low, high) in zip(raw_copies, CUTS):
        copy.wait_recv()
        cols = slice(low, high)
        sums = jnp.zeros((8, high - low), F32)
        inv = norm_row[1][0:1, cols]
        for q in range(8):
            rows = slice(q * 32, (q + 1) * 32)
            total = raw[rows, cols] + raw_in[rows, cols].astype(F32)
            state = s_tok[rows, cols].astype(F32)
            target = t_tok[rows, cols].astype(F32)
            grad = KEEP_COEF * state + ADD_COEF * (total * inv) - target
            dbranch = (ADD_COEF / SAMPLES * grad).astype(BF16)
            dbr[rows, cols] = dbranch
            wide = dbranch.astype(F32)
            dbn[rows, cols] = (wide * inv).astype(BF16)
            sums = sums + jnp.sum((wide * total).reshape(4, 8, high - low), axis=0)
        dot_rows[:, cols] = jnp.broadcast_to(
            jnp.sum(sums, axis=0, keepdims=True), (8, high - low)
        )
    dot_high = dot_rows[0:1].astype(BF16).astype(F32)
    dot_low = dot_rows[0:1] - dot_high
    row = lax.broadcasted_iota(jnp.int32, (HP, 1), 0)

    def second_grad(slab):
        value = dot(hid[pl.ds(slab * 4, 4)].reshape(4 * HP, PIX), dbr[...], NN)
        for j in range(4):
            block = value[j * HP : (j + 1) * HP]
            block = jnp.where(row == HALF, dot_high, block)
            block = jnp.where(row == HALF + 1, dot_low, block)
            gb[slab, j] = block.astype(BF16)

    def first_grad(slab):
        for j in range(4):
            value = pre[slab * 4 + j]
            sig = jax.nn.sigmoid(value)
            slope = sig * (1.0 + value * (1.0 - sig))
            grad = dh[j * 4 + slab]
            dpre[j] = (grad * gain[slab * 4 + j] * slope * SILU_GAIN).astype(BF16)
        value = dot(dpre[...].reshape(4 * HP, PIX), s_tok[...], NN)
        ga[slab] = value.reshape(4, HP, CP).astype(BF16)

    def hidden_grad(i, _):
        dh[pl.ds(i * 4, 4)] = dot(wb[i].reshape(4 * HP, CP), dbn[...], NT).reshape(4, HP, PIX)
        return 0

    def scatter_far(s, d):
        s.got_half[d] = send(
            s.g.at[at2(s, 2), at1(s, d)], s.half2.at[d], s.p2(1 if d < 2 else 3)
        )

    def scatter_near(s, d):
        way, e = (1, 3) if d < 2 else (0, 1)
        s.got_full[way, d] = send(
            s.g.at[at2(s, e), at1(s, d)], s.full2.at[way, d], s.p2(e)
        )

    def scatter_relay(s, d):
        s.got_half[d].wait_recv()
        way, e = (0, 1) if d < 2 else (1, 3)
        spot = (at2(s, e), at1(s, d))
        s.g[spot] = (s.g[spot].astype(F32) + s.half2[d].astype(F32)).astype(BF16)
        s.got_full[way, d] = send(s.g.at[spot[0], spot[1]], s.full2.at[way, d], s.p2(e))

    def scatter_sum(s, d):
        s.got_full[0, d].wait_recv()
        s.got_full[1, d].wait_recv()
        spot = (s.i2, at1(s, d))
        total = (
            s.g[spot].astype(F32) + s.full2[0, d].astype(F32) + s.full2[1, d].astype(F32)
        )
        if d == 0:
            s.own = total
        else:
            s.g[spot] = total.astype(BF16)

    def ring_far(s):
        spot = s.g.at[s.i2, at1(s, 2)]
        low, high = pl.ds(0, s.cut), pl.ds(s.cut, HP - s.cut)
        s.far_up = send(spot.at[low], s.half1.at[low], s.p1(1))
        s.far_down = send(spot.at[high], s.half1.at[high], s.p1(3))
        s.near = []

    def ring_near(s, d):
        low, high = pl.ds(0, s.cut), pl.ds(s.cut, HP - s.cut)
        part, way = (high, 0) if d == 1 else (low, 1)
        s.near.append(send(s.g.at[s.i2, at1(s, d), part], s.full1.at[way, part], s.p1(d)))

    def ring_relay(s, d):
        part, way, copy = (
            (slice(0, s.cut), 0, s.far_up) if d == 1 else (slice(s.cut, HP), 1, s.far_down)
        )
        copy.wait_recv()
        at = at1(s, d)
        s.g[s.i2, at, part] = (
            s.g[s.i2, at, part].astype(F32) + s.half1[part].astype(F32)
        ).astype(BF16)
        rows = pl.ds(part.start, part.stop - part.start)
        s.near.append(send(s.g.at[s.i2, at, rows], s.full1.at[way, rows], s.p1(d)))

    def ring_sum(s):
        for copy in s.near:
            copy.wait_recv()
        return s.own + s.full1[0].astype(F32) + s.full1[1].astype(F32)

    def start(s, grad):
        s.got_half, s.got_full = {}, {}
        grad(at2(s, 2))
        scatter_far(s, 1)
        scatter_far(s, 2)
        grad(at2(s, 1))
        scatter_near(s, 2)
        grad(at2(s, 3))
        scatter_near(s, 1)
        scatter_far(s, 0)
        scatter_far(s, 3)

    start(b, second_grad)
    lax.fori_loop(0, 4, hidden_grad, 0)
    start(a, first_grad)
    for d in (1, 2, 0, 3):
        scatter_relay(b, d)
    scatter_near(b, 3)
    scatter_near(b, 0)
    second_grad(x)
    first_grad(y)
    for d in (1, 2, 0, 3):
        scatter_relay(a, d)
    scatter_near(a, 3)
    scatter_near(a, 0)
    for s in (b, a):
        scatter_sum(s, 2)
        ring_far(s)
        scatter_sum(s, 1)
        ring_near(s, 1)
        ring_relay(s, 1)
    for s in (b, a):
        scatter_sum(s, 3)
        ring_near(s, 3)
        ring_relay(s, 3)
        scatter_sum(s, 0)

    def hand_out(out, zs, zr):
        for q in range(ROWS):
            cols = slice(q * CHAN_PAD, (q + 1) * CHAN_PAD)
            fill = jnp.zeros((HP, WP - CHAN_PAD), F32)
            zs[q] = jnp.concatenate([out[:, cols], fill], axis=1).astype(BF16)
        zr[r] = zs[r]
        return [
            send(zs.at[((z + dz) % 4) * 2 + (c + dc) % 2], zr.at[r], peer(dz=dz, dc=dc))
            for dz, dc in group
        ]

    grad2 = ring_sum(b)
    w2 = wb[x, y].astype(F32)
    inv2 = norm_row[1][0:1]
    dot2 = grad2[HALF : HALF + 1] + grad2[HALF + 1 : HALF + 2]
    z2_copies = hand_out(grad2 * inv2 - w2 * (dot2 * inv2 * inv2 * inv2), zs2, zr2)
    grad1 = ring_sum(a)
    w1 = wa[y, x].astype(F32)
    inv1 = lax.rsqrt(jnp.sum(w1 * w1, axis=1, keepdims=True) + 1.0)
    dot1 = jnp.sum(w1 * grad1, axis=1, keepdims=True)
    z1_copies = hand_out(grad1 * inv1 - w1 * (dot1 * inv1 * inv1 * inv1), zs1, zr1)

    for copy in z2_copies:
        copy.wait_recv()
    for core in range(2):
        value = sum(zr2[2 * q + core].astype(F32) for q in range(4))
        out2[0, core * HALF : (core + 1) * HALF, :] = value[:HALF, :CHAN]
    for copy in z1_copies:
        copy.wait_recv()
    for core in range(2):
        value = sum(zr1[2 * q + core].astype(F32) for q in range(4))
        value = jnp.concatenate([value, jnp.zeros((128 - HP, WP), F32)], axis=0).T
        out1[0, :, core * HALF : (core + 1) * HALF] = value[:CHAN, :HALF]
    for copy in started:
        copy.wait_send()


def local(clean, noise, bucket, mod_table, w_first, w_second):
    vmem = pl.BlockSpec(memory_space=pltpu.VMEM)
    smem = pl.BlockSpec(memory_space=pltpu.SMEM)
    hbm = pl.BlockSpec(memory_space=pl.ANY)
    block = (HP, CP)
    return pl.pallas_call(
        kernel,
        out_shape=(
            jax.ShapeDtypeStruct((1, CHAN, BLOCK), F32),
            jax.ShapeDtypeStruct((1, BLOCK, CHAN), F32),
        ),
        in_specs=[hbm, hbm, smem, hbm, hbm, hbm],
        out_specs=(vmem, vmem),
        scratch_shapes=[
            pltpu.VMEM(clean.shape, F32),
            pltpu.VMEM(noise.shape, F32),
            pltpu.VMEM((BUCKETS, WIDTH), F32),
            pltpu.VMEM((CHAN, BLOCK), F32),
            pltpu.VMEM((BLOCK, CHAN), F32),
            pltpu.VMEM((2, HP, WP), BF16),
            pltpu.VMEM((2, HP, WP), BF16),
            pltpu.VMEM((ROWS, HP, WP), BF16),
            pltpu.VMEM((ROWS, HP, WP), BF16),
            pltpu.VMEM((4, CHAN_PAD, PIX), BF16),
            pltpu.VMEM((4, CHAN_PAD, PIX), BF16),
            pltpu.VMEM((ROWS, CHAN_PAD, PIX), BF16),
            pltpu.VMEM((ROWS, CHAN_PAD, PIX), BF16),
            pltpu.VMEM((PIX, CP), BF16),
            pltpu.VMEM((PIX, CP), BF16),
            pltpu.VMEM((4, 4, *block), BF16),
            pltpu.VMEM((4, 4, *block), BF16),
            pltpu.VMEM((4, 4, *block), BF16),
            pltpu.VMEM((4, 4, *block), BF16),
            pltpu.VMEM((4, *block), BF16),
            pltpu.VMEM((2, 4, *block), BF16),
            pltpu.VMEM(block, BF16),
            pltpu.VMEM((2, *block), BF16),
            pltpu.VMEM((4, *block), BF16),
            pltpu.VMEM((2, 4, *block), BF16),
            pltpu.VMEM(block, BF16),
            pltpu.VMEM((2, *block), BF16),
            pltpu.VMEM((16, HP, PIX), F32),
            pltpu.VMEM((16, HP, PIX), F32),
            pltpu.VMEM((16, HP, PIX), BF16),
            pltpu.VMEM((4, HP, PIX), BF16),
            pltpu.VMEM((PIX, CP), F32),
            pltpu.VMEM((PIX, CP), BF16),
            pltpu.VMEM((PIX, CP), BF16),
            pltpu.VMEM((2, 8, CP), F32),
            pltpu.VMEM((8, CP), F32),
            pltpu.VMEM((PIX, CP), BF16),
            pltpu.VMEM((PIX, CP), BF16),
            pltpu.VMEM((8, CP), F32),
            pltpu.VMEM((16, HP, PIX), F32),
            pltpu.VMEM((ROWS, HP, WP), BF16),
            pltpu.VMEM((ROWS, HP, WP), BF16),
            pltpu.VMEM((ROWS, HP, WP), BF16),
            pltpu.VMEM((ROWS, HP, WP), BF16),
            pltpu.SemaphoreType.DMA((5,)),
            pltpu.SemaphoreType.DMA((MAX_COPIES,)),
            pltpu.SemaphoreType.DMA((MAX_COPIES,)),
        ],
        compiler_params=pltpu.CompilerParams(
            collective_id=0, has_side_effects=True, vmem_limit_bytes=60 * 1024 * 1024
        ),
    )(clean, noise, bucket, mod_table, w_first, w_second)


def solution(mesh):
    in_specs = (
        P("row", "col"),
        P("row", "col"),
        P(),
        P(),
        P(None, "row", "col"),
        P(None, "col", "row"),
    )
    out_specs = (P(None, "row", "col"), P(None, "col", "row"))
    return jax.shard_map(local, mesh=mesh, in_specs=in_specs, out_specs=out_specs, check_vma=False)
```

```python
import math

import jax
import jax.numpy as jnp
from jax import lax
from jax.experimental import pallas as pl
from jax.experimental.pallas import tpu as pltpu
from jax.sharding import PartitionSpec as P

MESH = pl.DeviceIdType.MESH
F32 = jnp.float32
BF16 = jnp.bfloat16

WIDTH = 1344
PIX = 256
SAMPLES = 64
BUCKETS = 32
MIX_WEIGHT = 0.3
KEEP_COEF = (1.0 - MIX_WEIGHT) / math.sqrt((1.0 - MIX_WEIGHT) ** 2 + MIX_WEIGHT**2)
ADD_COEF = MIX_WEIGHT / math.sqrt((1.0 - MIX_WEIGHT) ** 2 + MIX_WEIGHT**2)
SILU_GAIN = 1.0 / 0.596

ROWS = 8
CHAN = WIDTH // ROWS
CHAN_PAD = 176
CP = ROWS * CHAN_PAD
BLOCK = WIDTH // 16
HALF = BLOCK // 2
HP = 48
HT = 16 * HP
WP = 256
CUTS = ((0, 768), (768, 1408))
NN = (((1,), (0,)), ((), ()))
NT = (((1,), (1,)), ((), ()))
TN = (((0,), (0,)), ((), ()))
MAX_COPIES = 160
PLAN = (
    ("grad", "b", 2),
    ("hidden",),
    ("far", "b", 1),
    ("far", "b", 3),
    ("grad", "a", 2),
    ("far", "b", 2),
    ("far", "b", 0),
    ("far", "a", 1),
    ("far", "a", 2),
    ("far", "a", 3),
    ("grad", "b", 3),
    ("grad", "a", 3),
    ("grad", "b", 1),
    ("grad", "a", 1),
    ("near", "a", 3),
    ("near", "b", 3),
    ("relay", "b", 3),
    ("relay", "a", 2),
    ("near", "b", 2),
    ("grad", "a", 0),
    ("near", "a", 2),
    ("relay", "b", 2),
    ("relay", "a", 3),
    ("grad", "b", 0),
    ("near", "a", 1),
    ("near", "b", 1),
    ("far", "a", 0),
    ("relay", "b", 1),
    ("relay", "a", 1),
    ("sum", "b", 2),
    ("sum", "a", 2),
    ("ring_far", "a"),
    ("ring_far", "b"),
    ("near", "b", 0),
    ("near", "a", 0),
    ("relay", "b", 0),
    ("relay", "a", 0),
    ("sum", "b", 1),
    ("ring_near", "b", 1),
    ("sum", "b", 3),
    ("sum", "a", 1),
    ("ring_relay", "b", 1),
    ("sum", "a", 3),
    ("ring_near", "a", 1),
    ("ring_near", "a", 3),
    ("ring_near", "b", 3),
    ("ring_relay", "a", 3),
    ("ring_relay", "b", 3),
    ("ring_relay", "a", 1),
    ("sum", "a", 0),
    ("sum", "b", 0),
)


def dot(a, b, dims):
    return lax.dot_general(a, b, dims, preferred_element_type=F32)


def kernel(
    clean_hbm, noise_hbm, bucket, mod_hbm, w1_hbm, w2_hbm, out1, out2,
    clean, noise, mod, w1_in, w2_in, w1_out, w2_out, w1_got, w2_got,
    st, tg, s_all, t_all, s_tok, t_tok, wa, wb, ga, gb,
    ra1, ra2, rx1, rx2, rb1, rb2, ry1, ry2,
    gain, pre, hid, dpre, raw, raw_out, raw_in, norm_row, norm_in,
    dbr, dbn, dot_rows, dh, zs1, zs2, zr1, zr2, load_sems, send_sems, recv_sems,
):
    r = lax.axis_index("row")
    k = lax.axis_index("col")
    z, c = r // 2, r % 2
    y, x = k // 4, k % 4

    def peer(dz=0, dc=0, dy=0, dx=0):
        return (
            ((z + dz) % 4) * 2 + (c + dc) % 2,
            ((y + dy) % 4) * 4 + (x + dx) % 4,
        )

    started = []

    def send(src, dst, device):
        i = len(started)
        copy = pltpu.make_async_remote_copy(
            src_ref=src,
            dst_ref=dst,
            send_sem=send_sems.at[i],
            recv_sem=recv_sems.at[i],
            device_id=device,
            device_id_type=MESH,
        )
        copy.start()
        started.append(copy)
        return copy

    group = [(dz, dc) for dz in (1, 3, 2, 0) for dc in (0, 1) if (dz, dc) != (0, 0)]
    barrier = pltpu.get_barrier_semaphore()
    near = [peer(dz=dz, dc=dc) for dz, dc in group]
    near += [peer(dx=1), peer(dx=3), peer(dy=1), peer(dy=3)]
    for device in near:
        pl.semaphore_signal(barrier, inc=1, device_id=device, device_id_type=MESH)

    loads = [
        pltpu.make_async_copy(src, dst, load_sems.at[i])
        for i, (src, dst) in enumerate(
            (
                (w1_hbm.at[0], w1_in),
                (w2_hbm.at[:, 0], w2_in),
                (clean_hbm, clean),
                (noise_hbm, noise),
                (mod_hbm.at[0], mod),
            )
        )
    ]
    for load in loads:
        load.start()

    loads[0].wait()
    loads[1].wait()
    hid_of = lax.broadcasted_iota(jnp.int32, (HP, BLOCK), 0)
    col_of = lax.broadcasted_iota(jnp.int32, (HP, BLOCK), 1)
    w1_bf = w1_in[...].astype(BF16)
    w2_bf = w2_in[...].astype(BF16)
    for core in range(2):
        pick = (col_of == hid_of + HALF * core) & (hid_of < HALF)
        pick = jnp.where(pick, 1.0, 0.0).astype(BF16)
        fill = jnp.zeros((HP, WP - CHAN), F32)
        w1_out[core] = jnp.concatenate([dot(pick, w1_bf, NT), fill], axis=1).astype(BF16)
        w2_out[core] = jnp.concatenate([dot(pick, w2_bf, NN), fill], axis=1).astype(BF16)
    w1_got[r] = w1_out[c]
    w2_got[r] = w2_out[c]

    def state_piece(d):
        zq = (z + d) % 4
        level_of = jnp.full((1, PIX), bucket[k * 4 + zq], jnp.int32).astype(F32)
        level = jnp.exp(-3.0 + 5.0 * (level_of + 0.5) / BUCKETS)
        spread = jnp.sqrt(level * level + 0.25)
        cols = pl.ds(pl.multiple_of(zq * PIX, PIX), PIX)
        cl = clean[:, cols]
        no = noise[:, cols]
        pad = jnp.zeros((CHAN_PAD - CHAN, PIX), F32)
        state = (cl + level * no) / spread
        target = cl * (2.0 * level / spread) - no * (0.5 / spread)
        return (
            jnp.concatenate([state, pad], axis=0).astype(BF16),
            jnp.concatenate([target, pad], axis=0).astype(BF16),
        )

    pl.semaphore_wait(barrier, len(near))

    w1_copies = [
        send(w1_out.at[(c + dc) % 2], w1_got.at[r], peer(dz=dz, dc=dc)) for dz, dc in group
    ]
    w2_copies = [
        send(w2_out.at[(c + dc) % 2], w2_got.at[r], peer(dz=dz, dc=dc)) for dz, dc in group
    ]
    loads[2].wait()
    loads[3].wait()
    loads[4].wait()
    for d in range(4):
        state, target = state_piece(d)
        st[d] = state
        tg[d] = target
    s_all[r] = st[0]
    t_all[r] = tg[0]
    s_copies = {d: send(st.at[d], s_all.at[r], peer(dz=d)) for d in (2, 1, 3)}
    s_own = send(st.at[0], s_all.at[r], peer(dc=1))
    t_copies = {d: send(tg.at[d], t_all.at[r], peer(dz=d)) for d in (2, 1, 3)}
    t_own = send(tg.at[0], t_all.at[r], peer(dc=1))

    sample = k * 4 + z
    picked = lax.broadcasted_iota(jnp.int32, (BUCKETS, WIDTH), 0) == bucket[sample]
    mod_row = jnp.sum(jnp.where(picked, 1.0 + mod[...], 0.0), axis=0, keepdims=True)
    mod_row = jnp.concatenate([mod_row, jnp.zeros((1, CP - WIDTH), F32)], axis=1)
    for b in range(16):
        first = (BLOCK * b // 128) * 128
        lane = lax.broadcasted_iota(jnp.int32, (HP, 256), 1) + first
        row = lax.broadcasted_iota(jnp.int32, (HP, 256), 0)
        take = (lane == row + (BLOCK * b + HALF * c)) & (row < HALF)
        window = jnp.broadcast_to(mod_row[:, first : first + 256], (HP, 256))
        value = jnp.sum(jnp.where(take, window, 0.0), axis=1, keepdims=True)
        gain[b] = jnp.broadcast_to(value, (HP, PIX))

    class Side:
        pass

    def side_a():
        s = Side()
        s.w, s.g, s.i1, s.i2 = wa, ga, x, y
        s.p1 = lambda d: peer(dx=d)
        s.p2 = lambda d: peer(dy=d)
        s.cut = 32
        s.half1, s.half2, s.full1, s.full2 = rx1, ra1, rx2, ra2
        return s

    def side_b():
        s = Side()
        s.w, s.g, s.i1, s.i2 = wb, gb, y, x
        s.p1 = lambda d: peer(dy=d)
        s.p2 = lambda d: peer(dx=d)
        s.cut = 16
        s.half1, s.half2, s.full1, s.full2 = ry1, rb1, ry2, rb2
        return s

    a, b = side_a(), side_b()

    def at1(s, d):
        return (s.i1 + d) % 4

    def at2(s, d):
        return (s.i2 + d) % 4

    def spread_out(s, d):
        block = s.w.at[s.i2, at1(s, d)]
        s.second[d] = {e: send(block, block, s.p2(e)) for e in (1, 3)}

    for s, copies, got in ((a, w1_copies, w1_got), (b, w2_copies, w2_got)):
        for copy in copies:
            copy.wait_recv()
        s.w[s.i2, s.i1] = jnp.concatenate(
            [got[q][:, :CHAN_PAD].astype(F32) for q in range(ROWS)], axis=1
        ).astype(BF16)
        block = s.w.at[s.i2, s.i1]
        s.first = {d: send(block, block, s.p1(d)) for d in (1, 3)}
        s.second = {}
        spread_out(s, 0)

    for s in (a, b):
        s.first[1].wait_recv()
        block = s.w.at[s.i2, at1(s, 3), pl.ds(0, s.cut)]
        s.far_up = send(block, block, s.p1(1))
        s.first[3].wait_recv()
        block = s.w.at[s.i2, at1(s, 1), pl.ds(s.cut, HP - s.cut)]
        s.far_down = send(block, block, s.p1(3))
        spread_out(s, 3)
        spread_out(s, 1)
    for d in (2, 1, 3):
        s_copies[d].wait_recv()
        slot = s_all.at[((z - d) % 4) * 2 + c]
        s_copies[d + 4] = send(slot, slot, peer(dc=1))
    for s in (a, b):
        s.far_up.wait_recv()
        s.far_down.wait_recv()
        spread_out(s, 2)
        s.far = {}
    s_own.wait_recv()
    for d in (2, 1, 3):
        s_copies[d + 4].wait_recv()

    def first_half(slab):
        weights = wa[slab].reshape(4 * HP, CP)
        value = dot(weights, s_all[...].reshape(CP, PIX), NN).reshape(4, HP, PIX)
        for j in range(4):
            block = wa[slab, j].astype(F32)
            squares = jnp.sum(block * block, axis=1, keepdims=True)
            inv = jnp.broadcast_to(lax.rsqrt(squares + 1.0), (HP, PIX))
            act = value[j] * inv
            pre[slab * 4 + j] = act
            hidden = act * jax.nn.sigmoid(act) * SILU_GAIN * gain[slab * 4 + j]
            hid[j * 4 + slab] = hidden.astype(BF16)

    first_half(y)
    s_tok[...] = s_all[...].reshape(CP, PIX).T

    def pass_on(s, d, up):
        if up:
            s.second[d][1].wait_recv()
            block = s.w.at[at2(s, 3), at1(s, d)]
            s.far[d] = send(block, block, s.p2(1))
        else:
            s.second[d][3].wait_recv()
            block = s.w.at[at2(s, 1), at1(s, d)]
            s.far[d] = send(block, block, s.p2(3))

    for d, up in ((0, True), (3, False), (1, True), (2, False)):
        pass_on(a, d, up)
        pass_on(b, d, up)
    for d in (2, 1, 3):
        t_copies[d].wait_recv()
        slot = t_all.at[((z - d) % 4) * 2 + c]
        t_copies[d + 4] = send(slot, slot, peer(dc=1))

    def squares_of(slab):
        total = jnp.zeros((8, CP), F32)
        for j in range(4):
            block = wb[slab, j].astype(F32)
            total = total + jnp.sum((block * block).reshape(HP // 8, 8, CP), axis=0)
        return total

    for d in (3, 2):
        a.second[d][1].wait_recv()
    first_half(at2(a, 3))
    for d in (0, 1):
        a.second[d][3].wait_recv()
    first_half(at2(a, 1))
    t_own.wait_recv()
    for d in (2, 1, 3):
        t_copies[d + 4].wait_recv()
    t_tok[...] = t_all[...].reshape(CP, PIX).T
    for d in (3, 2):
        b.second[d][1].wait_recv()
    for d in (0, 1):
        b.second[d][3].wait_recv()
    squares = squares_of(x) + squares_of(at2(b, 1)) + squares_of(at2(b, 3))
    for d in (0, 3, 1, 2):
        a.far[d].wait_recv()
    first_half(at2(a, 2))
    for d in (0, 3, 1, 2):
        b.far[d].wait_recv()
    norm_row[0] = squares + squares_of(at2(b, 2))
    n_copy = send(norm_row.at[0], norm_in, peer(dc=1))

    raw_copies = []
    for low, high in CUTS:
        cols = slice(low, high)
        value = dot(
            hid[...].reshape(HT, PIX), wb[:, :, :, cols].reshape(HT, high - low), TN
        )
        raw[:, cols] = value
        raw_out[:, cols] = value.astype(BF16)
        part = pl.ds(low, high - low)
        raw_copies.append(send(raw_out.at[:, part], raw_in.at[:, part], peer(dc=1)))

    n_copy.wait_recv()
    norm = jnp.sum(norm_row[0] + norm_in[...], axis=0, keepdims=True)
    inv_row = lax.rsqrt(norm + 1.0)
    norm_row[1] = jnp.broadcast_to(inv_row, (8, CP))
    for copy, (low, high) in zip(raw_copies, CUTS):
        copy.wait_recv()
        cols = slice(low, high)
        sums = jnp.zeros((8, high - low), F32)
        inv = norm_row[1][0:1, cols]
        for q in range(8):
            rows = slice(q * 32, (q + 1) * 32)
            total = raw[rows, cols] + raw_in[rows, cols].astype(F32)
            state = s_tok[rows, cols].astype(F32)
            target = t_tok[rows, cols].astype(F32)
            grad = KEEP_COEF * state + ADD_COEF * (total * inv) - target
            dbranch = (ADD_COEF / SAMPLES * grad).astype(BF16)
            dbr[rows, cols] = dbranch
            wide = dbranch.astype(F32)
            dbn[rows, cols] = (wide * inv).astype(BF16)
            sums = sums + jnp.sum((wide * total).reshape(4, 8, high - low), axis=0)
        dot_rows[:, cols] = jnp.broadcast_to(
            jnp.sum(sums, axis=0, keepdims=True), (8, high - low)
        )
    dot_high = dot_rows[0:1].astype(BF16).astype(F32)
    dot_low = dot_rows[0:1] - dot_high
    row = lax.broadcasted_iota(jnp.int32, (HP, 1), 0)

    def second_grad(slab):
        value = dot(hid[pl.ds(slab * 4, 4)].reshape(4 * HP, PIX), dbr[...], NN)
        for j in range(4):
            block = value[j * HP : (j + 1) * HP]
            block = jnp.where(row == HALF, dot_high, block)
            block = jnp.where(row == HALF + 1, dot_low, block)
            gb[slab, j] = block.astype(BF16)

    def first_grad(slab):
        for j in range(4):
            value = pre[slab * 4 + j]
            sig = jax.nn.sigmoid(value)
            slope = sig * (1.0 + value * (1.0 - sig))
            grad = dh[j * 4 + slab]
            dpre[j] = (grad * gain[slab * 4 + j] * slope * SILU_GAIN).astype(BF16)
        value = dot(dpre[...].reshape(4 * HP, PIX), s_tok[...], NN)
        ga[slab] = value.reshape(4, HP, CP).astype(BF16)

    def hidden_grad(i, _):
        dh[pl.ds(i * 4, 4)] = dot(wb[i].reshape(4 * HP, CP), dbn[...], NT).reshape(4, HP, PIX)
        return 0

    def scatter_far(s, d):
        s.got_half[d] = send(
            s.g.at[at2(s, 2), at1(s, d)], s.half2.at[d], s.p2(1 if d < 2 else 3)
        )

    def scatter_near(s, d):
        way, e = (1, 3) if d < 2 else (0, 1)
        s.got_full[way, d] = send(
            s.g.at[at2(s, e), at1(s, d)], s.full2.at[way, d], s.p2(e)
        )

    def scatter_relay(s, d):
        s.got_half[d].wait_recv()
        way, e = (0, 1) if d < 2 else (1, 3)
        spot = (at2(s, e), at1(s, d))
        s.g[spot] = (s.g[spot].astype(F32) + s.half2[d].astype(F32)).astype(BF16)
        s.got_full[way, d] = send(s.g.at[spot[0], spot[1]], s.full2.at[way, d], s.p2(e))

    def scatter_sum(s, d):
        s.got_full[0, d].wait_recv()
        s.got_full[1, d].wait_recv()
        spot = (s.i2, at1(s, d))
        total = (
            s.g[spot].astype(F32) + s.full2[0, d].astype(F32) + s.full2[1, d].astype(F32)
        )
        if d == 0:
            s.own = total
        else:
            s.g[spot] = total.astype(BF16)

    def ring_far(s):
        spot = s.g.at[s.i2, at1(s, 2)]
        low, high = pl.ds(0, s.cut), pl.ds(s.cut, HP - s.cut)
        s.far_up = send(spot.at[low], s.half1.at[low], s.p1(1))
        s.far_down = send(spot.at[high], s.half1.at[high], s.p1(3))

    def ring_near(s, d):
        low, high = pl.ds(0, s.cut), pl.ds(s.cut, HP - s.cut)
        part, way = (high, 0) if d == 1 else (low, 1)
        s.near.append(send(s.g.at[s.i2, at1(s, d), part], s.full1.at[way, part], s.p1(d)))

    def ring_relay(s, d):
        part, way, copy = (
            (slice(0, s.cut), 0, s.far_up) if d == 1 else (slice(s.cut, HP), 1, s.far_down)
        )
        copy.wait_recv()
        at = at1(s, d)
        s.g[s.i2, at, part] = (
            s.g[s.i2, at, part].astype(F32) + s.half1[part].astype(F32)
        ).astype(BF16)
        rows = pl.ds(part.start, part.stop - part.start)
        s.near.append(send(s.g.at[s.i2, at, rows], s.full1.at[way, rows], s.p1(d)))

    def ring_sum(s):
        for copy in s.near:
            copy.wait_recv()
        return s.own + s.full1[0].astype(F32) + s.full1[1].astype(F32)

    sides = {"a": a, "b": b}
    for s in (a, b):
        s.got_half, s.got_full, s.near = {}, {}, []
    steps = {
        "far": scatter_far,
        "near": scatter_near,
        "relay": scatter_relay,
        "sum": scatter_sum,
        "ring_far": ring_far,
        "ring_near": ring_near,
        "ring_relay": ring_relay,
    }
    for step, *at in PLAN:
        if step == "hidden":
            lax.fori_loop(0, 4, hidden_grad, 0)
        elif step == "grad":
            side = sides[at[0]]
            (first_grad if side is a else second_grad)(at2(side, at[1]))
        else:
            steps[step](sides[at[0]], *at[1:])

    def hand_out(out, zs, zr):
        for q in range(ROWS):
            cols = slice(q * CHAN_PAD, (q + 1) * CHAN_PAD)
            fill = jnp.zeros((HP, WP - CHAN_PAD), F32)
            zs[q] = jnp.concatenate([out[:, cols], fill], axis=1).astype(BF16)
        zr[r] = zs[r]
        return [
            send(zs.at[((z + dz) % 4) * 2 + (c + dc) % 2], zr.at[r], peer(dz=dz, dc=dc))
            for dz, dc in group
        ]

    grad2 = ring_sum(b)
    w2 = wb[x, y].astype(F32)
    inv2 = norm_row[1][0:1]
    dot2 = grad2[HALF : HALF + 1] + grad2[HALF + 1 : HALF + 2]
    z2_copies = hand_out(grad2 * inv2 - w2 * (dot2 * inv2 * inv2 * inv2), zs2, zr2)
    grad1 = ring_sum(a)
    w1 = wa[y, x].astype(F32)
    inv1 = lax.rsqrt(jnp.sum(w1 * w1, axis=1, keepdims=True) + 1.0)
    dot1 = jnp.sum(w1 * grad1, axis=1, keepdims=True)
    z1_copies = hand_out(grad1 * inv1 - w1 * (dot1 * inv1 * inv1 * inv1), zs1, zr1)

    for copy in z2_copies:
        copy.wait_recv()
    for core in range(2):
        value = sum(zr2[2 * q + core].astype(F32) for q in range(4))
        out2[core * HALF : (core + 1) * HALF, 0, :] = value[:HALF, :CHAN]
    for copy in z1_copies:
        copy.wait_recv()
    for core in range(2):
        value = sum(zr1[2 * q + core].astype(F32) for q in range(4))
        value = jnp.concatenate([value, jnp.zeros((128 - HP, WP), F32)], axis=0).T
        out1[0, :, core * HALF : (core + 1) * HALF] = value[:CHAN, :HALF]
    for copy in started:
        copy.wait_send()


def local(clean, noise, bucket, mod_table, w_first, w_second):
    vmem = pl.BlockSpec(memory_space=pltpu.VMEM)
    smem = pl.BlockSpec(memory_space=pltpu.SMEM)
    hbm = pl.BlockSpec(memory_space=pl.ANY)
    block = (HP, CP)
    first, second = pl.pallas_call(
        kernel,
        out_shape=(
            jax.ShapeDtypeStruct((1, CHAN, BLOCK), F32),
            jax.ShapeDtypeStruct((BLOCK, 1, CHAN), F32),
        ),
        in_specs=[hbm, hbm, smem, hbm, hbm, hbm],
        out_specs=(vmem, vmem),
        scratch_shapes=[
            pltpu.VMEM(clean.shape, F32),
            pltpu.VMEM(noise.shape, F32),
            pltpu.VMEM((BUCKETS, WIDTH), F32),
            pltpu.VMEM((CHAN, BLOCK), F32),
            pltpu.VMEM((BLOCK, CHAN), F32),
            pltpu.VMEM((2, HP, WP), BF16),
            pltpu.VMEM((2, HP, WP), BF16),
            pltpu.VMEM((ROWS, HP, WP), BF16),
            pltpu.VMEM((ROWS, HP, WP), BF16),
            pltpu.VMEM((4, CHAN_PAD, PIX), BF16),
            pltpu.VMEM((4, CHAN_PAD, PIX), BF16),
            pltpu.VMEM((ROWS, CHAN_PAD, PIX), BF16),
            pltpu.VMEM((ROWS, CHAN_PAD, PIX), BF16),
            pltpu.VMEM((PIX, CP), BF16),
            pltpu.VMEM((PIX, CP), BF16),
            pltpu.VMEM((4, 4, *block), BF16),
            pltpu.VMEM((4, 4, *block), BF16),
            pltpu.VMEM((4, 4, *block), BF16),
            pltpu.VMEM((4, 4, *block), BF16),
            pltpu.VMEM((4, *block), BF16),
            pltpu.VMEM((2, 4, *block), BF16),
            pltpu.VMEM(block, BF16),
            pltpu.VMEM((2, *block), BF16),
            pltpu.VMEM((4, *block), BF16),
            pltpu.VMEM((2, 4, *block), BF16),
            pltpu.VMEM(block, BF16),
            pltpu.VMEM((2, *block), BF16),
            pltpu.VMEM((16, HP, PIX), F32),
            pltpu.VMEM((16, HP, PIX), F32),
            pltpu.VMEM((16, HP, PIX), BF16),
            pltpu.VMEM((4, HP, PIX), BF16),
            pltpu.VMEM((PIX, CP), F32),
            pltpu.VMEM((PIX, CP), BF16),
            pltpu.VMEM((PIX, CP), BF16),
            pltpu.VMEM((2, 8, CP), F32),
            pltpu.VMEM((8, CP), F32),
            pltpu.VMEM((PIX, CP), BF16),
            pltpu.VMEM((PIX, CP), BF16),
            pltpu.VMEM((8, CP), F32),
            pltpu.VMEM((16, HP, PIX), F32),
            pltpu.VMEM((ROWS, HP, WP), BF16),
            pltpu.VMEM((ROWS, HP, WP), BF16),
            pltpu.VMEM((ROWS, HP, WP), BF16),
            pltpu.VMEM((ROWS, HP, WP), BF16),
            pltpu.SemaphoreType.DMA((5,)),
            pltpu.SemaphoreType.DMA((MAX_COPIES,)),
            pltpu.SemaphoreType.DMA((MAX_COPIES,)),
        ],
        compiler_params=pltpu.CompilerParams(
            collective_id=0, has_side_effects=True, vmem_limit_bytes=60 * 1024 * 1024
        ),
    )(clean, noise, bucket, mod_table, w_first, jnp.transpose(w_second, (1, 0, 2)))
    return first, jnp.transpose(second, (1, 0, 2))


def solution(mesh):
    in_specs = (
        P("row", "col"),
        P("row", "col"),
        P(),
        P(),
        P(None, "row", "col"),
        P(None, "col", "row"),
    )
    out_specs = (P(None, "row", "col"), P(None, "col", "row"))
    return jax.shard_map(local, mesh=mesh, in_specs=in_specs, out_specs=out_specs, check_vma=False)
```

```python
import math

import jax
import jax.numpy as jnp
from jax import lax
from jax.experimental import pallas as pl
from jax.experimental.pallas import tpu as pltpu
from jax.sharding import PartitionSpec as P

MESH = pl.DeviceIdType.MESH
F32 = jnp.float32
BF16 = jnp.bfloat16

WIDTH = 1344
PIX = 256
SAMPLES = 64
BUCKETS = 32
MIX_WEIGHT = 0.3
KEEP_COEF = (1.0 - MIX_WEIGHT) / math.sqrt((1.0 - MIX_WEIGHT) ** 2 + MIX_WEIGHT**2)
ADD_COEF = MIX_WEIGHT / math.sqrt((1.0 - MIX_WEIGHT) ** 2 + MIX_WEIGHT**2)
SILU_GAIN = 1.0 / 0.596

ROWS = 8
CHAN = WIDTH // ROWS
CHAN_PAD = 176
CP = ROWS * CHAN_PAD
BLOCK = WIDTH // 16
HALF = BLOCK // 2
HP = 48
HT = 16 * HP
FOLD = HP + HP // 3
CUTS = ((0, 768), (768, 1408))
NN = (((1,), (0,)), ((), ()))
NT = (((1,), (1,)), ((), ()))
TN = (((0,), (0,)), ((), ()))
MAX_COPIES = 160
PLAN = (
    ("grad", "b", 2),
    ("far", "b", 0),
    ("far", "b", 2),
    ("hidden",),
    ("grad", "a", 2),
    ("far", "a", 1),
    ("far", "a", 2),
    ("grad", "a", 1),
    ("far", "b", 3),
    ("far", "b", 1),
    ("far", "a", 3),
    ("near", "a", 2),
    ("grad", "b", 1),
    ("near", "b", 2),
    ("grad", "a", 0),
    ("grad", "b", 3),
    ("relay", "b", 2),
    ("near", "a", 3),
    ("grad", "a", 3),
    ("grad", "b", 0),
    ("near", "a", 1),
    ("near", "b", 1),
    ("relay", "b", 3),
    ("relay", "b", 1),
    ("relay", "a", 2),
    ("relay", "a", 1),
    ("near", "b", 3),
    ("relay", "b", 0),
    ("near", "b", 0),
    ("sum", "b", 2),
    ("ring_far", "b"),
    ("relay", "a", 3),
    ("sum", "b", 1),
    ("far", "a", 0),
    ("sum", "a", 2),
    ("ring_far", "a"),
    ("sum", "b", 3),
    ("ring_near", "b", 1),
    ("ring_near", "b", 3),
    ("ring_relay", "b", 1),
    ("ring_relay", "b", 3),
    ("sum", "a", 1),
    ("relay", "a", 0),
    ("sum", "b", 0),
    ("near", "a", 0),
    ("sum", "a", 3),
    ("ring_relay", "a", 3),
    ("ring_near", "a", 1),
    ("ring_relay", "a", 1),
    ("ring_near", "a", 3),
    ("finish", "b"),
    ("sum", "a", 0),
    ("finish", "a"),
)


def dot(a, b, dims):
    return lax.dot_general(a, b, dims, preferred_element_type=F32)


def fold(block):
    third, rest = HP // 3, CHAN - 128
    below = [block[i * third : (i + 1) * third, 128:CHAN] for i in range(3)]
    below.append(jnp.zeros((third, 128 - 3 * rest), F32))
    return jnp.concatenate([block[:, :128], jnp.concatenate(below, axis=1)], axis=0)


def unfold(block):
    rest = CHAN - 128
    right = [block[HP:, i * rest : (i + 1) * rest] for i in range(3)]
    return jnp.concatenate([block[:HP], jnp.concatenate(right, axis=0)], axis=1)


def kernel(
    clean_hbm, noise_hbm, bucket, mod_hbm, w1_hbm, w2_hbm, out1, out2,
    clean, noise, mod, w1_in, w2_in, w1_out, w2_out, w1_got, w2_got,
    st, tg, s_all, t_all, s_tok, base, wa, wb, ga, gb,
    ra1, ra2, rx1, rx2, rb1, rb2, ry1, ry2,
    gain, pre, hid, dpre, raw, raw_out, raw_in, norm_row, norm_in,
    dbr, dbn, dot_rows, dh, zs1, zs2, zr1, zr2, load_sems, send_sems, recv_sems,
):
    r = lax.axis_index("row")
    k = lax.axis_index("col")
    z, c = r // 2, r % 2
    y, x = k // 4, k % 4

    def peer(dz=0, dc=0, dy=0, dx=0):
        return (
            ((z + dz) % 4) * 2 + (c + dc) % 2,
            ((y + dy) % 4) * 4 + (x + dx) % 4,
        )

    started = []

    def send(src, dst, device):
        i = len(started)
        copy = pltpu.make_async_remote_copy(
            src_ref=src,
            dst_ref=dst,
            send_sem=send_sems.at[i],
            recv_sem=recv_sems.at[i],
            device_id=device,
            device_id_type=MESH,
        )
        copy.start()
        started.append(copy)
        return copy

    group = [(dz, dc) for dz in (1, 3, 2, 0) for dc in (0, 1) if (dz, dc) != (0, 0)]
    barrier = pltpu.get_barrier_semaphore()
    near = [peer(dz=dz, dc=dc) for dz, dc in group]
    near += [peer(dx=1), peer(dx=3), peer(dy=1), peer(dy=3)]
    for device in near:
        pl.semaphore_signal(barrier, inc=1, device_id=device, device_id_type=MESH)

    loads = [
        pltpu.make_async_copy(src, dst, load_sems.at[i])
        for i, (src, dst) in enumerate(
            (
                (w1_hbm.at[0], w1_in),
                (w2_hbm.at[:, 0], w2_in),
                (clean_hbm, clean),
                (noise_hbm, noise),
                (mod_hbm.at[0], mod),
            )
        )
    ]
    for load in loads:
        load.start()

    loads[0].wait()
    loads[1].wait()
    hid_of = lax.broadcasted_iota(jnp.int32, (HP, BLOCK), 0)
    col_of = lax.broadcasted_iota(jnp.int32, (HP, BLOCK), 1)
    w1_bf = w1_in[...].astype(BF16)
    w2_bf = w2_in[...].astype(BF16)
    for core in range(2):
        pick = (col_of == hid_of + HALF * core) & (hid_of < HALF)
        pick = jnp.where(pick, 1.0, 0.0).astype(BF16)
        w1_out[core] = fold(dot(pick, w1_bf, NT)).astype(BF16)
        w2_out[core] = fold(dot(pick, w2_bf, NN)).astype(BF16)
    w1_got[r] = w1_out[c]
    w2_got[r] = w2_out[c]

    def state_piece(d):
        zq = (z + d) % 4
        level_of = jnp.full((1, PIX), bucket[k * 4 + zq], jnp.int32).astype(F32)
        level = jnp.exp(-3.0 + 5.0 * (level_of + 0.5) / BUCKETS)
        spread = jnp.sqrt(level * level + 0.25)
        cols = pl.ds(pl.multiple_of(zq * PIX, PIX), PIX)
        cl = clean[:, cols]
        no = noise[:, cols]
        pad = jnp.zeros((CHAN_PAD - CHAN, PIX), F32)
        state = (cl + level * no) / spread
        target = cl * (2.0 * level / spread) - no * (0.5 / spread)
        return (
            jnp.concatenate([state, pad], axis=0).astype(BF16),
            jnp.concatenate([target, pad], axis=0).astype(BF16),
        )

    pl.semaphore_wait(barrier, len(near))

    w1_copies = [
        send(w1_out.at[(c + dc) % 2], w1_got.at[r], peer(dz=dz, dc=dc)) for dz, dc in group
    ]
    w2_copies = [
        send(w2_out.at[(c + dc) % 2], w2_got.at[r], peer(dz=dz, dc=dc)) for dz, dc in group
    ]
    loads[2].wait()
    loads[3].wait()
    loads[4].wait()
    for d in range(4):
        state, target = state_piece(d)
        st[d] = state
        tg[d] = target
    s_all[r] = st[0]
    t_all[r] = tg[0]
    s_copies = {d: send(st.at[d], s_all.at[r], peer(dz=d)) for d in (2, 1, 3)}
    s_own = send(st.at[0], s_all.at[r], peer(dc=1))
    t_copies = {d: send(tg.at[d], t_all.at[r], peer(dz=d)) for d in (2, 1, 3)}
    t_own = send(tg.at[0], t_all.at[r], peer(dc=1))

    sample = k * 4 + z
    picked = lax.broadcasted_iota(jnp.int32, (BUCKETS, WIDTH), 0) == bucket[sample]
    mod_row = jnp.sum(jnp.where(picked, 1.0 + mod[...], 0.0), axis=0, keepdims=True)
    mod_row = jnp.concatenate([mod_row, jnp.zeros((1, CP - WIDTH), F32)], axis=1)
    for b in range(16):
        first = (BLOCK * b // 128) * 128
        lane = lax.broadcasted_iota(jnp.int32, (HP, 256), 1) + first
        row = lax.broadcasted_iota(jnp.int32, (HP, 256), 0)
        take = (lane == row + (BLOCK * b + HALF * c)) & (row < HALF)
        window = jnp.broadcast_to(mod_row[:, first : first + 256], (HP, 256))
        value = jnp.sum(jnp.where(take, window, 0.0), axis=1, keepdims=True)
        gain[b] = jnp.broadcast_to(value, (HP, PIX))

    class Side:
        pass

    def side_a():
        s = Side()
        s.w, s.g, s.i1, s.i2 = wa, ga, x, y
        s.p1 = lambda d: peer(dx=d)
        s.p2 = lambda d: peer(dy=d)
        s.cut = 32
        s.half1, s.half2, s.full1, s.full2 = rx1, ra1, rx2, ra2
        return s

    def side_b():
        s = Side()
        s.w, s.g, s.i1, s.i2 = wb, gb, y, x
        s.p1 = lambda d: peer(dy=d)
        s.p2 = lambda d: peer(dx=d)
        s.cut = 16
        s.half1, s.half2, s.full1, s.full2 = ry1, rb1, ry2, rb2
        return s

    a, b = side_a(), side_b()

    def at1(s, d):
        return (s.i1 + d) % 4

    def at2(s, d):
        return (s.i2 + d) % 4

    def spread_out(s, d):
        block = s.w.at[s.i2, at1(s, d)]
        s.second[d] = {e: send(block, block, s.p2(e)) for e in (1, 3)}

    for s, copies, got in ((a, w1_copies, w1_got), (b, w2_copies, w2_got)):
        for copy in copies:
            copy.wait_recv()
        fill = jnp.zeros((HP, CHAN_PAD - CHAN), F32)
        parts = []
        for q in range(ROWS):
            parts += [unfold(got[q].astype(F32)), fill]
        s.w[s.i2, s.i1] = jnp.concatenate(parts, axis=1).astype(BF16)
        block = s.w.at[s.i2, s.i1]
        s.first = {d: send(block, block, s.p1(d)) for d in (1, 3)}
        s.second = {}
        spread_out(s, 0)

    for s in (a, b):
        s.first[1].wait_recv()
        block = s.w.at[s.i2, at1(s, 3), pl.ds(0, s.cut)]
        s.far_up = send(block, block, s.p1(1))
        s.first[3].wait_recv()
        block = s.w.at[s.i2, at1(s, 1), pl.ds(s.cut, HP - s.cut)]
        s.far_down = send(block, block, s.p1(3))
        spread_out(s, 3)
        spread_out(s, 1)
    for d in (2, 1, 3):
        s_copies[d].wait_recv()
        slot = s_all.at[((z - d) % 4) * 2 + c]
        s_copies[d + 4] = send(slot, slot, peer(dc=1))
    for s in (a, b):
        s.far_up.wait_recv()
        s.far_down.wait_recv()
        spread_out(s, 2)
        s.far = {}
    s_own.wait_recv()
    for d in (2, 1, 3):
        s_copies[d + 4].wait_recv()

    def first_half(slab):
        weights = wa[slab].reshape(4 * HP, CP)
        value = dot(weights, s_all[...].reshape(CP, PIX), NN).reshape(4, HP, PIX)
        for j in range(4):
            block = wa[slab, j].astype(F32)
            squares = jnp.sum(block * block, axis=1, keepdims=True)
            inv = jnp.broadcast_to(lax.rsqrt(squares + 1.0), (HP, PIX))
            act = value[j] * inv
            pre[slab * 4 + j] = act
            hidden = act * jax.nn.sigmoid(act) * SILU_GAIN * gain[slab * 4 + j]
            hid[j * 4 + slab] = hidden.astype(BF16)

    first_half(y)
    s_tok[...] = s_all[...].reshape(CP, PIX).T

    def pass_on(s, d, up):
        if up:
            s.second[d][1].wait_recv()
            block = s.w.at[at2(s, 3), at1(s, d)]
            s.far[d] = send(block, block, s.p2(1))
        else:
            s.second[d][3].wait_recv()
            block = s.w.at[at2(s, 1), at1(s, d)]
            s.far[d] = send(block, block, s.p2(3))

    for d, up in ((0, True), (3, False), (1, True), (2, False)):
        pass_on(a, d, up)
        pass_on(b, d, up)
    for d in (2, 1, 3):
        t_copies[d].wait_recv()
        slot = t_all.at[((z - d) % 4) * 2 + c]
        t_copies[d + 4] = send(slot, slot, peer(dc=1))

    def squares_of(slab):
        total = jnp.zeros((8, CP), F32)
        for j in range(4):
            block = wb[slab, j].astype(F32)
            total = total + jnp.sum((block * block).reshape(HP // 8, 8, CP), axis=0)
        return total

    for d in (3, 2):
        a.second[d][1].wait_recv()
    first_half(at2(a, 3))
    for d in (0, 1):
        a.second[d][3].wait_recv()
    first_half(at2(a, 1))
    t_own.wait_recv()
    for d in (2, 1, 3):
        t_copies[d + 4].wait_recv()
    base[...] = KEEP_COEF * s_tok[...].astype(F32) - t_all[...].reshape(CP, PIX).T.astype(F32)
    for d in (3, 2):
        b.second[d][1].wait_recv()
    for d in (0, 1):
        b.second[d][3].wait_recv()
    squares = squares_of(x) + squares_of(at2(b, 1)) + squares_of(at2(b, 3))
    for d in (0, 3, 1, 2):
        a.far[d].wait_recv()
    first_half(at2(a, 2))
    def branch(slab, cols):
        weights = wb[slab, :, :, cols].reshape(4 * HP, cols.stop - cols.start)
        return dot(hid[pl.ds(slab * 4, 4)].reshape(4 * HP, PIX), weights, TN)

    for cut in CUTS:
        cols = slice(*cut)
        raw[:, cols] = branch(x, cols) + branch(at2(b, 1), cols) + branch(at2(b, 3), cols)
    for d in (0, 3, 1, 2):
        b.far[d].wait_recv()
    raw_copies = []
    for cut in CUTS:
        cols = slice(*cut)
        value = raw[:, cols] + branch(at2(b, 2), cols)
        raw[:, cols] = value
        raw_out[:, cols] = value.astype(BF16)
        part = pl.ds(cut[0], cut[1] - cut[0])
        raw_copies.append(send(raw_out.at[:, part], raw_in.at[:, part], peer(dc=1)))
    norm_row[0] = squares + squares_of(at2(b, 2))
    n_copy = send(norm_row.at[0], norm_in, peer(dc=1))

    n_copy.wait_recv()
    norm = jnp.sum(norm_row[0] + norm_in[...], axis=0, keepdims=True)
    inv_row = lax.rsqrt(norm + 1.0)
    norm_row[1] = jnp.broadcast_to(inv_row, (8, CP))
    for copy, (low, high) in zip(raw_copies, CUTS):
        copy.wait_recv()
        cols = slice(low, high)
        sums = jnp.zeros((8, high - low), F32)
        inv = norm_row[1][0:1, cols] * ADD_COEF
        for q in range(8):
            rows = slice(q * 32, (q + 1) * 32)
            total = raw[rows, cols] + raw_in[rows, cols].astype(F32)
            grad = base[rows, cols] + total * inv
            dbranch = (ADD_COEF * grad).astype(BF16)
            dbr[rows, cols] = dbranch
            product = dbranch.astype(F32) * total
            sums = sums + jnp.sum(product.reshape(4, 8, high - low), axis=0)
        dot_rows[:, cols] = jnp.broadcast_to(
            jnp.sum(sums, axis=0, keepdims=True), (8, high - low)
        )
    dot_high = dot_rows[0:1].astype(BF16).astype(F32)
    dot_low = dot_rows[0:1] - dot_high
    row = lax.broadcasted_iota(jnp.int32, (HP, 1), 0)

    def second_grad(slab):
        value = dot(hid[pl.ds(slab * 4, 4)].reshape(4 * HP, PIX), dbr[...], NN)
        for j in range(4):
            block = value[j * HP : (j + 1) * HP]
            block = jnp.where(row == HALF, dot_high, block)
            block = jnp.where(row == HALF + 1, dot_low, block)
            gb[slab, j] = block.astype(BF16)

    def first_grad(slab):
        for j in range(4):
            value = pre[slab * 4 + j]
            sig = jax.nn.sigmoid(value)
            slope = sig * (1.0 + value * (1.0 - sig))
            grad = dh[j * 4 + slab]
            dpre[j] = (grad * gain[slab * 4 + j] * slope * SILU_GAIN).astype(BF16)
        value = dot(dpre[...].reshape(4 * HP, PIX), s_tok[...], NN)
        ga[slab] = value.reshape(4, HP, CP).astype(BF16)

    def hidden_grad(i, _):
        dh[pl.ds(i * 4, 4)] = dot(wb[i].reshape(4 * HP, CP), dbn[...], NT).reshape(4, HP, PIX)
        return 0

    def scatter_far(s, d):
        s.got_half[d] = send(
            s.g.at[at2(s, 2), at1(s, d)], s.half2.at[d], s.p2(1 if d < 2 else 3)
        )

    def scatter_near(s, d):
        way, e = (1, 3) if d < 2 else (0, 1)
        s.got_full[way, d] = send(
            s.g.at[at2(s, e), at1(s, d)], s.full2.at[way, d], s.p2(e)
        )

    def scatter_relay(s, d):
        s.got_half[d].wait_recv()
        way, e = (0, 1) if d < 2 else (1, 3)
        spot = (at2(s, e), at1(s, d))
        s.g[spot] = (s.g[spot].astype(F32) + s.half2[d].astype(F32)).astype(BF16)
        s.got_full[way, d] = send(s.g.at[spot[0], spot[1]], s.full2.at[way, d], s.p2(e))

    def scatter_sum(s, d):
        s.got_full[0, d].wait_recv()
        s.got_full[1, d].wait_recv()
        spot = (s.i2, at1(s, d))
        total = (
            s.g[spot].astype(F32) + s.full2[0, d].astype(F32) + s.full2[1, d].astype(F32)
        )
        if d == 0:
            s.own = total
        else:
            s.g[spot] = total.astype(BF16)

    def ring_far(s):
        spot = s.g.at[s.i2, at1(s, 2)]
        low, high = pl.ds(0, s.cut), pl.ds(s.cut, HP - s.cut)
        s.far_up = send(spot.at[low], s.half1.at[low], s.p1(1))
        s.far_down = send(spot.at[high], s.half1.at[high], s.p1(3))

    def ring_near(s, d):
        low, high = pl.ds(0, s.cut), pl.ds(s.cut, HP - s.cut)
        part, way = (high, 0) if d == 1 else (low, 1)
        s.near.append(send(s.g.at[s.i2, at1(s, d), part], s.full1.at[way, part], s.p1(d)))

    def ring_relay(s, d):
        part, way, copy = (
            (slice(0, s.cut), 0, s.far_up) if d == 1 else (slice(s.cut, HP), 1, s.far_down)
        )
        copy.wait_recv()
        at = at1(s, d)
        s.g[s.i2, at, part] = (
            s.g[s.i2, at, part].astype(F32) + s.half1[part].astype(F32)
        ).astype(BF16)
        rows = pl.ds(part.start, part.stop - part.start)
        s.near.append(send(s.g.at[s.i2, at, rows], s.full1.at[way, rows], s.p1(d)))

    def ring_sum(s):
        for copy in s.near:
            copy.wait_recv()
        return s.own + s.full1[0].astype(F32) + s.full1[1].astype(F32)

    sides = {"a": a, "b": b}
    for s in (a, b):
        s.got_half, s.got_full, s.near = {}, {}, []
    steps = {
        "far": scatter_far,
        "near": scatter_near,
        "relay": scatter_relay,
        "sum": scatter_sum,
        "ring_far": ring_far,
        "ring_near": ring_near,
        "ring_relay": ring_relay,
    }
    def hand_out(out, zs, zr):
        for q in range(ROWS):
            first = q * CHAN_PAD
            zs[q] = fold(out[:, first : first + CHAN]).astype(BF16)
        zr[r] = zs[r]
        return [
            send(zs.at[((z + dz) % 4) * 2 + (c + dc) % 2], zr.at[r], peer(dz=dz, dc=dc))
            for dz, dc in group
        ]

    def finish_second():
        grad2 = ring_sum(b)
        w2 = wb[x, y].astype(F32)
        inv2 = norm_row[1][0:1]
        dot2 = grad2[HALF : HALF + 1] + grad2[HALF + 1 : HALF + 2]
        return hand_out(grad2 * inv2 - w2 * (dot2 * inv2 * inv2 * inv2), zs2, zr2)

    def finish_first():
        grad1 = ring_sum(a)
        w1 = wa[y, x].astype(F32)
        inv1 = lax.rsqrt(jnp.sum(w1 * w1, axis=1, keepdims=True) + 1.0)
        dot1 = jnp.sum(w1 * grad1, axis=1, keepdims=True)
        return hand_out(grad1 * inv1 - w1 * (dot1 * inv1 * inv1 * inv1), zs1, zr1)

    for step, *at in PLAN:
        if step == "hidden":
            dbn[...] = (dbr[...].astype(F32) * norm_row[1][0:1]).astype(BF16)
            lax.fori_loop(0, 4, hidden_grad, 0)
        elif step == "finish" and at[0] == "b":
            z2_copies = finish_second()
        elif step == "finish":
            z1_copies = finish_first()
        elif step == "grad":
            side = sides[at[0]]
            (first_grad if side is a else second_grad)(at2(side, at[1]))
        else:
            steps[step](sides[at[0]], *at[1:])

    for copy in z2_copies:
        copy.wait_recv()
    for core in range(2):
        value = unfold(sum(zr2[2 * q + core].astype(F32) for q in range(4)))
        out2[core * HALF : (core + 1) * HALF, 0, :] = value[:HALF]
    for copy in z1_copies:
        copy.wait_recv()
    for core in range(2):
        value = unfold(sum(zr1[2 * q + core].astype(F32) for q in range(4)))
        value = jnp.concatenate([value, jnp.zeros((HP, 256 - CHAN), F32)], axis=1)
        value = jnp.concatenate([value, jnp.zeros((128 - HP, 256), F32)], axis=0).T
        out1[0, :, core * HALF : (core + 1) * HALF] = value[:CHAN, :HALF]
    for copy in started:
        copy.wait_send()


def local(clean, noise, bucket, mod_table, w_first, w_second):
    vmem = pl.BlockSpec(memory_space=pltpu.VMEM)
    smem = pl.BlockSpec(memory_space=pltpu.SMEM)
    hbm = pl.BlockSpec(memory_space=pl.ANY)
    block = (HP, CP)
    first, second = pl.pallas_call(
        kernel,
        out_shape=(
            jax.ShapeDtypeStruct((1, CHAN, BLOCK), F32),
            jax.ShapeDtypeStruct((BLOCK, 1, CHAN), F32),
        ),
        in_specs=[hbm, hbm, smem, hbm, hbm, hbm],
        out_specs=(vmem, vmem),
        scratch_shapes=[
            pltpu.VMEM(clean.shape, F32),
            pltpu.VMEM(noise.shape, F32),
            pltpu.VMEM((BUCKETS, WIDTH), F32),
            pltpu.VMEM((CHAN, BLOCK), F32),
            pltpu.VMEM((BLOCK, CHAN), F32),
            pltpu.VMEM((2, FOLD, 128), BF16),
            pltpu.VMEM((2, FOLD, 128), BF16),
            pltpu.VMEM((ROWS, FOLD, 128), BF16),
            pltpu.VMEM((ROWS, FOLD, 128), BF16),
            pltpu.VMEM((4, CHAN_PAD, PIX), BF16),
            pltpu.VMEM((4, CHAN_PAD, PIX), BF16),
            pltpu.VMEM((ROWS, CHAN_PAD, PIX), BF16),
            pltpu.VMEM((ROWS, CHAN_PAD, PIX), BF16),
            pltpu.VMEM((PIX, CP), BF16),
            pltpu.VMEM((PIX, CP), F32),
            pltpu.VMEM((4, 4, *block), BF16),
            pltpu.VMEM((4, 4, *block), BF16),
            pltpu.VMEM((4, 4, *block), BF16),
            pltpu.VMEM((4, 4, *block), BF16),
            pltpu.VMEM((4, *block), BF16),
            pltpu.VMEM((2, 4, *block), BF16),
            pltpu.VMEM(block, BF16),
            pltpu.VMEM((2, *block), BF16),
            pltpu.VMEM((4, *block), BF16),
            pltpu.VMEM((2, 4, *block), BF16),
            pltpu.VMEM(block, BF16),
            pltpu.VMEM((2, *block), BF16),
            pltpu.VMEM((16, HP, PIX), F32),
            pltpu.VMEM((16, HP, PIX), F32),
            pltpu.VMEM((16, HP, PIX), BF16),
            pltpu.VMEM((4, HP, PIX), BF16),
            pltpu.VMEM((PIX, CP), F32),
            pltpu.VMEM((PIX, CP), BF16),
            pltpu.VMEM((PIX, CP), BF16),
            pltpu.VMEM((2, 8, CP), F32),
            pltpu.VMEM((8, CP), F32),
            pltpu.VMEM((PIX, CP), BF16),
            pltpu.VMEM((PIX, CP), BF16),
            pltpu.VMEM((8, CP), F32),
            pltpu.VMEM((16, HP, PIX), F32),
            pltpu.VMEM((ROWS, FOLD, 128), BF16),
            pltpu.VMEM((ROWS, FOLD, 128), BF16),
            pltpu.VMEM((ROWS, FOLD, 128), BF16),
            pltpu.VMEM((ROWS, FOLD, 128), BF16),
            pltpu.SemaphoreType.DMA((5,)),
            pltpu.SemaphoreType.DMA((MAX_COPIES,)),
            pltpu.SemaphoreType.DMA((MAX_COPIES,)),
        ],
        compiler_params=pltpu.CompilerParams(
            collective_id=0, has_side_effects=True, vmem_limit_bytes=60 * 1024 * 1024
        ),
    )(clean, noise, bucket, mod_table, w_first, jnp.transpose(w_second, (1, 0, 2)))
    return first / SAMPLES, jnp.transpose(second / SAMPLES, (1, 0, 2))


def solution(mesh):
    in_specs = (
        P("row", "col"),
        P("row", "col"),
        P(),
        P(),
        P(None, "row", "col"),
        P(None, "col", "row"),
    )
    out_specs = (P(None, "row", "col"), P(None, "col", "row"))
    return jax.shard_map(local, mesh=mesh, in_specs=in_specs, out_specs=out_specs, check_vma=False)
```

```python
import math

import jax
import jax.numpy as jnp
from jax import lax
from jax.experimental import pallas as pl
from jax.experimental.pallas import tpu as pltpu
from jax.sharding import PartitionSpec as P

MESH = pl.DeviceIdType.MESH
F32 = jnp.float32
BF16 = jnp.bfloat16

WIDTH = 1344
PIX = 256
SAMPLES = 64
BUCKETS = 32
MIX_WEIGHT = 0.3
KEEP_COEF = (1.0 - MIX_WEIGHT) / math.sqrt((1.0 - MIX_WEIGHT) ** 2 + MIX_WEIGHT**2)
ADD_COEF = MIX_WEIGHT / math.sqrt((1.0 - MIX_WEIGHT) ** 2 + MIX_WEIGHT**2)
SILU_GAIN = 1.0 / 0.596

ROWS = 8
CHAN = WIDTH // ROWS
CHAN_PAD = 176
CP = ROWS * CHAN_PAD
BLOCK = WIDTH // 16
HALF = BLOCK // 2
HP = 48
HT = 16 * HP
STRIPS = CP // 128
FULL = 40
SIZE_W = STRIPS * FULL + 24
SIZE_G = STRIPS * FULL + 40
FOLD = HP + HP // 3
CUTS = ((0, 768), (768, 1408))
NN = (((1,), (0,)), ((), ()))
NT = (((1,), (1,)), ((), ()))
TN = (((0,), (0,)), ((), ()))
MAX_COPIES = 160
PLAN = (
    ("grad", "b", 2),
    ("far", "b", 2),
    ("far", "b", 3),
    ("far", "b", 1),
    ("far", "b", 0),
    ("hidden",),
    ("grad", "a", 2),
    ("far", "a", 1),
    ("far", "a", 2),
    ("grad", "a", 3),
    ("grad", "b", 0),
    ("grad", "a", 1),
    ("far", "a", 0),
    ("grad", "b", 3),
    ("grad", "b", 1),
    ("far", "a", 3),
    ("grad", "a", 0),
    ("relay", "b", 2),
    ("near", "b", 2),
    ("near", "a", 1),
    ("near", "a", 2),
    ("near", "b", 3),
    ("relay", "b", 1),
    ("relay", "b", 3),
    ("relay", "a", 1),
    ("relay", "a", 2),
    ("sum", "b", 2),
    ("ring_far", "b"),
    ("near", "a", 3),
    ("near", "b", 1),
    ("near", "b", 0),
    ("relay", "b", 0),
    ("relay", "a", 3),
    ("sum", "a", 2),
    ("sum", "b", 3),
    ("ring_far", "a"),
    ("sum", "b", 1),
    ("ring_near", "b", 1),
    ("ring_near", "b", 3),
    ("ring_relay", "b", 1),
    ("relay", "a", 0),
    ("ring_relay", "b", 3),
    ("near", "a", 0),
    ("sum", "a", 1),
    ("sum", "a", 3),
    ("ring_near", "a", 3),
    ("ring_near", "a", 1),
    ("ring_relay", "a", 1),
    ("sum", "b", 0),
    ("ring_relay", "a", 3),
    ("finish", "b"),
    ("sum", "a", 0),
    ("finish", "a"),
)


def dot(a, b, dims):
    return lax.dot_general(a, b, dims, preferred_element_type=F32)


def fold(block):
    third, rest = HP // 3, CHAN - 128
    below = [block[i * third : (i + 1) * third, 128:CHAN] for i in range(3)]
    below.append(jnp.zeros((third, 128 - 3 * rest), F32))
    return jnp.concatenate([block[:, :128], jnp.concatenate(below, axis=1)], axis=0)


def unfold(block):
    rest = CHAN - 128
    right = [block[HP:, i * rest : (i + 1) * rest] for i in range(3)]
    return jnp.concatenate([block[:HP], jnp.concatenate(right, axis=0)], axis=1)


def pack(block, ref, at):
    size = ref.shape[2]
    left = (size - STRIPS * FULL) // STRIPS
    rest = []
    for j in range(STRIPS):
        lanes = slice(128 * j, 128 * (j + 1))
        ref[(*at, slice(FULL * j, FULL * (j + 1)))] = block[:FULL, lanes].astype(BF16)
        rest.append(block[FULL : FULL + left, lanes])
    fill = size - STRIPS * (FULL + left)
    rest.append(jnp.zeros((fill, 128), F32))
    ref[(*at, slice(STRIPS * FULL, size))] = jnp.concatenate(rest, axis=0).astype(BF16)


def unpack(strips):
    left = (strips.shape[0] - STRIPS * FULL) // STRIPS
    fill = jnp.zeros((HP - FULL - left, 128), F32)
    parts = []
    for j in range(STRIPS):
        first = STRIPS * FULL + left * j
        rest = jnp.concatenate([strips[first : first + left], fill], axis=0)
        parts.append(jnp.concatenate([strips[FULL * j : FULL * (j + 1)], rest], axis=0))
    return jnp.concatenate(parts, axis=1)


def kernel(
    clean_hbm, noise_hbm, bucket, mod_hbm, w1_hbm, w2_hbm, out1, out2,
    clean, noise, mod, w1_in, w2_in, w1_out, w2_out, w1_got, w2_got,
    st, tg, s_all, t_all, s_tok, base, wa, wb, wa_strips, wb_strips, ga, gb,
    ra1, ra2, rx1, rx2, rb1, rb2, ry1, ry2,
    gain, pre, hid, dpre, raw, raw_out, raw_in, norm_row, norm_in,
    dbr, dbn, dot_rows, dh, zs1, zs2, zr1, zr2, load_sems, send_sems, recv_sems,
):
    r = lax.axis_index("row")
    k = lax.axis_index("col")
    z, c = r // 2, r % 2
    y, x = k // 4, k % 4

    def peer(dz=0, dc=0, dy=0, dx=0):
        return (
            ((z + dz) % 4) * 2 + (c + dc) % 2,
            ((y + dy) % 4) * 4 + (x + dx) % 4,
        )

    started = []

    def send(src, dst, device):
        i = len(started)
        copy = pltpu.make_async_remote_copy(
            src_ref=src,
            dst_ref=dst,
            send_sem=send_sems.at[i],
            recv_sem=recv_sems.at[i],
            device_id=device,
            device_id_type=MESH,
        )
        copy.start()
        started.append(copy)
        return copy

    group = [(dz, dc) for dz in (1, 3, 2, 0) for dc in (0, 1) if (dz, dc) != (0, 0)]
    barrier = pltpu.get_barrier_semaphore()
    near = [peer(dz=dz, dc=dc) for dz, dc in group]
    near += [peer(dx=1), peer(dx=3), peer(dy=1), peer(dy=3)]
    for device in near:
        pl.semaphore_signal(barrier, inc=1, device_id=device, device_id_type=MESH)

    loads = [
        pltpu.make_async_copy(src, dst, load_sems.at[i])
        for i, (src, dst) in enumerate(
            (
                (w1_hbm.at[0], w1_in),
                (w2_hbm.at[:, 0], w2_in),
                (clean_hbm, clean),
                (noise_hbm, noise),
                (mod_hbm.at[0], mod),
            )
        )
    ]
    for load in loads:
        load.start()

    loads[0].wait()
    loads[1].wait()
    hid_of = lax.broadcasted_iota(jnp.int32, (HP, BLOCK), 0)
    col_of = lax.broadcasted_iota(jnp.int32, (HP, BLOCK), 1)
    w1_bf = w1_in[...].astype(BF16)
    w2_bf = w2_in[...].astype(BF16)
    for core in range(2):
        pick = (col_of == hid_of + HALF * core) & (hid_of < HALF)
        pick = jnp.where(pick, 1.0, 0.0).astype(BF16)
        w1_out[core] = fold(dot(pick, w1_bf, NT)).astype(BF16)
        w2_out[core] = fold(dot(pick, w2_bf, NN)).astype(BF16)
    w1_got[r] = w1_out[c]
    w2_got[r] = w2_out[c]

    def state_piece(d):
        zq = (z + d) % 4
        level_of = jnp.full((1, PIX), bucket[k * 4 + zq], jnp.int32).astype(F32)
        level = jnp.exp(-3.0 + 5.0 * (level_of + 0.5) / BUCKETS)
        spread = jnp.sqrt(level * level + 0.25)
        cols = pl.ds(pl.multiple_of(zq * PIX, PIX), PIX)
        cl = clean[:, cols]
        no = noise[:, cols]
        pad = jnp.zeros((CHAN_PAD - CHAN, PIX), F32)
        state = (cl + level * no) / spread
        target = cl * (2.0 * level / spread) - no * (0.5 / spread)
        return (
            jnp.concatenate([state, pad], axis=0).astype(BF16),
            jnp.concatenate([target, pad], axis=0).astype(BF16),
        )

    pl.semaphore_wait(barrier, len(near))

    w1_copies = [
        send(w1_out.at[(c + dc) % 2], w1_got.at[r], peer(dz=dz, dc=dc)) for dz, dc in group
    ]
    w2_copies = [
        send(w2_out.at[(c + dc) % 2], w2_got.at[r], peer(dz=dz, dc=dc)) for dz, dc in group
    ]
    loads[2].wait()
    loads[3].wait()
    loads[4].wait()
    for d in range(4):
        state, target = state_piece(d)
        st[d] = state
        tg[d] = target
    s_all[r] = st[0]
    t_all[r] = tg[0]
    s_copies = {d: send(st.at[d], s_all.at[r], peer(dz=d)) for d in (2, 1, 3)}
    s_own = send(st.at[0], s_all.at[r], peer(dc=1))
    t_copies = {d: send(tg.at[d], t_all.at[r], peer(dz=d)) for d in (2, 1, 3)}
    t_own = send(tg.at[0], t_all.at[r], peer(dc=1))

    sample = k * 4 + z
    picked = lax.broadcasted_iota(jnp.int32, (BUCKETS, WIDTH), 0) == bucket[sample]
    mod_row = jnp.sum(jnp.where(picked, 1.0 + mod[...], 0.0), axis=0, keepdims=True)
    mod_row = jnp.concatenate([mod_row, jnp.zeros((1, CP - WIDTH), F32)], axis=1)
    for b in range(16):
        first = (BLOCK * b // 128) * 128
        lane = lax.broadcasted_iota(jnp.int32, (HP, 256), 1) + first
        row = lax.broadcasted_iota(jnp.int32, (HP, 256), 0)
        take = (lane == row + (BLOCK * b + HALF * c)) & (row < HALF)
        window = jnp.broadcast_to(mod_row[:, first : first + 256], (HP, 256))
        value = jnp.sum(jnp.where(take, window, 0.0), axis=1, keepdims=True)
        gain[b] = jnp.broadcast_to(value, (HP, PIX))

    class Side:
        pass

    def side_a():
        s = Side()
        s.w, s.full, s.g, s.i1, s.i2 = wa_strips, wa, ga, x, y
        s.p1 = lambda d: peer(dx=d)
        s.p2 = lambda d: peer(dy=d)
        s.cut = (SIZE_W // 2, SIZE_W // 2)
        s.half1, s.half2, s.full1, s.full2 = rx1, ra1, rx2, ra2
        return s

    def side_b():
        s = Side()
        s.w, s.full, s.g, s.i1, s.i2 = wb_strips, wb, gb, y, x
        s.p1 = lambda d: peer(dy=d)
        s.p2 = lambda d: peer(dx=d)
        s.cut = (SIZE_W // 2, SIZE_G // 2)
        s.half1, s.half2, s.full1, s.full2 = ry1, rb1, ry2, rb2
        return s

    a, b = side_a(), side_b()

    def at1(s, d):
        return (s.i1 + d) % 4

    def at2(s, d):
        return (s.i2 + d) % 4

    def spread_out(s, d):
        block = s.w.at[s.i2, at1(s, d)]
        s.second[d] = {e: send(block, block, s.p2(e)) for e in (1, 3)}

    for s, copies, got in ((a, w1_copies, w1_got), (b, w2_copies, w2_got)):
        for copy in copies:
            copy.wait_recv()
        fill = jnp.zeros((HP, CHAN_PAD - CHAN), F32)
        parts = []
        for q in range(ROWS):
            parts += [unfold(got[q].astype(F32)), fill]
        whole = jnp.concatenate(parts, axis=1)
        s.full[s.i2, s.i1] = whole.astype(BF16)
        pack(whole, s.w, (s.i2, s.i1))
        block = s.w.at[s.i2, s.i1]
        s.first = {d: send(block, block, s.p1(d)) for d in (1, 3)}
        s.second = {}
        spread_out(s, 0)

    for s in (a, b):
        s.first[1].wait_recv()
        block = s.w.at[s.i2, at1(s, 3), pl.ds(0, s.cut[0])]
        s.far_up = send(block, block, s.p1(1))
        s.first[3].wait_recv()
        block = s.w.at[s.i2, at1(s, 1), pl.ds(s.cut[0], s.cut[0])]
        s.far_down = send(block, block, s.p1(3))
        spread_out(s, 3)
        spread_out(s, 1)
    for d in (2, 1, 3):
        s_copies[d].wait_recv()
        slot = s_all.at[((z - d) % 4) * 2 + c]
        s_copies[d + 4] = send(slot, slot, peer(dc=1))
    for s in (a, b):
        s.far_up.wait_recv()
        s.far_down.wait_recv()
        spread_out(s, 2)
        s.far = {}
    s_own.wait_recv()
    for d in (2, 1, 3):
        s_copies[d + 4].wait_recv()

    def spread(s, slab, blocks):
        for d in blocks:
            at = (slab, at1(s, d))
            s.full[at] = unpack(s.w[at].astype(F32)).astype(BF16)

    def first_half(slab):
        weights = wa[slab].reshape(4 * HP, CP)
        value = dot(weights, s_all[...].reshape(CP, PIX), NN).reshape(4, HP, PIX)
        for j in range(4):
            block = wa[slab, j].astype(F32)
            squares = jnp.sum(block * block, axis=1, keepdims=True)
            inv = jnp.broadcast_to(lax.rsqrt(squares + 1.0), (HP, PIX))
            act = value[j] * inv
            pre[slab * 4 + j] = act
            hidden = act * jax.nn.sigmoid(act) * SILU_GAIN * gain[slab * 4 + j]
            hid[j * 4 + slab] = hidden.astype(BF16)

    spread(a, y, (1, 2, 3))
    first_half(y)
    s_tok[...] = s_all[...].reshape(CP, PIX).T

    def pass_on(s, d, up):
        if up:
            s.second[d][1].wait_recv()
            block = s.w.at[at2(s, 3), at1(s, d)]
            s.far[d] = send(block, block, s.p2(1))
        else:
            s.second[d][3].wait_recv()
            block = s.w.at[at2(s, 1), at1(s, d)]
            s.far[d] = send(block, block, s.p2(3))

    for d, up in ((0, True), (3, False), (1, True), (2, False)):
        pass_on(a, d, up)
        pass_on(b, d, up)
    for d in (2, 1, 3):
        t_copies[d].wait_recv()
        slot = t_all.at[((z - d) % 4) * 2 + c]
        t_copies[d + 4] = send(slot, slot, peer(dc=1))

    def squares_of(slab):
        total = jnp.zeros((8, CP), F32)
        for j in range(4):
            block = wb[slab, j].astype(F32)
            total = total + jnp.sum((block * block).reshape(HP // 8, 8, CP), axis=0)
        return total

    for d in (3, 2):
        a.second[d][1].wait_recv()
    spread(a, at2(a, 3), range(4))
    first_half(at2(a, 3))
    for d in (0, 1):
        a.second[d][3].wait_recv()
    spread(a, at2(a, 1), range(4))
    first_half(at2(a, 1))
    t_own.wait_recv()
    for d in (2, 1, 3):
        t_copies[d + 4].wait_recv()
    base[...] = KEEP_COEF * s_tok[...].astype(F32) - t_all[...].reshape(CP, PIX).T.astype(F32)
    for d in (3, 2):
        b.second[d][1].wait_recv()
    for d in (0, 1):
        b.second[d][3].wait_recv()
    spread(b, x, (1, 2, 3))
    spread(b, at2(b, 1), range(4))
    spread(b, at2(b, 3), range(4))
    squares = squares_of(x) + squares_of(at2(b, 1)) + squares_of(at2(b, 3))
    for d in (0, 3, 1, 2):
        a.far[d].wait_recv()
    spread(a, at2(a, 2), range(4))
    first_half(at2(a, 2))
    def branch(slab, cols):
        weights = wb[slab, :, :, cols].reshape(4 * HP, cols.stop - cols.start)
        return dot(hid[pl.ds(slab * 4, 4)].reshape(4 * HP, PIX), weights, TN)

    for cut in CUTS:
        cols = slice(*cut)
        raw[:, cols] = branch(x, cols) + branch(at2(b, 1), cols) + branch(at2(b, 3), cols)
    for d in (0, 3, 1, 2):
        b.far[d].wait_recv()
    spread(b, at2(b, 2), range(4))
    raw_copies = []
    for cut in CUTS:
        cols = slice(*cut)
        value = raw[:, cols] + branch(at2(b, 2), cols)
        raw[:, cols] = value
        raw_out[:, cols] = value.astype(BF16)
        part = pl.ds(cut[0], cut[1] - cut[0])
        raw_copies.append(send(raw_out.at[:, part], raw_in.at[:, part], peer(dc=1)))
    norm_row[0] = squares + squares_of(at2(b, 2))
    n_copy = send(norm_row.at[0], norm_in, peer(dc=1))

    n_copy.wait_recv()
    norm = jnp.sum(norm_row[0] + norm_in[...], axis=0, keepdims=True)
    inv_row = lax.rsqrt(norm + 1.0)
    norm_row[1] = jnp.broadcast_to(inv_row, (8, CP))
    for copy, (low, high) in zip(raw_copies, CUTS):
        copy.wait_recv()
        cols = slice(low, high)
        sums = jnp.zeros((8, high - low), F32)
        inv = norm_row[1][0:1, cols] * ADD_COEF
        for q in range(8):
            rows = slice(q * 32, (q + 1) * 32)
            total = raw[rows, cols] + raw_in[rows, cols].astype(F32)
            grad = base[rows, cols] + total * inv
            dbranch = (ADD_COEF * grad).astype(BF16)
            dbr[rows, cols] = dbranch
            product = dbranch.astype(F32) * total
            sums = sums + jnp.sum(product.reshape(4, 8, high - low), axis=0)
        dot_rows[:, cols] = jnp.broadcast_to(
            jnp.sum(sums, axis=0, keepdims=True), (8, high - low)
        )
    row = lax.broadcasted_iota(jnp.int32, (HP, 1), 0)

    def second_grad(slab):
        value = dot(hid[pl.ds(slab * 4, 4)].reshape(4 * HP, PIX), dbr[...], NN)
        for j in range(4):
            block = value[j * HP : (j + 1) * HP]
            block = jnp.where(row == HALF, dot_rows[0:1], block)
            pack(block, gb, (slab, j))

    def first_grad(slab):
        for j in range(4):
            value = pre[slab * 4 + j]
            sig = jax.nn.sigmoid(value)
            slope = sig * (1.0 + value * (1.0 - sig))
            grad = dh[j * 4 + slab]
            dpre[j] = (grad * gain[slab * 4 + j] * slope * SILU_GAIN).astype(BF16)
        value = dot(dpre[...].reshape(4 * HP, PIX), s_tok[...], NN)
        for j in range(4):
            pack(value[j * HP : (j + 1) * HP], ga, (slab, j))

    def hidden_grad(i, _):
        dh[pl.ds(i * 4, 4)] = dot(wb[i].reshape(4 * HP, CP), dbn[...], NT).reshape(4, HP, PIX)
        return 0

    def scatter_far(s, d):
        s.got_half[d] = send(
            s.g.at[at2(s, 2), at1(s, d)], s.half2.at[d], s.p2(1 if d < 2 else 3)
        )

    def scatter_near(s, d):
        way, e = (1, 3) if d < 2 else (0, 1)
        s.got_full[way, d] = send(
            s.g.at[at2(s, e), at1(s, d)], s.full2.at[way, d], s.p2(e)
        )

    def scatter_relay(s, d):
        s.got_half[d].wait_recv()
        way, e = (0, 1) if d < 2 else (1, 3)
        spot = (at2(s, e), at1(s, d))
        s.g[spot] = (s.g[spot].astype(F32) + s.half2[d].astype(F32)).astype(BF16)
        s.got_full[way, d] = send(s.g.at[spot[0], spot[1]], s.full2.at[way, d], s.p2(e))

    def scatter_sum(s, d):
        s.got_full[0, d].wait_recv()
        s.got_full[1, d].wait_recv()
        spot = (s.i2, at1(s, d))
        total = (
            s.g[spot].astype(F32) + s.full2[0, d].astype(F32) + s.full2[1, d].astype(F32)
        )
        if d == 0:
            s.own = total
        else:
            s.g[spot] = total.astype(BF16)

    def ring_far(s):
        spot = s.g.at[s.i2, at1(s, 2)]
        low, high = pl.ds(0, s.cut[1]), pl.ds(s.cut[1], s.cut[1])
        s.far_up = send(spot.at[low], s.half1.at[low], s.p1(1))
        s.far_down = send(spot.at[high], s.half1.at[high], s.p1(3))

    def ring_near(s, d):
        low, high = pl.ds(0, s.cut[1]), pl.ds(s.cut[1], s.cut[1])
        part, way = (high, 0) if d == 1 else (low, 1)
        s.near.append(send(s.g.at[s.i2, at1(s, d), part], s.full1.at[way, part], s.p1(d)))

    def ring_relay(s, d):
        part, way, copy = (
            (slice(0, s.cut[1]), 0, s.far_up)
            if d == 1
            else (slice(s.cut[1], 2 * s.cut[1]), 1, s.far_down)
        )
        copy.wait_recv()
        at = at1(s, d)
        s.g[s.i2, at, part] = (
            s.g[s.i2, at, part].astype(F32) + s.half1[part].astype(F32)
        ).astype(BF16)
        rows = pl.ds(part.start, part.stop - part.start)
        s.near.append(send(s.g.at[s.i2, at, rows], s.full1.at[way, rows], s.p1(d)))

    def ring_sum(s):
        for copy in s.near:
            copy.wait_recv()
        return s.own + s.full1[0].astype(F32) + s.full1[1].astype(F32)

    sides = {"a": a, "b": b}
    for s in (a, b):
        s.got_half, s.got_full, s.near = {}, {}, []
    steps = {
        "far": scatter_far,
        "near": scatter_near,
        "relay": scatter_relay,
        "sum": scatter_sum,
        "ring_far": ring_far,
        "ring_near": ring_near,
        "ring_relay": ring_relay,
    }
    def hand_out(out, zs, zr):
        for q in range(ROWS):
            first = q * CHAN_PAD
            zs[q] = fold(out[:, first : first + CHAN]).astype(BF16)
        zr[r] = zs[r]
        return [
            send(zs.at[((z + dz) % 4) * 2 + (c + dc) % 2], zr.at[r], peer(dz=dz, dc=dc))
            for dz, dc in group
        ]

    def finish_second():
        grad2 = unpack(ring_sum(b))
        w2 = wb[x, y].astype(F32)
        inv2 = norm_row[1][0:1]
        dot2 = grad2[HALF : HALF + 1]
        return hand_out(grad2 * inv2 - w2 * (dot2 * inv2 * inv2 * inv2), zs2, zr2)

    def finish_first():
        grad1 = unpack(ring_sum(a))
        w1 = wa[y, x].astype(F32)
        inv1 = lax.rsqrt(jnp.sum(w1 * w1, axis=1, keepdims=True) + 1.0)
        dot1 = jnp.sum(w1 * grad1, axis=1, keepdims=True)
        return hand_out(grad1 * inv1 - w1 * (dot1 * inv1 * inv1 * inv1), zs1, zr1)

    for step, *at in PLAN:
        if step == "hidden":
            dbn[...] = (dbr[...].astype(F32) * norm_row[1][0:1]).astype(BF16)
            lax.fori_loop(0, 4, hidden_grad, 0)
        elif step == "finish" and at[0] == "b":
            z2_copies = finish_second()
        elif step == "finish":
            z1_copies = finish_first()
        elif step == "grad":
            side = sides[at[0]]
            (first_grad if side is a else second_grad)(at2(side, at[1]))
        else:
            steps[step](sides[at[0]], *at[1:])

    for copy in z2_copies:
        copy.wait_recv()
    for core in range(2):
        value = unfold(sum(zr2[2 * q + core].astype(F32) for q in range(4)))
        out2[core * HALF : (core + 1) * HALF, 0, :] = value[:HALF]
    for copy in z1_copies:
        copy.wait_recv()
    for core in range(2):
        value = unfold(sum(zr1[2 * q + core].astype(F32) for q in range(4)))
        value = jnp.concatenate([value, jnp.zeros((HP, 256 - CHAN), F32)], axis=1)
        value = jnp.concatenate([value, jnp.zeros((128 - HP, 256), F32)], axis=0).T
        out1[0, :, core * HALF : (core + 1) * HALF] = value[:CHAN, :HALF]
    for copy in started:
        copy.wait_send()


def local(clean, noise, bucket, mod_table, w_first, w_second):
    vmem = pl.BlockSpec(memory_space=pltpu.VMEM)
    smem = pl.BlockSpec(memory_space=pltpu.SMEM)
    hbm = pl.BlockSpec(memory_space=pl.ANY)
    block = (HP, CP)
    first, second = pl.pallas_call(
        kernel,
        out_shape=(
            jax.ShapeDtypeStruct((1, CHAN, BLOCK), F32),
            jax.ShapeDtypeStruct((BLOCK, 1, CHAN), F32),
        ),
        in_specs=[hbm, hbm, smem, hbm, hbm, hbm],
        out_specs=(vmem, vmem),
        scratch_shapes=[
            pltpu.VMEM(clean.shape, F32),
            pltpu.VMEM(noise.shape, F32),
            pltpu.VMEM((BUCKETS, WIDTH), F32),
            pltpu.VMEM((CHAN, BLOCK), F32),
            pltpu.VMEM((BLOCK, CHAN), F32),
            pltpu.VMEM((2, FOLD, 128), BF16),
            pltpu.VMEM((2, FOLD, 128), BF16),
            pltpu.VMEM((ROWS, FOLD, 128), BF16),
            pltpu.VMEM((ROWS, FOLD, 128), BF16),
            pltpu.VMEM((4, CHAN_PAD, PIX), BF16),
            pltpu.VMEM((4, CHAN_PAD, PIX), BF16),
            pltpu.VMEM((ROWS, CHAN_PAD, PIX), BF16),
            pltpu.VMEM((ROWS, CHAN_PAD, PIX), BF16),
            pltpu.VMEM((PIX, CP), BF16),
            pltpu.VMEM((PIX, CP), F32),
            pltpu.VMEM((4, 4, *block), BF16),
            pltpu.VMEM((4, 4, *block), BF16),
            pltpu.VMEM((4, 4, SIZE_W, 128), BF16),
            pltpu.VMEM((4, 4, SIZE_W, 128), BF16),
            pltpu.VMEM((4, 4, SIZE_W, 128), BF16),
            pltpu.VMEM((4, 4, SIZE_G, 128), BF16),
            pltpu.VMEM((4, SIZE_W, 128), BF16),
            pltpu.VMEM((2, 4, SIZE_W, 128), BF16),
            pltpu.VMEM((SIZE_W, 128), BF16),
            pltpu.VMEM((2, SIZE_W, 128), BF16),
            pltpu.VMEM((4, SIZE_G, 128), BF16),
            pltpu.VMEM((2, 4, SIZE_G, 128), BF16),
            pltpu.VMEM((SIZE_G, 128), BF16),
            pltpu.VMEM((2, SIZE_G, 128), BF16),
            pltpu.VMEM((16, HP, PIX), F32),
            pltpu.VMEM((16, HP, PIX), F32),
            pltpu.VMEM((16, HP, PIX), BF16),
            pltpu.VMEM((4, HP, PIX), BF16),
            pltpu.VMEM((PIX, CP), F32),
            pltpu.VMEM((PIX, CP), BF16),
            pltpu.VMEM((PIX, CP), BF16),
            pltpu.VMEM((2, 8, CP), F32),
            pltpu.VMEM((8, CP), F32),
            pltpu.VMEM((PIX, CP), BF16),
            pltpu.VMEM((PIX, CP), BF16),
            pltpu.VMEM((8, CP), F32),
            pltpu.VMEM((16, HP, PIX), F32),
            pltpu.VMEM((ROWS, FOLD, 128), BF16),
            pltpu.VMEM((ROWS, FOLD, 128), BF16),
            pltpu.VMEM((ROWS, FOLD, 128), BF16),
            pltpu.VMEM((ROWS, FOLD, 128), BF16),
            pltpu.SemaphoreType.DMA((5,)),
            pltpu.SemaphoreType.DMA((MAX_COPIES,)),
            pltpu.SemaphoreType.DMA((MAX_COPIES,)),
        ],
        compiler_params=pltpu.CompilerParams(
            collective_id=0, has_side_effects=True, vmem_limit_bytes=60 * 1024 * 1024
        ),
    )(clean, noise, bucket, mod_table, w_first, jnp.transpose(w_second, (1, 0, 2)))
    return first / SAMPLES, jnp.transpose(second / SAMPLES, (1, 0, 2))


def solution(mesh):
    in_specs = (
        P("row", "col"),
        P("row", "col"),
        P(),
        P(),
        P(None, "row", "col"),
        P(None, "col", "row"),
    )
    out_specs = (P(None, "row", "col"), P(None, "col", "row"))
    return jax.shard_map(local, mesh=mesh, in_specs=in_specs, out_specs=out_specs, check_vma=False)
```

```python
import math

import jax
import jax.numpy as jnp
from jax import lax
from jax.experimental import pallas as pl
from jax.experimental.pallas import tpu as pltpu
from jax.sharding import PartitionSpec as P

MESH = pl.DeviceIdType.MESH
F32 = jnp.float32
BF16 = jnp.bfloat16

WIDTH = 1344
PIX = 256
SAMPLES = 64
BUCKETS = 32
MIX_WEIGHT = 0.3
KEEP_COEF = (1.0 - MIX_WEIGHT) / math.sqrt((1.0 - MIX_WEIGHT) ** 2 + MIX_WEIGHT**2)
ADD_COEF = MIX_WEIGHT / math.sqrt((1.0 - MIX_WEIGHT) ** 2 + MIX_WEIGHT**2)
SILU_GAIN = 1.0 / 0.596

ROWS = 8
CHAN = WIDTH // ROWS
CHAN_PAD = 176
CP = 1408
BLOCK = WIDTH // 16
HALF = BLOCK // 2
HP = 48
HT = 16 * HP
STRIPS = CP // 128
FULL = 40
LAST = CP - 128
BELOW = 24
SIZE_W = (STRIPS - 1) * FULL + BELOW + 24
SIZE_G = (STRIPS - 1) * FULL + BELOW + 40
FOLD = HALF + HALF // 3
CUTS = ((0, 512), (512, 1024), (1024, 1408))
NN = (((1,), (0,)), ((), ()))
NT = (((1,), (1,)), ((), ()))
TN = (((0,), (0,)), ((), ()))
SENDS, LANDINGS = 12, 54
FAR = (2, 1, 0, 3)
PLAN = (
    ("grad", "b", 2, FAR),
    ("hidden",),
    ("grad", "a", 2, (1, 2)),
    ("grad", "a", 1),
    ("grad", "b", 3),
    ("far", "a", 3),
    ("near", "a", 2),
    ("grad", "a", 3),
    ("grad", "b", 1),
    ("near", "b", 2),
    ("far", "a", 0),
    ("grad", "a", 0),
    ("relay", "b", 2),
    ("relay", "a", 2),
    ("relay", "a", 1),
    ("relay", "b", 3),
    ("near", "b", 1),
    ("near", "b", 3),
    ("relay", "b", 1),
    ("grad", "b", 0),
    ("near", "a", 1),
    ("sum", "b", 2),
    ("ring_far", "b"),
    ("sum", "a", 2),
    ("relay", "b", 0),
    ("near", "a", 3),
    ("ring_far", "a"),
    ("near", "b", 0),
    ("relay", "a", 3),
    ("sum", "b", 3),
    ("sum", "b", 1),
    ("ring_near", "b", 1),
    ("ring_near", "b", 3),
    ("ring_relay", "b", 3),
    ("sum", "a", 1),
    ("ring_relay", "b", 1),
    ("near", "a", 0),
    ("relay", "a", 0),
    ("ring_near", "a", 1),
    ("sum", "a", 3),
    ("ring_relay", "a", 3),
    ("ring_near", "a", 3),
    ("ring_relay", "a", 1),
    ("sum", "b", 0),
    ("finish", "b"),
    ("sum", "a", 0),
    ("finish", "a"),
)
GATHER = (
    ("first", "a", 1),
    ("first", "a", 3),
    ("spread", "a", 1),
    ("first", "b", 3),
    ("first", "b", 1),
    ("spread", "b", 3),
    ("spread", "a", 3),
    ("spread", "b", 1),
    ("halves", "b"),
    ("halves", "a"),
    ("share", "s"),
    ("on", "b", 0),
    ("pair", "a", 3),
    ("on", "a", 1),
    ("on", "a", 0),
    ("on", "a", 3),
    ("on", "b", 3),
    ("own",),
    ("share", "t"),
    ("on", "a", 2),
    ("pair", "a", 1),
    ("on", "b", 1),
    ("on", "b", 2),
    ("above",),
    ("pair", "b", 3),
    ("below",),
    ("pair", "b", 1),
    ("near",),
    ("target",),
    ("early",),
    ("far", "a"),
    ("opposite",),
    ("far", "b"),
    ("last",),
)


def dot(a, b, dims):
    return lax.dot_general(a, b, dims, preferred_element_type=F32)


def fold(block):
    third, rest = HALF // 3, CHAN - 128
    below = [block[i * third : (i + 1) * third, 128:CHAN] for i in range(3)]
    below.append(jnp.zeros((third, 128 - 3 * rest), F32))
    return jnp.concatenate([block[:HALF, :128], jnp.concatenate(below, axis=1)], axis=0)


def unfold(block):
    rest = CHAN - 128
    right = [block[HALF:, i * rest : (i + 1) * rest] for i in range(3)]
    return jnp.concatenate([block[:HALF], jnp.concatenate(right, axis=0)], axis=1)


def pack(block, ref, at):
    size = ref.shape[-2]
    whole = (STRIPS - 1) * FULL
    left = (size - whole - BELOW) // STRIPS
    rest = []
    for j in range(STRIPS):
        lanes = slice(128 * j, 128 * (j + 1))
        if j < STRIPS - 1:
            ref[(*at, slice(FULL * j, FULL * (j + 1)))] = block[:FULL, lanes].astype(BF16)
        rest.append(block[FULL : FULL + left, lanes])
    end = block[:FULL, LAST : LAST + 64]
    short = jnp.zeros((2 * BELOW - FULL, 64), F32)
    end = jnp.concatenate([end[:BELOW], jnp.concatenate([end[BELOW:], short], axis=0)], axis=1)
    ref[(*at, slice(whole, whole + BELOW))] = end.astype(BF16)
    rest.append(jnp.zeros((size - whole - BELOW - left * STRIPS, 128), F32))
    ref[(*at, slice(whole + BELOW, size))] = jnp.concatenate(rest, axis=0).astype(BF16)


def unpack(strips):
    whole = (STRIPS - 1) * FULL
    left = (strips.shape[0] - whole - BELOW) // STRIPS
    fill = jnp.zeros((HP - FULL - left, 128), F32)
    end = strips[whole : whole + BELOW]
    end = jnp.concatenate([end[:, :64], end[: FULL - BELOW, 64:]], axis=0)
    end = jnp.concatenate([end, jnp.zeros((FULL, 64), F32)], axis=1)
    parts = []
    for j in range(STRIPS):
        first = whole + BELOW + left * j
        rest = jnp.concatenate([strips[first : first + left], fill], axis=0)
        strip = strips[FULL * j : FULL * (j + 1)] if j < STRIPS - 1 else end
        parts.append(jnp.concatenate([strip, rest], axis=0))
    return jnp.concatenate(parts, axis=1)


def kernel(
    clean_hbm, noise_hbm, bucket, mod_hbm, w1_hbm, w2_hbm, out1, out2,
    clean, noise, mod, w1_in, w2_in, w1_out, w2_out, w1_got, w2_got,
    st, tg, s_all, t_all, s_full, s_tok, base, wa, wb, wa_strips, wb_strips, ga, gb,
    ra1, ra2, rx1, rx2, rb1, rb2, ry1, ry2,
    gain, pre, hid, dpre, raw, raw_out, raw_in, norm_row, norm_in,
    dbr, dbn, dot_rows, far_grad, zs1, zs2, zr1, zr2, load_sems, send_sems, recv_sems,
):
    r = lax.axis_index("row")
    k = lax.axis_index("col")
    z, c = r // 2, r % 2
    y, x = k // 4, k % 4

    def peer(dz=0, dc=0, dy=0, dx=0):
        return (
            ((z + dz) % 4) * 2 + (c + dc) % 2,
            ((y + dy) % 4) * 4 + (x + dx) % 4,
        )

    out_names, in_names = [], []

    def place(names, name):
        if name not in names:
            names.append(name)
        return names.index(name)

    def copy_of(src, dst, device, out, into):
        return pltpu.make_async_remote_copy(
            src_ref=src,
            dst_ref=dst,
            send_sem=send_sems.at[place(out_names, out)],
            recv_sem=recv_sems.at[place(in_names, into)],
            device_id=device,
            device_id_type=MESH,
        )

    def send(src, dst, device, out, into):
        copy_of(src, dst, device, out, into).start()

    def landed(name, view):
        copy_of(view, view, peer(dc=1), out_names[0], name).wait_recv()

    def sent(name, view):
        copy_of(view, view, peer(dc=1), name, in_names[0]).wait_send()

    group = [(dz, dc) for dz in (2, 1, 3, 0) for dc in (0, 1) if (dz, dc) != (0, 0)]
    barrier = pltpu.get_barrier_semaphore()
    near = [peer(dz=dz, dc=dc) for dz, dc in group]
    near += [peer(dx=1), peer(dx=3), peer(dy=1), peer(dy=3)]
    for device in near:
        pl.semaphore_signal(barrier, inc=1, device_id=device, device_id_type=MESH)

    loads = [
        pltpu.make_async_copy(src, dst, load_sems.at[i])
        for i, (src, dst) in enumerate(
            (
                (w1_hbm.at[0], w1_in),
                (w2_hbm.at[:, 0], w2_in),
                (clean_hbm, clean),
                (noise_hbm, noise),
                (mod_hbm.at[0], mod),
            )
        )
    ]
    loads[0].start()
    loads[1].start()

    hid_of = lax.broadcasted_iota(jnp.int32, (HP, BLOCK), 0)
    col_of = lax.broadcasted_iota(jnp.int32, (HP, BLOCK), 1)

    picks = [(col_of == hid_of + HALF * core) & (hid_of < HALF) for core in range(2)]
    picks = [jnp.where(pick, 1.0, 0.0).astype(BF16) for pick in picks]

    def cut_weights(load, source, dims, out):
        load.wait()
        value = source[...].astype(BF16)
        for core in range(2):
            out[core] = fold(dot(picks[core], value, dims)).astype(BF16)

    def send_weights(out, got, name):
        for dz, dc in group:
            send(out.at[(c + dc) % 2], got.at[r], peer(dz=dz, dc=dc), name, name)
        got[r] = out[c]

    cut_weights(loads[0], w1_in, NT, w1_out)
    for load in loads[2:]:
        load.start()
    def state_piece(d):
        zq = (z + d) % 4
        level_of = jnp.full((1, PIX), bucket[k * 4 + zq], jnp.int32).astype(F32)
        level = jnp.exp(-3.0 + 5.0 * (level_of + 0.5) / BUCKETS)
        spread = jnp.sqrt(level * level + 0.25)
        cols = pl.ds(pl.multiple_of(zq * PIX, PIX), PIX)
        cl = clean[:, cols]
        no = noise[:, cols]
        pad = jnp.zeros((CHAN_PAD - CHAN, PIX), F32)
        state = (cl + level * no) / spread
        target = cl * (2.0 * level / spread) - no * (0.5 / spread)
        return (
            jnp.concatenate([state, pad], axis=0).astype(BF16),
            jnp.concatenate([target, pad], axis=0).astype(BF16),
        )

    pl.semaphore_wait(barrier, len(near))

    send_weights(w1_out, w1_got, "w1")
    cut_weights(loads[1], w2_in, NN, w2_out)
    send_weights(w2_out, w2_got, "w2")
    loads[2].wait()
    loads[3].wait()
    loads[4].wait()
    for d in range(4):
        state, target = state_piece(d)
        st[d] = state
        tg[d] = target
    s_all[r] = st[0]
    t_all[r] = tg[0]
    for own, everyone, name in ((st, s_all, "s"), (tg, t_all, "t")):
        for d in (2, 1, 3):
            send(own.at[d], everyone.at[r], peer(dz=d), name, name)
        send(own.at[0], everyone.at[r], peer(dc=1), name, name + "2")

    def share(everyone, name):
        landed(name, everyone.at[pl.ds(0, 3)])
        for d in (2, 1, 3):
            slot = everyone.at[((z - d) % 4) * 2 + c]
            send(slot, slot, peer(dc=1), name, name + "2")

    sample = k * 4 + z
    picked = lax.broadcasted_iota(jnp.int32, (BUCKETS, WIDTH), 0) == bucket[sample]
    mod_row = jnp.sum(jnp.where(picked, 1.0 + mod[...], 0.0), axis=0, keepdims=True)
    mod_row = jnp.concatenate([mod_row, jnp.zeros((1, CP - WIDTH), F32)], axis=1)
    for b in range(16):
        first = (BLOCK * b // 128) * 128
        lane = lax.broadcasted_iota(jnp.int32, (HP, 256), 1) + first
        row = lax.broadcasted_iota(jnp.int32, (HP, 256), 0)
        take = (lane == row + (BLOCK * b + HALF * c)) & (row < HALF)
        window = jnp.broadcast_to(mod_row[:, first : first + 256], (HP, 256))
        value = jnp.sum(jnp.where(take, window, 0.0), axis=1, keepdims=True)
        gain[b] = jnp.broadcast_to(value, (HP, PIX))

    class Side:
        pass

    def side_a():
        s = Side()
        s.ag, s.rs = "ag_a", "rs_a"
        s.w, s.full, s.g, s.i1, s.i2 = wa_strips, wa, ga, x, y
        s.p1 = lambda d: peer(dx=d)
        s.p2 = lambda d: peer(dy=d)
        s.cut = (SIZE_W // 2, SIZE_W // 2)
        s.half1, s.half2, s.full1, s.full2 = rx1, ra1, rx2, ra2
        return s

    def side_b():
        s = Side()
        s.ag, s.rs = "ag_b", "rs_b"
        s.w, s.full, s.g, s.i1, s.i2 = wb_strips, wb, gb, y, x
        s.p1 = lambda d: peer(dy=d)
        s.p2 = lambda d: peer(dx=d)
        s.cut = (SIZE_W // 2, SIZE_G // 2)
        s.half1, s.half2, s.full1, s.full2 = ry1, rb1, ry2, rb2
        return s

    a, b = side_a(), side_b()

    def at1(s, d):
        return (s.i1 + d) % 4

    def at2(s, d):
        return (s.i2 + d) % 4

    def spot(s, d2, d1):
        return at2(s, d2) * 4 + at1(s, d1)

    def spread_out(s, d):
        block = s.w.at[spot(s, 0, d)]
        for e in (1, 3):
            onward = (e == 1) == (d < 2)
            name = (s.ag, "on", d) if onward else (s.ag, "pair", e)
            send(block, block, s.p2(e), s.ag, name)

    for s, name, got in ((a, "w1", w1_got), (b, "w2", w2_got)):
        landed(name, got.at[pl.ds(0, ROWS - 1)])
        parts = [unfold(got[q].astype(F32)) for q in range(ROWS)]
        parts.append(jnp.zeros((HALF, CP - WIDTH), F32))
        whole = jnp.concatenate(parts, axis=1)
        whole = jnp.concatenate([whole, jnp.zeros((HP - HALF, CP), F32)], axis=0)
        pack(whole, s.w, (spot(s, 0, 0),))
        block = s.w.at[spot(s, 0, 0)]
        for d in (1, 3):
            send(block, block, s.p1(d), s.ag, (s.ag, "first", d))
        spread_out(s, 0)
        s.full[s.i2, s.i1] = whole.astype(BF16)

    def pass_first(s, d):
        landed((s.ag, "first", d), s.w.at[0])
        first = 0 if d == 1 else s.cut[0]
        block = s.w.at[spot(s, 0, 4 - d), pl.ds(first, s.cut[0])]
        send(block, block, s.p1(d), s.ag, (s.ag, "halves"))

    def meet_halves(s):
        landed((s.ag, "halves"), s.w.at[0])
        spread_out(s, 2)

    def spread(s, d2, blocks):
        for d in blocks:
            at = (at2(s, d2), at1(s, d))
            s.full[at] = unpack(s.w[spot(s, d2, d)].astype(F32)).astype(BF16)

    def first_half(slab):
        weights = wa[slab].reshape(4 * HP, CP)
        value = dot(weights, s_full[...], NN).reshape(4, HP, PIX)
        for j in range(4):
            block = wa[slab, j].astype(F32)
            squares = jnp.sum(block * block, axis=1, keepdims=True)
            inv = jnp.broadcast_to(lax.rsqrt(squares + 1.0), (HP, PIX))
            act = value[j] * inv
            pre[slab * 4 + j] = act
            hidden = act * jax.nn.sigmoid(act) * SILU_GAIN * gain[slab * 4 + j]
            hid[j * 4 + slab] = hidden.astype(BF16)

    def pass_on(s, d):
        landed((s.ag, "on", d), s.w.at[0])
        e = 1 if d < 2 else 3
        block = s.w.at[spot(s, 4 - e, d)]
        send(block, block, s.p2(e), s.ag, (s.ag, "far"))

    def squares_of(slab):
        total = jnp.zeros((8, CP), F32)
        for j in range(4):
            block = wb[slab, j].astype(F32)
            total = total + jnp.sum((block * block).reshape(HP // 8, 8, CP), axis=0)
        return total

    def states_of(blocks):
        return jnp.concatenate([hid[i * 4 + j] for i, j in blocks], axis=0).T

    def branch(states, blocks, cols):
        weights = jnp.concatenate([wb[i, j, :, cols] for i, j in blocks], axis=0)
        return dot(states, weights, NN)

    def all_channels(blocks):
        parts = [blocks[q].astype(F32)[:CHAN] for q in range(ROWS)]
        parts.append(jnp.zeros((CP - WIDTH, PIX), F32))
        return jnp.concatenate(parts, axis=0).astype(BF16)

    def own_slab():
        landed("s2", s_all.at[pl.ds(0, 4)])
        s_full[...] = all_channels(s_all)
        spread(a, 0, (1, 2, 3))
        first_half(y)
        s_tok[...] = s_full[...].T

    def other_slab(d):
        spread(a, d, range(4))
        first_half(at2(a, d))

    def target_part():
        landed("t2", t_all.at[pl.ds(0, 4)])
        base[...] = KEEP_COEF * s_tok[...].astype(F32) - all_channels(t_all).T.astype(F32)

    def near_slabs():
        spread(b, 0, (1, 2, 3))
        spread(b, 1, range(4))
        spread(b, 3, range(4))
        norm_row[0] = squares_of(x) + squares_of(at2(b, 1)) + squares_of(at2(b, 3))

    def early_branch():
        blocks = [(at2(b, i), at2(a, j)) for i in (0, 1, 3) for j in (0, 1, 3)]
        states = states_of(blocks)
        for cut in CUTS:
            cols = slice(*cut)
            raw[:, cols] = branch(states, blocks, cols)

    def last_slab():
        spread(b, 2, range(4))
        norm_row[0] += squares_of(at2(b, 2))
        send(norm_row.at[0], norm_in, peer(dc=1), "norm", "norm")

    sides = {"a": a, "b": b}
    steps = {
        "first": pass_first,
        "spread": spread_out,
        "halves": meet_halves,
        "on": pass_on,
        "pair": lambda s, e: landed((s.ag, "pair", e), s.w.at[pl.ds(0, 2)]),
        "far": lambda s: landed((s.ag, "far"), s.w.at[pl.ds(0, 4)]),
        "own": own_slab,
        "below": lambda: other_slab(3),
        "above": lambda: other_slab(1),
        "opposite": lambda: other_slab(2),
        "target": target_part,
        "near": near_slabs,
        "early": early_branch,
        "last": last_slab,
    }
    for step, *at in GATHER:
        if step == "share":
            share(s_all if at[0] == "s" else t_all, at[0])
        else:
            steps[step](*(sides.get(q, q) for q in at))
    late = [(at2(b, i), at2(a, 2)) for i in (0, 1, 3)] + [(at2(b, 2), j) for j in range(4)]
    states = states_of(late)
    for i, cut in enumerate(CUTS):
        cols = slice(*cut)
        value = raw[:, cols] + branch(states, late, cols)
        raw[:, cols] = value
        raw_out[:, cols] = value.astype(BF16)
        part = pl.ds(cut[0], cut[1] - cut[0])
        send(raw_out.at[:, part], raw_in.at[:, part], peer(dc=1), "raw", ("raw", i))

    landed("norm", norm_in)
    norm = jnp.sum(norm_row[0] + norm_in[...], axis=0, keepdims=True)
    inv_row = lax.rsqrt(norm + 1.0)
    norm_row[1] = jnp.broadcast_to(inv_row, (8, CP))
    far_states = jnp.concatenate([hid[spot(b, 2, d)] for d in FAR], axis=0)
    for i, (low, high) in enumerate(CUTS):
        landed(("raw", i), raw_in.at[:, pl.ds(low, high - low)])
        cols = slice(low, high)
        sums = jnp.zeros((8, high - low), F32)
        inv = norm_row[1][0:1, cols] * ADD_COEF
        for q in range(8):
            rows = slice(q * 32, (q + 1) * 32)
            total = raw[rows, cols] + raw_in[rows, cols].astype(F32)
            grad = base[rows, cols] + total * inv
            dbranch = (ADD_COEF * grad).astype(BF16)
            dbr[rows, cols] = dbranch
            product = dbranch.astype(F32) * total
            sums = sums + jnp.sum(product.reshape(4, 8, high - low), axis=0)
        dot_rows[:, cols] = jnp.broadcast_to(
            jnp.sum(sums, axis=0, keepdims=True), (8, high - low)
        )
        far_grad[:, cols] = dot(far_states, dbr[:, cols], NN)
    row = lax.broadcasted_iota(jnp.int32, (HP, 1), 0)

    def second_grad(d2, first=()):
        order = (*first, *(d for d in range(4) if d not in first))
        places = [spot(b, d2, d) for d in order]
        if d2 == 2:
            value = far_grad[...]
        else:
            value = dot(jnp.concatenate([hid[i] for i in places], axis=0), dbr[...], NN)
        for j, d in enumerate(order):
            block = value[j * HP : (j + 1) * HP]
            block = jnp.where(row == HALF, dot_rows[0:1], block)
            pack(block, gb, (places[j],))
            if d in first:
                scatter_far(b, d)

    def first_grad(d2, first=()):
        slab = at2(a, d2)
        order = (*first, *(d for d in range(4) if d not in first))
        at = [at1(a, d) for d in order]
        weights = jnp.concatenate([wb[i, slab] for i in at], axis=0)
        back = dot(weights, dbn[...], NT).reshape(4, HP, PIX)
        for j in range(4):
            value = pre[slab * 4 + at[j]]
            sig = jax.nn.sigmoid(value)
            slope = sig * (1.0 + value * (1.0 - sig))
            dpre[j] = (back[j] * gain[slab * 4 + at[j]] * slope * SILU_GAIN).astype(BF16)
        value = dot(dpre[...].reshape(4 * HP, PIX), s_tok[...], NN)
        for j, d in enumerate(order):
            pack(value[j * HP : (j + 1) * HP], ga, (slab * 4 + at[j],))
            if d in first:
                scatter_far(a, d)

    def scatter_far(s, d):
        e = 1 if d < 2 else 3
        send(s.g.at[spot(s, 2, d)], s.half2.at[d], s.p2(e), s.rs, (s.rs, "half", d))

    def scatter_on(s, d, e):
        way = 0 if e == 1 else 1
        send(s.g.at[spot(s, e, d)], s.full2.at[way, d], s.p2(e), s.rs, (s.rs, "full", d))

    def scatter_near(s, d):
        scatter_on(s, d, 3 if d < 2 else 1)

    def scatter_relay(s, d):
        landed((s.rs, "half", d), s.half2.at[0])
        e = 1 if d < 2 else 3
        at = spot(s, e, d)
        s.g[at] = (s.g[at].astype(F32) + s.half2[d].astype(F32)).astype(BF16)
        scatter_on(s, d, e)

    def scatter_sum(s, d):
        landed((s.rs, "full", d), s.full2.at[0, pl.ds(0, 2)])
        at = spot(s, 0, d)
        total = s.g[at].astype(F32) + s.full2[0, d].astype(F32) + s.full2[1, d].astype(F32)
        if d == 0:
            s.own = total
        else:
            s.g[at] = total.astype(BF16)

    def ring_on(s, d, part):
        way = 0 if d == 1 else 1
        rows = pl.ds(part * s.cut[1], s.cut[1])
        send(s.g.at[spot(s, 0, d), rows], s.full1.at[way, rows], s.p1(d), s.rs, (s.rs, "near"))

    def ring_far(s):
        for part, d in enumerate((1, 3)):
            rows = pl.ds(part * s.cut[1], s.cut[1])
            send(s.g.at[spot(s, 0, 2), rows], s.half1.at[rows], s.p1(d), s.rs, (s.rs, "far", d))

    def ring_near(s, d):
        ring_on(s, d, 1 if d == 1 else 0)

    def ring_relay(s, d):
        part = 0 if d == 1 else 1
        rows = slice(part * s.cut[1], (part + 1) * s.cut[1])
        landed((s.rs, "far", d), s.half1.at[pl.ds(0, s.cut[1])])
        at = spot(s, 0, d)
        s.g[at, rows] = (s.g[at, rows].astype(F32) + s.half1[rows].astype(F32)).astype(BF16)
        ring_on(s, d, part)

    def ring_sum(s):
        landed((s.rs, "near"), s.full1)
        return s.own + s.full1[0].astype(F32) + s.full1[1].astype(F32)

    steps = {
        "far": scatter_far,
        "near": scatter_near,
        "relay": scatter_relay,
        "sum": scatter_sum,
        "ring_far": ring_far,
        "ring_near": ring_near,
        "ring_relay": ring_relay,
    }
    def hand_out(out, zs, zr, name):
        for q in range(ROWS):
            first = q * CHAN
            zs[q] = fold(out[:, first : first + CHAN]).astype(BF16)
        for dz, dc in group:
            slot = zs.at[((z + dz) % 4) * 2 + (c + dc) % 2]
            send(slot, zr.at[r], peer(dz=dz, dc=dc), name, name)
        zr[r] = zs[r]

    def finish_second():
        inv2 = norm_row[1][0:1]
        scaled = wb[x, y].astype(F32) * (inv2 * inv2 * inv2)
        grad2 = unpack(ring_sum(b))
        hand_out(grad2 * inv2 - scaled * grad2[HALF : HALF + 1], zs2, zr2, "z2")

    def finish_first():
        w1 = wa[y, x].astype(F32)
        inv1 = lax.rsqrt(jnp.sum(w1 * w1, axis=1, keepdims=True) + 1.0)
        scaled = w1 * (inv1 * inv1 * inv1)
        grad1 = unpack(ring_sum(a))
        dot1 = jnp.sum(w1 * grad1, axis=1, keepdims=True)
        hand_out(grad1 * inv1 - scaled * dot1, zs1, zr1, "z1")

    for step, *at in PLAN:
        if step == "hidden":
            dbn[...] = (dbr[...].astype(F32) * norm_row[1][0:1]).astype(BF16)
        elif step == "finish" and at[0] == "b":
            finish_second()
        elif step == "finish":
            finish_first()
        elif step == "grad":
            side = sides[at[0]]
            (first_grad if side is a else second_grad)(*at[1:])
        else:
            steps[step](sides[at[0]], *at[1:])

    landed("z2", zr2.at[pl.ds(0, ROWS - 1)])
    for core in range(2):
        value = unfold(sum(zr2[2 * q + core].astype(F32) for q in range(4))) / SAMPLES
        out2[core * HALF : (core + 1) * HALF, 0, :] = value
    landed("z1", zr1.at[pl.ds(0, ROWS - 1)])
    both = [sum(zr1[2 * q + core].astype(F32) for q in range(4)) / SAMPLES for core in range(2)]
    both.append(jnp.zeros((128 - 2 * FOLD, 128), F32))
    turned = jnp.concatenate(both, axis=0).T
    third, rest = HALF // 3, CHAN - 128
    top, bottom = [], []
    for core in range(2):
        first = core * FOLD
        top.append(turned[:, first : first + HALF])
        for i in range(3):
            lanes = slice(first + HALF, first + FOLD)
            bottom.append(turned[i * rest : (i + 1) * rest, lanes])
    out1[0, :128, :] = jnp.concatenate(top, axis=1)
    out1[0, 128:, :] = jnp.concatenate(bottom, axis=1)
    for name, view in (("w1", w1_got), ("w2", w2_got), ("s", s_all), ("t", t_all), ("z1", zs1), ("z2", zs2)):
        sent(name, view.at[pl.ds(0, ROWS - 1)])
    for s in (a, b):
        sent(s.ag, s.w.at[pl.ds(0, 15)])
        sent(s.rs, s.g.at[pl.ds(0, 15)])
    sent("norm", norm_in)
    sent("raw", raw_out)
    if (len(out_names), len(in_names)) != (SENDS, LANDINGS):
        raise ValueError((len(out_names), len(in_names)))


def write_out(first, second, out1, out2, sems):
    copies = [
        pltpu.make_async_copy(src, dst, sems.at[i])
        for i, (src, dst) in enumerate(((first, out1), (second, out2)))
    ]
    for copy in copies:
        copy.start()
    for copy in copies:
        copy.wait()


def local(clean, noise, bucket, mod_table, w_first, w_second):
    vmem = pl.BlockSpec(memory_space=pltpu.VMEM)
    smem = pl.BlockSpec(memory_space=pltpu.SMEM)
    hbm = pl.BlockSpec(memory_space=pl.ANY)
    block = (HP, CP)
    first, second = pl.pallas_call(
        kernel,
        out_shape=(
            jax.ShapeDtypeStruct((1, CHAN, BLOCK), F32),
            jax.ShapeDtypeStruct((BLOCK, 1, CHAN), F32),
        ),
        in_specs=[hbm, hbm, smem, hbm, hbm, hbm],
        out_specs=(vmem, vmem),
        scratch_shapes=[
            pltpu.VMEM(clean.shape, F32),
            pltpu.VMEM(noise.shape, F32),
            pltpu.VMEM((BUCKETS, WIDTH), F32),
            pltpu.VMEM((CHAN, BLOCK), F32),
            pltpu.VMEM((BLOCK, CHAN), F32),
            pltpu.VMEM((2, FOLD, 128), BF16),
            pltpu.VMEM((2, FOLD, 128), BF16),
            pltpu.VMEM((ROWS, FOLD, 128), BF16),
            pltpu.VMEM((ROWS, FOLD, 128), BF16),
            pltpu.VMEM((4, CHAN_PAD, PIX), BF16),
            pltpu.VMEM((4, CHAN_PAD, PIX), BF16),
            pltpu.VMEM((ROWS, CHAN_PAD, PIX), BF16),
            pltpu.VMEM((ROWS, CHAN_PAD, PIX), BF16),
            pltpu.VMEM((CP, PIX), BF16),
            pltpu.VMEM((PIX, CP), BF16),
            pltpu.VMEM((PIX, CP), F32),
            pltpu.VMEM((4, 4, *block), BF16),
            pltpu.VMEM((4, 4, *block), BF16),
            pltpu.VMEM((16, SIZE_W, 128), BF16),
            pltpu.VMEM((16, SIZE_W, 128), BF16),
            pltpu.VMEM((16, SIZE_W, 128), BF16),
            pltpu.VMEM((16, SIZE_G, 128), BF16),
            pltpu.VMEM((4, SIZE_W, 128), BF16),
            pltpu.VMEM((2, 4, SIZE_W, 128), BF16),
            pltpu.VMEM((SIZE_W, 128), BF16),
            pltpu.VMEM((2, SIZE_W, 128), BF16),
            pltpu.VMEM((4, SIZE_G, 128), BF16),
            pltpu.VMEM((2, 4, SIZE_G, 128), BF16),
            pltpu.VMEM((SIZE_G, 128), BF16),
            pltpu.VMEM((2, SIZE_G, 128), BF16),
            pltpu.VMEM((16, HP, PIX), F32),
            pltpu.VMEM((16, HP, PIX), F32),
            pltpu.VMEM((16, HP, PIX), BF16),
            pltpu.VMEM((4, HP, PIX), BF16),
            pltpu.VMEM((PIX, CP), F32),
            pltpu.VMEM((PIX, CP), BF16),
            pltpu.VMEM((PIX, CP), BF16),
            pltpu.VMEM((2, 8, CP), F32),
            pltpu.VMEM((8, CP), F32),
            pltpu.VMEM((PIX, CP), BF16),
            pltpu.VMEM((PIX, CP), BF16),
            pltpu.VMEM((8, CP), F32),
            pltpu.VMEM((4 * HP, CP), F32),
            pltpu.VMEM((ROWS, FOLD, 128), BF16),
            pltpu.VMEM((ROWS, FOLD, 128), BF16),
            pltpu.VMEM((ROWS, FOLD, 128), BF16),
            pltpu.VMEM((ROWS, FOLD, 128), BF16),
            pltpu.SemaphoreType.DMA((5,)),
            pltpu.SemaphoreType.DMA((SENDS,)),
            pltpu.SemaphoreType.DMA((LANDINGS,)),
        ],
        compiler_params=pltpu.CompilerParams(
            collective_id=0, has_side_effects=True, vmem_limit_bytes=55040 * 1024
        ),
    )(clean, noise, bucket, mod_table, w_first, jnp.transpose(w_second, (1, 0, 2)))
    first, second = pl.pallas_call(
        write_out,
        out_shape=(
            jax.ShapeDtypeStruct(first.shape, F32),
            jax.ShapeDtypeStruct(second.shape, F32),
        ),
        in_specs=[hbm, hbm],
        out_specs=(hbm, hbm),
        scratch_shapes=[pltpu.SemaphoreType.DMA((2,))],
        compiler_params=pltpu.CompilerParams(vmem_limit_bytes=1024 * 1024),
    )(first, second)
    return first, jnp.transpose(second, (1, 0, 2))


def solution(mesh):
    in_specs = (
        P("row", "col"),
        P("row", "col"),
        P(),
        P(),
        P(None, "row", "col"),
        P(None, "col", "row"),
    )
    out_specs = (P(None, "row", "col"), P(None, "col", "row"))
    return jax.shard_map(local, mesh=mesh, in_specs=in_specs, out_specs=out_specs, check_vma=False)
```

```python
import math

import jax
import jax.numpy as jnp
from jax import lax
from jax.experimental import pallas as pl
from jax.experimental.pallas import tpu as pltpu
from jax.sharding import PartitionSpec as P

MESH = pl.DeviceIdType.MESH
F32 = jnp.float32
BF16 = jnp.bfloat16

WIDTH = 1344
PIX = 256
SAMPLES = 64
BUCKETS = 32
MIX_WEIGHT = 0.3
KEEP_COEF = (1.0 - MIX_WEIGHT) / math.sqrt((1.0 - MIX_WEIGHT) ** 2 + MIX_WEIGHT**2)
ADD_COEF = MIX_WEIGHT / math.sqrt((1.0 - MIX_WEIGHT) ** 2 + MIX_WEIGHT**2)
SILU_GAIN = 1.0 / 0.596

ROWS = 8
CHAN = WIDTH // ROWS
CHAN_PAD = 176
CP = 1408
BLOCK = WIDTH // 16
HALF = BLOCK // 2
HP = 48
HT = 16 * HP
STRIPS = CP // 128
FULL = 40
LAST = CP - 128
BELOW = 24
SIZE_W = (STRIPS - 1) * FULL + BELOW + 24
SIZE_G = (STRIPS - 1) * FULL + BELOW + 40
FOLD = HALF + HALF // 3
CUTS = ((0, 512), (512, 1024), (1024, 1408))
NN = (((1,), (0,)), ((), ()))
NT = (((1,), (1,)), ((), ()))
TN = (((0,), (0,)), ((), ()))
SENDS, LANDINGS = 12, 54
FAR = (2, 1, 0, 3)
PLAN = (
    ("grad", "b", 2, FAR),
    ("hidden",),
    ("grad", "a", 2, (1, 2)),
    ("grad", "a", 1),
    ("grad", "b", 3),
    ("far", "a", 3),
    ("near", "a", 2),
    ("grad", "a", 3),
    ("grad", "b", 1),
    ("near", "b", 2),
    ("far", "a", 0),
    ("grad", "a", 0),
    ("relay", "b", 2),
    ("relay", "a", 2),
    ("relay", "a", 1),
    ("relay", "b", 3),
    ("near", "b", 1),
    ("near", "b", 3),
    ("relay", "b", 1),
    ("grad", "b", 0),
    ("near", "a", 1),
    ("sum", "b", 2),
    ("ring_far", "b"),
    ("sum", "a", 2),
    ("relay", "b", 0),
    ("near", "a", 3),
    ("ring_far", "a"),
    ("near", "b", 0),
    ("relay", "a", 3),
    ("sum", "b", 3),
    ("sum", "b", 1),
    ("ring_near", "b", 1),
    ("ring_near", "b", 3),
    ("ring_relay", "b", 3),
    ("sum", "a", 1),
    ("ring_relay", "b", 1),
    ("near", "a", 0),
    ("relay", "a", 0),
    ("ring_near", "a", 1),
    ("sum", "a", 3),
    ("ring_relay", "a", 3),
    ("ring_near", "a", 3),
    ("ring_relay", "a", 1),
    ("sum", "b", 0),
    ("finish", "b"),
    ("sum", "a", 0),
    ("finish", "a"),
)
GATHER = (
    ("first", "a", 1),
    ("first", "a", 3),
    ("spread", "a", 1),
    ("first", "b", 3),
    ("first", "b", 1),
    ("spread", "b", 3),
    ("spread", "a", 3),
    ("spread", "b", 1),
    ("halves", "b"),
    ("halves", "a"),
    ("share", "s"),
    ("on", "b", 0),
    ("pair", "a", 3),
    ("on", "a", 1),
    ("on", "a", 0),
    ("on", "a", 3),
    ("on", "b", 3),
    ("own",),
    ("share", "t"),
    ("on", "a", 2),
    ("pair", "a", 1),
    ("on", "b", 1),
    ("on", "b", 2),
    ("above",),
    ("pair", "b", 3),
    ("below",),
    ("pair", "b", 1),
    ("near",),
    ("target",),
    ("early",),
    ("far", "a"),
    ("opposite",),
    ("far", "b"),
    ("last",),
)


def dot(a, b, dims):
    return lax.dot_general(a, b, dims, preferred_element_type=F32)


def fold(block):
    third, rest = HALF // 3, CHAN - 128
    below = [block[i * third : (i + 1) * third, 128:CHAN] for i in range(3)]
    below.append(jnp.zeros((third, 128 - 3 * rest), F32))
    return jnp.concatenate([block[:HALF, :128], jnp.concatenate(below, axis=1)], axis=0)


def unfold(block):
    rest = CHAN - 128
    right = [block[HALF:, i * rest : (i + 1) * rest] for i in range(3)]
    return jnp.concatenate([block[:HALF], jnp.concatenate(right, axis=0)], axis=1)


def pack(block, ref, at):
    size = ref.shape[-2]
    whole = (STRIPS - 1) * FULL
    left = (size - whole - BELOW) // STRIPS
    rest = []
    for j in range(STRIPS):
        lanes = slice(128 * j, 128 * (j + 1))
        if j < STRIPS - 1:
            ref[(*at, slice(FULL * j, FULL * (j + 1)))] = block[:FULL, lanes].astype(BF16)
        rest.append(block[FULL : FULL + left, lanes])
    end = block[:FULL, LAST : LAST + 64]
    short = jnp.zeros((2 * BELOW - FULL, 64), F32)
    end = jnp.concatenate([end[:BELOW], jnp.concatenate([end[BELOW:], short], axis=0)], axis=1)
    ref[(*at, slice(whole, whole + BELOW))] = end.astype(BF16)
    rest.append(jnp.zeros((size - whole - BELOW - left * STRIPS, 128), F32))
    ref[(*at, slice(whole + BELOW, size))] = jnp.concatenate(rest, axis=0).astype(BF16)


def unpack(strips):
    whole = (STRIPS - 1) * FULL
    left = (strips.shape[0] - whole - BELOW) // STRIPS
    fill = jnp.zeros((HP - FULL - left, 128), F32)
    end = strips[whole : whole + BELOW]
    end = jnp.concatenate([end[:, :64], end[: FULL - BELOW, 64:]], axis=0)
    end = jnp.concatenate([end, jnp.zeros((FULL, 64), F32)], axis=1)
    parts = []
    for j in range(STRIPS):
        first = whole + BELOW + left * j
        rest = jnp.concatenate([strips[first : first + left], fill], axis=0)
        strip = strips[FULL * j : FULL * (j + 1)] if j < STRIPS - 1 else end
        parts.append(jnp.concatenate([strip, rest], axis=0))
    return jnp.concatenate(parts, axis=1)


def kernel(
    clean_hbm, noise_hbm, bucket, mod_hbm, w1_hbm, w2_hbm, out1, out2,
    clean, noise, mod, w1_in, w2_in, w1_out, w2_out, w1_got, w2_got,
    st, tg, s_all, t_all, s_full, s_tok, base, wa, wb, wa_strips, wb_strips, ga, gb,
    ra1, ra2, rx1, rx2, rb1, rb2, ry1, ry2,
    gain, pre, hid, dpre, raw, raw_out, raw_in, norm_row, norm_in,
    dbr, dbn, dot_rows, far_grad, zs1, zs2, zr1, zr2, load_sems, send_sems, recv_sems,
):
    r = lax.axis_index("row")
    k = lax.axis_index("col")
    z, c = r // 2, r % 2
    y, x = k // 4, k % 4

    def peer(dz=0, dc=0, dy=0, dx=0):
        return (
            ((z + dz) % 4) * 2 + (c + dc) % 2,
            ((y + dy) % 4) * 4 + (x + dx) % 4,
        )

    out_names, in_names = [], []

    def place(names, name):
        if name not in names:
            names.append(name)
        return names.index(name)

    def copy_of(src, dst, device, out, into):
        return pltpu.make_async_remote_copy(
            src_ref=src,
            dst_ref=dst,
            send_sem=send_sems.at[place(out_names, out)],
            recv_sem=recv_sems.at[place(in_names, into)],
            device_id=device,
            device_id_type=MESH,
        )

    def send(src, dst, device, out, into):
        copy_of(src, dst, device, out, into).start()

    def landed(name, view):
        copy_of(view, view, peer(dc=1), out_names[0], name).wait_recv()

    def sent(name, view):
        copy_of(view, view, peer(dc=1), name, in_names[0]).wait_send()

    group = [(dz, dc) for dz in (2, 1, 3, 0) for dc in (0, 1) if (dz, dc) != (0, 0)]
    barrier = pltpu.get_barrier_semaphore()
    near = [peer(dz=dz, dc=dc) for dz, dc in group]
    near += [peer(dx=1), peer(dx=3), peer(dy=1), peer(dy=3)]
    for device in near:
        pl.semaphore_signal(barrier, inc=1, device_id=device, device_id_type=MESH)

    loads = [
        pltpu.make_async_copy(src, dst, load_sems.at[i])
        for i, (src, dst) in enumerate(
            (
                (w1_hbm.at[0], w1_in),
                (w2_hbm.at[:, 0], w2_in),
                (clean_hbm, clean),
                (noise_hbm, noise),
                (mod_hbm.at[0], mod),
            )
        )
    ]
    for load in loads:
        load.start()

    hid_of = lax.broadcasted_iota(jnp.int32, (HP, BLOCK), 0)
    col_of = lax.broadcasted_iota(jnp.int32, (HP, BLOCK), 1)

    picks = [(col_of == hid_of + HALF * core) & (hid_of < HALF) for core in range(2)]
    picks = [jnp.where(pick, 1.0, 0.0).astype(BF16) for pick in picks]

    def cut_weights(load, source, dims, out, got):
        load.wait()
        value = source[...].astype(BF16)
        for core in range(2):
            out[core] = fold(dot(picks[core], value, dims)).astype(BF16)
        got[r] = out[c]

    def send_weights(out, got, name):
        for dz, dc in group:
            send(out.at[(c + dc) % 2], got.at[r], peer(dz=dz, dc=dc), name, name)

    cut_weights(loads[0], w1_in, NT, w1_out, w1_got)
    def state_piece(d):
        zq = (z + d) % 4
        level_of = jnp.full((1, PIX), bucket[k * 4 + zq], jnp.int32).astype(F32)
        level = jnp.exp(-3.0 + 5.0 * (level_of + 0.5) / BUCKETS)
        spread = jnp.sqrt(level * level + 0.25)
        cols = pl.ds(pl.multiple_of(zq * PIX, PIX), PIX)
        cl = clean[:, cols]
        no = noise[:, cols]
        pad = jnp.zeros((CHAN_PAD - CHAN, PIX), F32)
        state = (cl + level * no) / spread
        target = cl * (2.0 * level / spread) - no * (0.5 / spread)
        return (
            jnp.concatenate([state, pad], axis=0).astype(BF16),
            jnp.concatenate([target, pad], axis=0).astype(BF16),
        )

    pl.semaphore_wait(barrier, len(near))

    send_weights(w1_out, w1_got, "w1")
    cut_weights(loads[1], w2_in, NN, w2_out, w2_got)
    send_weights(w2_out, w2_got, "w2")
    loads[2].wait()
    loads[3].wait()
    loads[4].wait()
    for d in range(4):
        state, target = state_piece(d)
        st[d] = state
        tg[d] = target
    s_all[r] = st[0]
    t_all[r] = tg[0]
    for own, everyone, name in ((st, s_all, "s"), (tg, t_all, "t")):
        for d in (2, 1, 3):
            send(own.at[d], everyone.at[r], peer(dz=d), name, name)
        send(own.at[0], everyone.at[r], peer(dc=1), name, name + "2")

    def share(everyone, name):
        landed(name, everyone.at[pl.ds(0, 3)])
        for d in (2, 1, 3):
            slot = everyone.at[((z - d) % 4) * 2 + c]
            send(slot, slot, peer(dc=1), name, name + "2")

    sample = k * 4 + z
    picked = lax.broadcasted_iota(jnp.int32, (BUCKETS, WIDTH), 0) == bucket[sample]
    mod_row = jnp.sum(jnp.where(picked, 1.0 + mod[...], 0.0), axis=0, keepdims=True)
    mod_row = jnp.concatenate([mod_row, jnp.zeros((1, CP - WIDTH), F32)], axis=1)
    for b in range(16):
        first = (BLOCK * b // 128) * 128
        lane = lax.broadcasted_iota(jnp.int32, (HP, 256), 1) + first
        row = lax.broadcasted_iota(jnp.int32, (HP, 256), 0)
        take = (lane == row + (BLOCK * b + HALF * c)) & (row < HALF)
        window = jnp.broadcast_to(mod_row[:, first : first + 256], (HP, 256))
        value = jnp.sum(jnp.where(take, window, 0.0), axis=1, keepdims=True)
        gain[b] = jnp.broadcast_to(value, (HP, PIX))

    class Side:
        pass

    def side_a():
        s = Side()
        s.ag, s.rs = "ag_a", "rs_a"
        s.w, s.full, s.g, s.i1, s.i2 = wa_strips, wa, ga, x, y
        s.p1 = lambda d: peer(dx=d)
        s.p2 = lambda d: peer(dy=d)
        s.cut = (SIZE_W // 2, SIZE_W // 2)
        s.half1, s.half2, s.full1, s.full2 = rx1, ra1, rx2, ra2
        return s

    def side_b():
        s = Side()
        s.ag, s.rs = "ag_b", "rs_b"
        s.w, s.full, s.g, s.i1, s.i2 = wb_strips, wb, gb, y, x
        s.p1 = lambda d: peer(dy=d)
        s.p2 = lambda d: peer(dx=d)
        s.cut = (SIZE_W // 2, SIZE_G // 2)
        s.half1, s.half2, s.full1, s.full2 = ry1, rb1, ry2, rb2
        return s

    a, b = side_a(), side_b()

    def at1(s, d):
        return (s.i1 + d) % 4

    def at2(s, d):
        return (s.i2 + d) % 4

    def spot(s, d2, d1):
        return at2(s, d2) * 4 + at1(s, d1)

    def spread_out(s, d):
        block = s.w.at[spot(s, 0, d)]
        for e in (1, 3):
            onward = (e == 1) == (d < 2)
            name = (s.ag, "on", d) if onward else (s.ag, "pair", e)
            send(block, block, s.p2(e), s.ag, name)

    for s, name, got in ((a, "w1", w1_got), (b, "w2", w2_got)):
        landed(name, got.at[pl.ds(0, ROWS - 1)])
        parts = [unfold(got[q].astype(F32)) for q in range(ROWS)]
        parts.append(jnp.zeros((HALF, CP - WIDTH), F32))
        whole = jnp.concatenate(parts, axis=1)
        whole = jnp.concatenate([whole, jnp.zeros((HP - HALF, CP), F32)], axis=0)
        pack(whole, s.w, (spot(s, 0, 0),))
        block = s.w.at[spot(s, 0, 0)]
        for d in (1, 3):
            send(block, block, s.p1(d), s.ag, (s.ag, "first", d))
        spread_out(s, 0)
        s.full[s.i2, s.i1] = whole.astype(BF16)

    def pass_first(s, d):
        landed((s.ag, "first", d), s.w.at[0])
        first = 0 if d == 1 else s.cut[0]
        block = s.w.at[spot(s, 0, 4 - d), pl.ds(first, s.cut[0])]
        send(block, block, s.p1(d), s.ag, (s.ag, "halves"))

    def meet_halves(s):
        landed((s.ag, "halves"), s.w.at[0])
        spread_out(s, 2)

    def spread(s, d2, blocks):
        for d in blocks:
            at = (at2(s, d2), at1(s, d))
            s.full[at] = unpack(s.w[spot(s, d2, d)].astype(F32)).astype(BF16)

    def first_half(slab):
        weights = wa[slab].reshape(4 * HP, CP)
        value = dot(weights, s_full[...], NN).reshape(4, HP, PIX)
        for j in range(4):
            block = wa[slab, j].astype(F32)
            squares = jnp.sum(block * block, axis=1, keepdims=True)
            inv = jnp.broadcast_to(lax.rsqrt(squares + 1.0), (HP, PIX))
            act = value[j] * inv
            pre[slab * 4 + j] = act
            hidden = act * jax.nn.sigmoid(act) * SILU_GAIN * gain[slab * 4 + j]
            hid[j * 4 + slab] = hidden.astype(BF16)

    def pass_on(s, d):
        landed((s.ag, "on", d), s.w.at[0])
        e = 1 if d < 2 else 3
        block = s.w.at[spot(s, 4 - e, d)]
        send(block, block, s.p2(e), s.ag, (s.ag, "far"))

    def squares_of(slab):
        total = jnp.zeros((8, CP), F32)
        for j in range(4):
            block = wb[slab, j].astype(F32)
            total = total + jnp.sum((block * block).reshape(HP // 8, 8, CP), axis=0)
        return total

    def states_of(blocks):
        return jnp.concatenate([hid[i * 4 + j] for i, j in blocks], axis=0).T

    def branch(states, blocks, cols):
        weights = jnp.concatenate([wb[i, j, :, cols] for i, j in blocks], axis=0)
        return dot(states, weights, NN)

    def all_channels(blocks):
        parts = [blocks[q].astype(F32)[:CHAN] for q in range(ROWS)]
        parts.append(jnp.zeros((CP - WIDTH, PIX), F32))
        return jnp.concatenate(parts, axis=0).astype(BF16)

    def own_slab():
        landed("s2", s_all.at[pl.ds(0, 4)])
        s_full[...] = all_channels(s_all)
        spread(a, 0, (1, 2, 3))
        first_half(y)
        s_tok[...] = s_full[...].T

    def other_slab(d):
        spread(a, d, range(4))
        first_half(at2(a, d))

    def target_part():
        landed("t2", t_all.at[pl.ds(0, 4)])
        base[...] = KEEP_COEF * s_tok[...].astype(F32) - all_channels(t_all).T.astype(F32)

    def near_slabs():
        spread(b, 0, (1, 2, 3))
        spread(b, 1, range(4))
        spread(b, 3, range(4))
        norm_row[0] = squares_of(x) + squares_of(at2(b, 1)) + squares_of(at2(b, 3))

    def early_branch():
        blocks = [(at2(b, i), at2(a, j)) for i in (0, 1, 3) for j in (0, 1, 3)]
        states = states_of(blocks)
        for cut in CUTS:
            cols = slice(*cut)
            raw[:, cols] = branch(states, blocks, cols)

    def last_slab():
        spread(b, 2, range(4))
        norm_row[0] += squares_of(at2(b, 2))
        send(norm_row.at[0], norm_in, peer(dc=1), "norm", "norm")

    sides = {"a": a, "b": b}
    steps = {
        "first": pass_first,
        "spread": spread_out,
        "halves": meet_halves,
        "on": pass_on,
        "pair": lambda s, e: landed((s.ag, "pair", e), s.w.at[pl.ds(0, 2)]),
        "far": lambda s: landed((s.ag, "far"), s.w.at[pl.ds(0, 4)]),
        "own": own_slab,
        "below": lambda: other_slab(3),
        "above": lambda: other_slab(1),
        "opposite": lambda: other_slab(2),
        "target": target_part,
        "near": near_slabs,
        "early": early_branch,
        "last": last_slab,
    }
    for step, *at in GATHER:
        if step == "share":
            share(s_all if at[0] == "s" else t_all, at[0])
        else:
            steps[step](*(sides.get(q, q) for q in at))
    late = [(at2(b, i), at2(a, 2)) for i in (0, 1, 3)] + [(at2(b, 2), j) for j in range(4)]
    states = states_of(late)
    for i, cut in enumerate(CUTS):
        cols = slice(*cut)
        value = raw[:, cols] + branch(states, late, cols)
        raw[:, cols] = value
        raw_out[:, cols] = value.astype(BF16)
        part = pl.ds(cut[0], cut[1] - cut[0])
        send(raw_out.at[:, part], raw_in.at[:, part], peer(dc=1), "raw", ("raw", i))

    landed("norm", norm_in)
    norm = jnp.sum(norm_row[0] + norm_in[...], axis=0, keepdims=True)
    inv_row = lax.rsqrt(norm + 1.0)
    norm_row[1] = jnp.broadcast_to(inv_row, (8, CP))
    far_states = jnp.concatenate([hid[spot(b, 2, d)] for d in FAR], axis=0)
    for i, (low, high) in enumerate(CUTS):
        landed(("raw", i), raw_in.at[:, pl.ds(low, high - low)])
        cols = slice(low, high)
        sums = jnp.zeros((8, high - low), F32)
        inv = norm_row[1][0:1, cols] * ADD_COEF
        for q in range(8):
            rows = slice(q * 32, (q + 1) * 32)
            total = raw[rows, cols] + raw_in[rows, cols].astype(F32)
            grad = base[rows, cols] + total * inv
            dbranch = (ADD_COEF * grad).astype(BF16)
            dbr[rows, cols] = dbranch
            product = dbranch.astype(F32) * total
            sums = sums + jnp.sum(product.reshape(4, 8, high - low), axis=0)
        dot_rows[:, cols] = jnp.broadcast_to(
            jnp.sum(sums, axis=0, keepdims=True), (8, high - low)
        )
        far_grad[:, cols] = dot(far_states, dbr[:, cols], NN)
    row = lax.broadcasted_iota(jnp.int32, (HP, 1), 0)

    def second_grad(d2, first=()):
        order = (*first, *(d for d in range(4) if d not in first))
        places = [spot(b, d2, d) for d in order]
        if d2 == 2:
            value = far_grad[...]
        else:
            value = dot(jnp.concatenate([hid[i] for i in places], axis=0), dbr[...], NN)
        for j, d in enumerate(order):
            block = value[j * HP : (j + 1) * HP]
            block = jnp.where(row == HALF, dot_rows[0:1], block)
            pack(block, gb, (places[j],))
            if d in first:
                scatter_far(b, d)

    def first_grad(d2, first=()):
        slab = at2(a, d2)
        order = (*first, *(d for d in range(4) if d not in first))
        at = [at1(a, d) for d in order]
        weights = jnp.concatenate([wb[i, slab] for i in at], axis=0)
        back = dot(weights, dbn[...], NT).reshape(4, HP, PIX)
        for j in range(4):
            value = pre[slab * 4 + at[j]]
            sig = jax.nn.sigmoid(value)
            slope = sig * (1.0 + value * (1.0 - sig))
            dpre[j] = (back[j] * gain[slab * 4 + at[j]] * slope * SILU_GAIN).astype(BF16)
        value = dot(dpre[...].reshape(4 * HP, PIX), s_tok[...], NN)
        for j, d in enumerate(order):
            pack(value[j * HP : (j + 1) * HP], ga, (slab * 4 + at[j],))
            if d in first:
                scatter_far(a, d)

    def scatter_far(s, d):
        e = 1 if d < 2 else 3
        send(s.g.at[spot(s, 2, d)], s.half2.at[d], s.p2(e), s.rs, (s.rs, "half", d))

    def scatter_on(s, d, e):
        way = 0 if e == 1 else 1
        send(s.g.at[spot(s, e, d)], s.full2.at[way, d], s.p2(e), s.rs, (s.rs, "full", d))

    def scatter_near(s, d):
        scatter_on(s, d, 3 if d < 2 else 1)

    def scatter_relay(s, d):
        landed((s.rs, "half", d), s.half2.at[0])
        e = 1 if d < 2 else 3
        at = spot(s, e, d)
        s.g[at] = (s.g[at].astype(F32) + s.half2[d].astype(F32)).astype(BF16)
        scatter_on(s, d, e)

    def scatter_sum(s, d):
        landed((s.rs, "full", d), s.full2.at[0, pl.ds(0, 2)])
        at = spot(s, 0, d)
        total = s.g[at].astype(F32) + s.full2[0, d].astype(F32) + s.full2[1, d].astype(F32)
        if d == 0:
            s.own = total
        else:
            s.g[at] = total.astype(BF16)

    def ring_on(s, d, part):
        way = 0 if d == 1 else 1
        rows = pl.ds(part * s.cut[1], s.cut[1])
        send(s.g.at[spot(s, 0, d), rows], s.full1.at[way, rows], s.p1(d), s.rs, (s.rs, "near"))

    def ring_far(s):
        for part, d in enumerate((1, 3)):
            rows = pl.ds(part * s.cut[1], s.cut[1])
            send(s.g.at[spot(s, 0, 2), rows], s.half1.at[rows], s.p1(d), s.rs, (s.rs, "far", d))

    def ring_near(s, d):
        ring_on(s, d, 1 if d == 1 else 0)

    def ring_relay(s, d):
        part = 0 if d == 1 else 1
        rows = slice(part * s.cut[1], (part + 1) * s.cut[1])
        landed((s.rs, "far", d), s.half1.at[pl.ds(0, s.cut[1])])
        at = spot(s, 0, d)
        s.g[at, rows] = (s.g[at, rows].astype(F32) + s.half1[rows].astype(F32)).astype(BF16)
        ring_on(s, d, part)

    def ring_sum(s):
        landed((s.rs, "near"), s.full1)
        return s.own + s.full1[0].astype(F32) + s.full1[1].astype(F32)

    steps = {
        "far": scatter_far,
        "near": scatter_near,
        "relay": scatter_relay,
        "sum": scatter_sum,
        "ring_far": ring_far,
        "ring_near": ring_near,
        "ring_relay": ring_relay,
    }
    def hand_out(out, zs, zr, name):
        for q in range(ROWS):
            first = q * CHAN
            zs[q] = fold(out[:, first : first + CHAN]).astype(BF16)
        zr[r] = zs[r]
        for dz, dc in group:
            slot = zs.at[((z + dz) % 4) * 2 + (c + dc) % 2]
            send(slot, zr.at[r], peer(dz=dz, dc=dc), name, name)

    def finish_second():
        inv2 = norm_row[1][0:1]
        scaled = wb[x, y].astype(F32) * (inv2 * inv2 * inv2)
        grad2 = unpack(ring_sum(b))
        hand_out(grad2 * inv2 - scaled * grad2[HALF : HALF + 1], zs2, zr2, "z2")

    def finish_first():
        w1 = wa[y, x].astype(F32)
        inv1 = lax.rsqrt(jnp.sum(w1 * w1, axis=1, keepdims=True) + 1.0)
        scaled = w1 * (inv1 * inv1 * inv1)
        grad1 = unpack(ring_sum(a))
        dot1 = jnp.sum(w1 * grad1, axis=1, keepdims=True)
        hand_out(grad1 * inv1 - scaled * dot1, zs1, zr1, "z1")

    for step, *at in PLAN:
        if step == "hidden":
            dbn[...] = (dbr[...].astype(F32) * norm_row[1][0:1]).astype(BF16)
        elif step == "finish" and at[0] == "b":
            finish_second()
        elif step == "finish":
            finish_first()
        elif step == "grad":
            side = sides[at[0]]
            (first_grad if side is a else second_grad)(*at[1:])
        else:
            steps[step](sides[at[0]], *at[1:])

    landed("z2", zr2.at[pl.ds(0, ROWS - 1)])
    for core in range(2):
        value = unfold(sum(zr2[2 * q + core].astype(F32) for q in range(4))) / SAMPLES
        out2[core * HALF : (core + 1) * HALF, 0, :] = value
    landed("z1", zr1.at[pl.ds(0, ROWS - 1)])
    both = [sum(zr1[2 * q + core].astype(F32) for q in range(4)) / SAMPLES for core in range(2)]
    both.append(jnp.zeros((128 - 2 * FOLD, 128), F32))
    turned = jnp.concatenate(both, axis=0).T
    third, rest = HALF // 3, CHAN - 128
    top, bottom = [], []
    for core in range(2):
        first = core * FOLD
        top.append(turned[:, first : first + HALF])
        for i in range(3):
            lanes = slice(first + HALF, first + FOLD)
            bottom.append(turned[i * rest : (i + 1) * rest, lanes])
    out1[0, :128, :] = jnp.concatenate(top, axis=1)
    out1[0, 128:, :] = jnp.concatenate(bottom, axis=1)
    for name, view in (("w1", w1_got), ("w2", w2_got), ("s", s_all), ("t", t_all), ("z1", zs1), ("z2", zs2)):
        sent(name, view.at[pl.ds(0, ROWS - 1)])
    for s in (a, b):
        sent(s.ag, s.w.at[pl.ds(0, 15)])
        sent(s.rs, s.g.at[pl.ds(0, 15)])
    sent("norm", norm_in)
    sent("raw", raw_out)
    if (len(out_names), len(in_names)) != (SENDS, LANDINGS):
        raise ValueError((len(out_names), len(in_names)))


def write_out(first, second, out1, out2, sems):
    copies = [
        pltpu.make_async_copy(src, dst, sems.at[i])
        for i, (src, dst) in enumerate(((first, out1), (second, out2)))
    ]
    for copy in copies:
        copy.start()
    for copy in copies:
        copy.wait()


def local(clean, noise, bucket, mod_table, w_first, w_second):
    vmem = pl.BlockSpec(memory_space=pltpu.VMEM)
    smem = pl.BlockSpec(memory_space=pltpu.SMEM)
    hbm = pl.BlockSpec(memory_space=pl.ANY)
    block = (HP, CP)
    first, second = pl.pallas_call(
        kernel,
        out_shape=(
            jax.ShapeDtypeStruct((1, CHAN, BLOCK), F32),
            jax.ShapeDtypeStruct((BLOCK, 1, CHAN), F32),
        ),
        in_specs=[hbm, hbm, smem, hbm, hbm, hbm],
        out_specs=(vmem, vmem),
        scratch_shapes=[
            pltpu.VMEM(clean.shape, F32),
            pltpu.VMEM(noise.shape, F32),
            pltpu.VMEM((BUCKETS, WIDTH), F32),
            pltpu.VMEM((CHAN, BLOCK), F32),
            pltpu.VMEM((BLOCK, CHAN), F32),
            pltpu.VMEM((2, FOLD, 128), BF16),
            pltpu.VMEM((2, FOLD, 128), BF16),
            pltpu.VMEM((ROWS, FOLD, 128), BF16),
            pltpu.VMEM((ROWS, FOLD, 128), BF16),
            pltpu.VMEM((4, CHAN_PAD, PIX), BF16),
            pltpu.VMEM((4, CHAN_PAD, PIX), BF16),
            pltpu.VMEM((ROWS, CHAN_PAD, PIX), BF16),
            pltpu.VMEM((ROWS, CHAN_PAD, PIX), BF16),
            pltpu.VMEM((CP, PIX), BF16),
            pltpu.VMEM((PIX, CP), BF16),
            pltpu.VMEM((PIX, CP), F32),
            pltpu.VMEM((4, 4, *block), BF16),
            pltpu.VMEM((4, 4, *block), BF16),
            pltpu.VMEM((16, SIZE_W, 128), BF16),
            pltpu.VMEM((16, SIZE_W, 128), BF16),
            pltpu.VMEM((16, SIZE_W, 128), BF16),
            pltpu.VMEM((16, SIZE_G, 128), BF16),
            pltpu.VMEM((4, SIZE_W, 128), BF16),
            pltpu.VMEM((2, 4, SIZE_W, 128), BF16),
            pltpu.VMEM((SIZE_W, 128), BF16),
            pltpu.VMEM((2, SIZE_W, 128), BF16),
            pltpu.VMEM((4, SIZE_G, 128), BF16),
            pltpu.VMEM((2, 4, SIZE_G, 128), BF16),
            pltpu.VMEM((SIZE_G, 128), BF16),
            pltpu.VMEM((2, SIZE_G, 128), BF16),
            pltpu.VMEM((16, HP, PIX), F32),
            pltpu.VMEM((16, HP, PIX), F32),
            pltpu.VMEM((16, HP, PIX), BF16),
            pltpu.VMEM((4, HP, PIX), BF16),
            pltpu.VMEM((PIX, CP), F32),
            pltpu.VMEM((PIX, CP), BF16),
            pltpu.VMEM((PIX, CP), BF16),
            pltpu.VMEM((2, 8, CP), F32),
            pltpu.VMEM((8, CP), F32),
            pltpu.VMEM((PIX, CP), BF16),
            pltpu.VMEM((PIX, CP), BF16),
            pltpu.VMEM((8, CP), F32),
            pltpu.VMEM((4 * HP, CP), F32),
            pltpu.VMEM((ROWS, FOLD, 128), BF16),
            pltpu.VMEM((ROWS, FOLD, 128), BF16),
            pltpu.VMEM((ROWS, FOLD, 128), BF16),
            pltpu.VMEM((ROWS, FOLD, 128), BF16),
            pltpu.SemaphoreType.DMA((5,)),
            pltpu.SemaphoreType.DMA((SENDS,)),
            pltpu.SemaphoreType.DMA((LANDINGS,)),
        ],
        compiler_params=pltpu.CompilerParams(
            collective_id=0,
            has_side_effects=True,
            vmem_limit_bytes=55040 * 1024,
        ),
    )(clean, noise, bucket, mod_table, w_first, jnp.transpose(w_second, (1, 0, 2)))
    first, second = pl.pallas_call(
        write_out,
        out_shape=(
            jax.ShapeDtypeStruct(first.shape, F32),
            jax.ShapeDtypeStruct(second.shape, F32),
        ),
        in_specs=[hbm, hbm],
        out_specs=(hbm, hbm),
        scratch_shapes=[pltpu.SemaphoreType.DMA((2,))],
        compiler_params=pltpu.CompilerParams(vmem_limit_bytes=1024 * 1024),
    )(first, second)
    return first, jnp.transpose(second, (1, 0, 2))


def solution(mesh):
    in_specs = (
        P("row", "col"),
        P("row", "col"),
        P(),
        P(),
        P(None, "row", "col"),
        P(None, "col", "row"),
    )
    out_specs = (P(None, "row", "col"), P(None, "col", "row"))
    return jax.shard_map(local, mesh=mesh, in_specs=in_specs, out_specs=out_specs, check_vma=False)
```
